32 devices in a mesh: group: 2 (over core), fsdp: 4 (over z), tp: 4 (over y, x).
Axes of the slice: x: 2, y: 2, z: 4, core: 2. Of those that a mesh axis runs over, the one named last changes fastest.
Arguments:
- text_embeds: bfloat16 [4096, 8192], P(('group', 'fsdp'), 'tp'), may hold values from -6 to 6
- image_embeds: bfloat16 [2048, 8192], P(('group', 'fsdp'), 'tp'), may hold values from -6 to 6
- key_weight: bfloat16 [8192, 512], P(('group', 'fsdp')), may hold values from -0.0625 to 0.0625
- key_bias: float32 [512], P('tp'), may hold values from -3 to 3
- key_cot: bfloat16 [4096, 512], P(('group', 'fsdp')), may hold values from -6 to 6
- image_owner: int32 [2048], P(('group', 'fsdp')), may hold values from 0 to 7, as said below
- image_slot: int32 [4096], P(('group', 'fsdp')), may hold values from -1 to 511, as said below
- seq_lengths: int32 [16], P(('group', 'fsdp')), may hold values from 248 to 256, as said below
Outputs:
- key_rows: bfloat16 [4096, 512], P(('group', 'fsdp'), 'tp')
- text_grad: bfloat16 [4096, 8192], P(('group', 'fsdp'), 'tp')
- image_grad: bfloat16 [2048, 8192], P(('group', 'fsdp'), 'tp')
- weight_grad: float32 [8192, 512], P(('group', 'fsdp'), 'tp')
The draws below stay inside these ranges and needn't reach their ends.
Inputs may be any that keep to these rules, and one draw needn't show every extreme that they name: `image_owner`: A source block of 256 image tokens sends at most 64 of them to one owner, and some block sends exactly 64 to some owner; an owner takes at most 448 image tokens in all, and some owner takes exactly that many. Every image token has exactly one position, as step one says. `image_slot`: slots are distinct within an owner block, and image tokens sit only at live positions. `seq_lengths`: some sequence has length 256.
All inputs are finite; a program needn't handle non-finite values.
Results may differ from the reference program's by a relative error of at most 0.0046.
Values may be sent and summed in bfloat16 or wider, within the bound.
A program may use at most 64 MiB of HBM per device.

```python
import jax
import jax.numpy as jnp
from jax import lax

D = 8192
HEAD_DIM = 128
LENGTH = 256
SEQ_DEV = 2
KW = 512
UNITS = 8
LANG_DEV = 512
IMG_DEV = 256
CAP = 64
LANG_TOKENS = 4096
IMG_TOKENS = 2048


def layout_tables(key):
    base_key = jax.random.fold_in(key, 9137)
    subkeys = jax.random.split(base_key, 8)
    unit_count = UNITS
    quantum = LANG_DEV // (8 * UNITS)
    ordinal = jnp.arange(unit_count, dtype=jnp.int32)
    heavy_count = jax.random.randint(subkeys[0], (), 1, unit_count // 2 + 1)
    light_count = jax.random.randint(subkeys[1], (), 1, unit_count // 2 + 1)
    owner_sorted = jnp.where(ordinal < heavy_count, 6 * quantum, jnp.where(ordinal < unit_count - heavy_count, 3 * quantum, 0)).astype(jnp.int32)
    offset_sorted = jnp.where(ordinal < light_count, 2 * quantum, jnp.where(ordinal < unit_count - light_count, quantum, 0)).astype(jnp.int32)
    owner_load = owner_sorted[jax.random.permutation(subkeys[2], unit_count)]
    offset_load = offset_sorted[jax.random.permutation(subkeys[3], unit_count)]
    shift_index = (ordinal[None, :] - ordinal[:, None]) % unit_count
    counts = (owner_load[None, :] + offset_load[shift_index]).astype(jnp.int32)
    cum_owner = jnp.cumsum(counts, axis=1)
    token_index = jnp.arange(IMG_DEV, dtype=jnp.int32)
    owner_list = jnp.sum((cum_owner[:, None, :] <= token_index[None, :, None]).astype(jnp.int32), axis=2)
    row_keys = jax.random.split(subkeys[4], unit_count)
    row_perms = jax.vmap(lambda one_key: jax.random.permutation(one_key, IMG_DEV))(row_keys)
    owners = jnp.take_along_axis(owner_list, row_perms, axis=1).astype(jnp.int32)
    seq_total = unit_count * SEQ_DEV
    padding = jax.random.randint(subkeys[5], (seq_total,), 0, LENGTH // 32 + 1)
    full_one = jax.random.randint(subkeys[6], (), 0, seq_total)
    lengths = (LENGTH - jnp.where(jnp.arange(seq_total) == full_one, 0, padding)).astype(jnp.int32)
    within = jnp.arange(LANG_DEV, dtype=jnp.int32)
    live_table = within[None, :] % LENGTH < lengths.reshape(unit_count, SEQ_DEV)[:, within // LENGTH]
    place_keys = jax.random.split(subkeys[7], unit_count)
    place_perms = jax.vmap(lambda one_key: jax.random.permutation(one_key, LANG_DEV))(place_keys)
    live_perm = jnp.take_along_axis(live_table, place_perms, axis=1)
    arrival = jnp.cumsum(live_perm.astype(jnp.int32), axis=1) - 1
    incoming = jnp.sum(counts, axis=0)
    chosen = live_perm & (arrival < incoming[:, None])
    cum_source = jnp.cumsum(counts, axis=0).T
    source_ids = jnp.sum((cum_source[:, None, :] <= arrival[:, :, None]).astype(jnp.int32), axis=2)
    source_ids = jnp.clip(source_ids, 0, unit_count - 1)
    start_table = (jnp.cumsum(counts, axis=0) - counts).T
    source_start = jnp.take_along_axis(start_table, source_ids, axis=1)
    slot_value = jnp.where(chosen, source_ids * CAP + arrival - source_start, -1).astype(jnp.int32)
    slots = jnp.zeros((unit_count, LANG_DEV), jnp.int32).at[ordinal[:, None], place_perms].set(slot_value)
    return (owners.reshape(-1), slots.reshape(-1), lengths)


def draw_image_owner(key, part):
    return layout_tables(key)[0]


def draw_image_slot(key, part):
    return layout_tables(key)[1]


def draw_seq_lengths(key, part):
    return layout_tables(key)[2]


def spiked(values, rng, source, target, shards_of, factor):
    def block_of(dim):
        return (jnp.arange(values.shape[dim]) // (values.shape[dim] // shards_of)).reshape((-1,) + (1,) * (values.ndim - 1 - dim))

    near = jax.random.permutation(rng, shards_of)[block_of(target)]
    second = (block_of(target) + shards_of // 2) % shards_of
    return jnp.where((block_of(source) == near) | (block_of(source) == second), factor * values, values)


def levels(rng, dims, cuts, least, high):
    def one(axis_at, blocks):
        steps = jax.random.uniform(jax.random.fold_in(jax.random.fold_in(rng, 6), axis_at), (blocks,), jnp.float32, least / len(cuts), high / len(cuts))
        return jnp.repeat(jnp.exp(steps), dims[axis_at] // blocks).reshape((-1,) + (1,) * (len(dims) - axis_at - 1))

    factor_of = one(*cuts[0])
    for cut in cuts[1:]:
        factor_of = factor_of * one(*cut)
    return factor_of


def bell_draw(stream_key, shape, width, limit, cuts=(), kind=jnp.bfloat16):
    loudness = levels(stream_key, shape, cuts, -0.22, 0.18) if cuts else 1.0
    drawn = jax.random.normal(stream_key, shape, jnp.float32) * width * loudness
    return jnp.minimum(jnp.maximum(drawn, -limit), limit).astype(kind)


def heavy_noise(own_key, extent, width, reach, shards, heavy, held_as=jnp.bfloat16):
    result = width * jax.random.normal(own_key, extent, jnp.float32)
    if shards:
        result = result * levels(own_key, extent, shards, -0.22, 0.18)
    return jnp.clip(spiked(result, jax.random.fold_in(own_key, 3), *heavy), -reach, reach).astype(held_as)


def setup_inputs(seed: int = 0) -> dict:
    key_list = jax.random.split(jax.random.key(seed), 9)
    return {
        "text_embeds": heavy_noise(key_list[0], (LANG_TOKENS, D), 1.0, 6.0, ((0, 8), (1, 4)), (0, 1, 8, 2.0)),
        "image_embeds": bell_draw(key_list[1], (IMG_TOKENS, D), 1.0, 6.0, ((0, 8), (1, 4))),
        "key_weight": bell_draw(key_list[2], (D, KW), D ** -0.5, 0.0625, ((0, 8),)),
        "key_bias": bell_draw(key_list[3], (KW,), 0.5, 3.0, ((0, 4),), jnp.float32),
        "key_cot": bell_draw(key_list[4], (LANG_TOKENS, KW), 1.0, 6.0, ((0, 8),)),
        "image_owner": draw_image_owner(jax.random.fold_in(key_list[8], 71), 0),
        "image_slot": draw_image_slot(jax.random.fold_in(key_list[8], 71), 0),
        "seq_lengths": draw_seq_lengths(jax.random.fold_in(key_list[8], 71), 0),
    }


ROPE_BASE = 1000000.0


def angles(row_total):
    position = (jnp.arange(row_total, dtype=jnp.int32) % LENGTH).astype(jnp.float32)
    frequency = ROPE_BASE ** (-(jnp.arange(HEAD_DIM // 2, dtype=jnp.float32) * 2.0) / HEAD_DIM)
    angle_table = position[:, None] * frequency[None, :]
    return jnp.cos(angle_table), jnp.sin(angle_table)


def rotate(values, cosine, sine, direction):
    row_total = values.shape[0]
    by_head = values.reshape(row_total, -1, HEAD_DIM)
    half_dim = HEAD_DIM // 2
    front_half = by_head[..., :half_dim]
    second = by_head[..., half_dim:]
    cos_part = cosine[:, None, :]
    sin_part = direction * sine[:, None, :]
    rotated = jnp.concatenate([front_half * cos_part - second * sin_part, second * cos_part + front_half * sin_part], axis=-1)
    return rotated.reshape(row_total, -1)


def reference(text_embeds, image_embeds, key_weight, key_bias, key_cot, image_owner, image_slot, seq_lengths):
    unit_count = UNITS
    owners = image_owner.reshape(unit_count, IMG_DEV)
    ordinal = jnp.arange(unit_count, dtype=jnp.int32)
    marks = (owners[:, :, None] == ordinal[None, None, :]).astype(jnp.int32)
    before = jnp.cumsum(marks, axis=1) - marks
    owner_rank = jnp.sum(before * marks, axis=2)
    destination = owners * (unit_count * CAP) + ordinal[:, None] * CAP + owner_rank
    source_table = jnp.zeros((unit_count * unit_count * CAP,), jnp.int32).at[destination.reshape(-1)].set(jnp.arange(unit_count * IMG_DEV, dtype=jnp.int32))
    slots = image_slot.reshape(unit_count, LANG_DEV)
    is_image = (slots >= 0).reshape(-1)
    lookup = (ordinal[:, None] * (unit_count * CAP) + jnp.maximum(slots, 0)).reshape(-1)
    image_row = source_table[lookup]
    hidden = jnp.where(is_image[:, None], image_embeds[image_row], text_embeds)
    position = jnp.arange(LANG_TOKENS, dtype=jnp.int32)
    live_mask = ((position % LENGTH) < seq_lengths[position // LENGTH]).astype(jnp.float32)
    cosine, sine = angles(LANG_TOKENS)
    projected = jnp.dot(hidden, key_weight, preferred_element_type=jnp.float32) + key_bias
    key_rows = (rotate(projected, cosine, sine, 1.0) * live_mask[:, None]).astype(jnp.bfloat16)
    masked = key_cot.astype(jnp.float32) * live_mask[:, None]
    rotated_back = rotate(masked, cosine, sine, -1.0).astype(jnp.bfloat16)
    hidden_grad = lax.dot_general(rotated_back, key_weight, (((1,), (1,)), ((), ())), preferred_element_type=jnp.float32).astype(jnp.bfloat16)
    text_grad = jnp.where(is_image[:, None], jnp.zeros_like(hidden_grad), hidden_grad)
    token_place = jnp.zeros((unit_count * IMG_DEV,), jnp.int32).at[jnp.where(is_image, image_row, unit_count * IMG_DEV)].set(position, mode="drop")
    image_grad = hidden_grad[token_place]
    weight_grad = lax.dot_general(hidden, rotated_back, (((0,), (0,)), ((), ())), preferred_element_type=jnp.float32) / LANG_DEV
    return key_rows, text_grad, image_grad, weight_grad
```

```python
import functools

import jax
import jax.numpy as jnp
import numpy as np
from jax import lax
from jax.experimental import pallas as pl
from jax.experimental.pallas import tpu as pltpu
from jax.sharding import PartitionSpec as P

HEAD_DIM = 128
LENGTH = 256


ROPE_BASE = 1000000.0


def angles(row_total):
    position = (jnp.arange(row_total, dtype=jnp.int32) % LENGTH).astype(jnp.float32)
    frequency = ROPE_BASE ** (-(jnp.arange(HEAD_DIM // 2, dtype=jnp.float32) * 2.0) / HEAD_DIM)
    angle_table = position[:, None] * frequency[None, :]
    return (jnp.cos(angle_table), jnp.sin(angle_table))


def rotate(values, cosine, sine, direction):
    row_total = values.shape[0]
    by_head = values.reshape(row_total, -1, HEAD_DIM)
    half_dim = HEAD_DIM // 2
    front_half = by_head[..., :half_dim]
    second = by_head[..., half_dim:]
    cos_part = cosine[:, None, :]
    sin_part = direction * sine[:, None, :]
    rotated = jnp.concatenate(
        [front_half * cos_part - second * sin_part, second * cos_part + front_half * sin_part],
        axis=-1,
    )
    return rotated.reshape(row_total, -1)


def send_slots(owners, unit_count, capacity):
    onehot_marks = (owners[:, None] == jnp.arange(unit_count, dtype=jnp.int32)[None, :]).astype(
        jnp.int32
    )
    before = jnp.cumsum(onehot_marks, axis=0) - onehot_marks
    owner_rank = jnp.sum(before * onehot_marks, axis=1)
    return owners * capacity + owner_rank


def share_kernel(text_ref, image_ref, back_ref, image_back_ref, out_ref):
    contract = (((0,), (0,)), ((), ()))
    part = lax.dot_general(
        text_ref[...], back_ref[...], contract, preferred_element_type=jnp.float32
    ) + lax.dot_general(
        image_ref[...], image_back_ref[...], contract, preferred_element_type=jnp.float32
    )
    part = part.astype(out_ref.dtype)
    width = out_ref.shape[2]
    for head in range(out_ref.shape[0]):
        out_ref[head] = part[:, head * width : (head + 1) * width]


def weight_shares(text, image, back, image_back, head_cols):
    columns = text.shape[1]
    heads = back.shape[1] // head_cols
    tile = min(512, columns)
    return pl.pallas_call(
        share_kernel,
        grid=(columns // tile,),
        in_specs=[
            pl.BlockSpec((text.shape[0], tile), lambda i: (0, i)),
            pl.BlockSpec((image.shape[0], tile), lambda i: (0, i)),
            pl.BlockSpec(back.shape, lambda i: (0, 0)),
            pl.BlockSpec(image_back.shape, lambda i: (0, 0)),
        ],
        out_specs=pl.BlockSpec((heads, tile, head_cols), lambda i: (0, i, 0)),
        out_shape=jax.ShapeDtypeStruct((heads, columns, head_cols), jnp.bfloat16),
        cost_estimate=pl.CostEstimate(
            flops=2 * (text.size + image.size) * back.shape[1],
            bytes_accessed=2 * (text.size + image.size + columns * back.shape[1]),
            transcendentals=0,
        ),
    )(text, image, back, image_back)


def project_kernel(text_ref, image_ref, weight_ref, out_ref):
    step = pl.program_id(0)
    last = pl.num_programs(0) - 1
    rows = jnp.where(step == last, image_ref[...], text_ref[...])
    part = jnp.dot(rows, weight_ref[...], preferred_element_type=jnp.float32).astype(out_ref.dtype)
    width = out_ref.shape[2]
    for head in range(out_ref.shape[0]):
        out_ref[head] = part[:, head * width : (head + 1) * width]


def projection_parts(text, image, weight, head_cols):
    heads = weight.shape[1] // head_cols
    tile, columns = image.shape
    text_tiles = text.shape[0] // tile
    return pl.pallas_call(
        project_kernel,
        grid=(text_tiles + 1,),
        in_specs=[
            pl.BlockSpec((tile, columns), lambda i: (jnp.minimum(i, text_tiles - 1), 0)),
            pl.BlockSpec((tile, columns), lambda i: (0, 0)),
            pl.BlockSpec(weight.shape, lambda i: (0, 0)),
        ],
        out_specs=pl.BlockSpec((heads, tile, head_cols), lambda i: (0, i, 0)),
        out_shape=jax.ShapeDtypeStruct((heads, text.shape[0] + tile, head_cols), jnp.bfloat16),
        cost_estimate=pl.CostEstimate(
            flops=2 * (text.size + image.size) * weight.shape[1],
            bytes_accessed=2 * (text.size + image.size + weight.size),
            transcendentals=0,
        ),
    )(text, image, weight)


def spread(piece, axis):
    count = lax.axis_size(axis)
    copies = jnp.broadcast_to(piece[None], (count,) + piece.shape)
    got = lax.all_to_all(copies, axis, split_axis=0, concat_axis=0, tiled=True)
    return got.reshape((count * piece.shape[0],) + piece.shape[1:])


def shifted(values, axis, step):
    count = lax.axis_size(axis)
    return lax.ppermute(values, axis, [(i, (i + step) % count) for i in range(count)])


def exchange_sum(blocks, axis):
    count = lax.axis_size(axis)
    me = lax.axis_index(axis)
    total = lax.dynamic_index_in_dim(blocks, me, 0, keepdims=False).astype(jnp.float32)
    for step in range(1, count):
        block = lax.dynamic_index_in_dim(blocks, (me + step) % count, 0, keepdims=False)
        total = total + shifted(block, axis, step).astype(jnp.float32)
    return total


def share_rows(piece, axis):
    count = lax.axis_size(axis)
    me = lax.axis_index(axis)
    rows = piece.shape[0]
    full = jnp.zeros((count * rows,) + piece.shape[1:], piece.dtype)
    full = lax.dynamic_update_slice_in_dim(full, piece, me * rows, 0)
    for step in range(1, count):
        source = (me + count - step) % count
        full = lax.dynamic_update_slice_in_dim(full, shifted(piece, axis, step), source * rows, 0)
    return full


def per_device_plain(
    text_embeds, image_embeds, key_weight, key_bias, key_cot, image_owner, image_slot, seq_lengths
):
    row_count, columns = text_embeds.shape
    image_count = image_embeds.shape[0]
    units = ("group", "fsdp")
    core_count = lax.axis_size("group")
    fsdp_count = lax.axis_size("fsdp")
    tp_count = lax.axis_size("tp")
    unit_count = core_count * fsdp_count
    capacity = row_count // unit_count
    slot_count = unit_count * capacity
    head_cols = key_bias.shape[0]
    key_cols = head_cols * tp_count
    weight_block = key_weight.shape[0]
    halves = unit_count // tp_count
    tp_index = lax.axis_index("tp")

    position = jnp.arange(row_count, dtype=jnp.int32)
    seq_ids = position // LENGTH
    seq_marks = seq_ids[:, None] == jnp.arange(seq_lengths.shape[0], dtype=jnp.int32)[None, :]
    live_limit = jnp.sum(jnp.where(seq_marks, seq_lengths[None, :], 0), axis=1)
    live_mask = (position % LENGTH < live_limit).astype(jnp.float32)
    cosine, sine = angles(row_count)
    masked = key_cot.astype(jnp.float32) * live_mask[:, None]
    rotated_back = rotate(masked, cosine, sine, -1.0).astype(jnp.bfloat16)
    is_image = image_slot >= 0
    text_back = jnp.where(is_image[:, None], jnp.zeros_like(rotated_back), rotated_back)

    slot_ids = jnp.arange(slot_count, dtype=jnp.int32)
    place = (image_slot[:, None] == slot_ids[None, :]).astype(jnp.bfloat16)
    returning = lax.dot_general(
        place, rotated_back, (((0,), (0,)), ((), ())), preferred_element_type=jnp.float32
    ).astype(jnp.bfloat16)
    returned = lax.all_to_all(
        returning.reshape(unit_count, capacity, key_cols), units, split_axis=0, concat_axis=0,
        tiled=True,
    ).reshape(slot_count, key_cols)
    slots_out = send_slots(image_owner, unit_count, capacity)
    pick = (slots_out[:, None] == slot_ids[None, :]).astype(jnp.bfloat16)
    image_back = jnp.dot(pick, returned, preferred_element_type=jnp.float32).astype(jnp.bfloat16)

    piece_rows = weight_block // tp_count
    own_piece = lax.dynamic_slice_in_dim(key_weight, tp_index * piece_rows, piece_rows, 0)
    moves = []
    for unit in range(unit_count):
        for part in range(tp_count):
            target = (unit % halves) * tp_count + part
            moves.append((unit * tp_count + part, target * tp_count + unit // halves))
    own_piece = lax.ppermute(own_piece, units + ("tp",), moves)
    chip_rows = spread(own_piece, "fsdp")

    shares = weight_shares(text_embeds, image_embeds, text_back, image_back, head_cols)
    shares = shares.reshape(core_count, fsdp_count, weight_block, head_cols)
    shares = exchange_sum(shares, "group").astype(jnp.bfloat16)
    shares, chip_rows = lax.optimization_barrier((shares, chip_rows))
    shares = lax.all_to_all(shares, "fsdp", split_axis=0, concat_axis=0, tiled=True)
    weight_grad = jnp.sum(shares.astype(jnp.float32), axis=0) / row_count
    returns = []
    for unit in range(unit_count):
        for part in range(tp_count):
            holder = (unit % halves) + part * halves
            returns.append((holder * tp_count + unit // halves, unit * tp_count + part))
    weight_grad = lax.ppermute(weight_grad, units + ("tp",), returns)

    weight_rows = share_rows(chip_rows, "group")
    both = projection_parts(text_embeds, image_embeds, weight_rows, head_cols)
    both = exchange_sum(both, "tp")
    image_proj = both[row_count:].astype(jnp.bfloat16)
    outgoing = lax.dot_general(
        pick, image_proj, (((0,), (0,)), ((), ())), preferred_element_type=jnp.float32
    ).astype(jnp.bfloat16)
    received = lax.all_to_all(
        outgoing.reshape(unit_count, capacity, head_cols), units, split_axis=0, concat_axis=0,
        tiled=True,
    ).reshape(slot_count, head_cols)
    placed = jnp.dot(place, received, preferred_element_type=jnp.float32)
    projected = jnp.where(is_image[:, None], placed, both[:row_count]) + key_bias
    key_rows = (rotate(projected, cosine, sine, 1.0) * live_mask[:, None]).astype(jnp.bfloat16)

    contract = (((1,), (1,)), ((), ()))
    text_grad = lax.dot_general(
        text_back, weight_rows, contract, preferred_element_type=jnp.float32
    ).astype(jnp.bfloat16)
    image_grad = lax.dot_general(
        image_back, weight_rows, contract, preferred_element_type=jnp.float32
    ).astype(jnp.bfloat16)
    return (key_rows, text_grad, image_grad, weight_grad)


MESH = pl.DeviceIdType.MESH
HALF = HEAD_DIM // 2
ROWS_TO_COLS = (((0,), (0,)), ((), ()))
COLS_TO_COLS = (((1,), (1,)), ((), ()))
W_PARTS = 4
G_PARTS = 8


def fused_kernel(
    groups, fsdp, tp, capacity,
    text_ref, image_ref, weight_ref, bias_ref, cot_ref, owner_ref, slot_ref, lens_ref, cos_ref, sin_ref,
    keys_out, text_out, image_out, wgrad_out,
    x, w, cot, cosv, sinv, back, pick_t, place_t, is_img,
    d1_src, d1_dst, d2_src, pf, pa, pb, chain, above, below, y, yb, yr, c2_src, c2_dst, gout, landed, wg, keys,
    ld, w_recv, w_up, w_dn, w_dd, d1_s, d1_r, d2_s, d2_r, ci_s, ci_r, ct_s, ct_r, c2_s, c2_r,
    p_s, p_r, ab_r, be_r, ch_s, g_s, g_r, st,
):
    f32, bf16 = jnp.float32, jnp.bfloat16
    g, z, t = lax.axis_index("group"), lax.axis_index("fsdp"), lax.axis_index("tp")
    units = groups * fsdp
    me = g * fsdp + z
    rows, images = text_ref.shape[0], image_ref.shape[0]
    both = rows + images
    columns = text_ref.shape[1]
    slots = units * capacity
    cols = bias_ref.shape[1]
    block = weight_ref.shape[0]
    blocks = units // tp
    w_rows, g_rows = block // W_PARTS, block // G_PARTS
    w_steps, g_steps = blocks * W_PARTS, blocks * G_PARTS
    first = t * blocks
    carrier, z0 = first // fsdp, lax.rem(first, fsdp)
    carries = g == carrier
    inside = (z >= z0) & (z < z0 + blocks)
    far_end = jnp.logical_not(inside) & ((z == 0) | (z == fsdp - 1))
    adjacent = inside | (z == z0 - 1) | (z == z0 + blocks)
    my_cols = pl.ds(pl.multiple_of(t * cols, cols), cols)
    peer = (1 - g, z, t)

    def near_block(k):
        within = lax.rem(z - z0 + k + blocks, blocks)
        return jnp.where(inside, within, jnp.where(z < z0, k, blocks - 1 - k))

    def unit_of(i):
        v = lax.rem(me + i, units)
        return v, (v // fsdp, lax.rem(v, fsdp), t)

    def head_of(i):
        q = lax.rem(t + i, tp)
        return q, (g, z, q)

    def remote(src, dst, send, recv, device):
        return pltpu.make_async_remote_copy(
            src_ref=src, dst_ref=dst, send_sem=send, recv_sem=recv, device_id=device, device_id_type=MESH
        )

    barrier = pltpu.get_barrier_semaphore()
    for i in range(1, units):
        pl.semaphore_signal(barrier, inc=1, device_id=unit_of(i)[1], device_id_type=MESH)
    for i in range(1, tp):
        q = head_of(i)[0]
        for core in range(groups):
            pl.semaphore_signal(barrier, inc=1, device_id=(core, z, q), device_id_type=MESH)

    loads = [
        pltpu.make_async_copy(cot_ref, cot, ld.at[0]),
        pltpu.make_async_copy(cos_ref, cosv, ld.at[1]),
        pltpu.make_async_copy(sin_ref, sinv, ld.at[2]),
        pltpu.make_async_copy(text_ref, x.at[pl.ds(0, rows)], ld.at[3]),
        pltpu.make_async_copy(image_ref, x.at[pl.ds(rows, images)], ld.at[4]),
    ]
    for load in loads[:3]:
        load.start()

    def w_slice(b, c):
        return pl.ds(pl.multiple_of(b * block + c * w_rows, w_rows), w_rows)

    def w_load(b, c):
        return pltpu.make_async_copy(
            weight_ref.at[pl.ds(pl.multiple_of(c * w_rows, w_rows), w_rows)], w.at[w_slice(b, c)], w_recv.at[b * W_PARTS + c]
        )

    @pl.when(carries & inside)
    def _():
        for c in range(W_PARTS):
            w_load(z - z0, c).start()

    for load in loads[3:]:
        load.start()

    slot_ids = lax.broadcasted_iota(jnp.int32, (slots, rows), 0)
    place_t[...] = jnp.where(slot_ids == slot_ref[...], 1.0, 0.0).astype(bf16)
    is_img[...] = lax.dot_general(
        place_t[...], jnp.ones((slots, cols), bf16), ROWS_TO_COLS, preferred_element_type=f32
    )
    row_ids = lax.broadcasted_iota(jnp.int32, (LENGTH, HEAD_DIM), 0)

    def live(s):
        return row_ids < lens_ref[0:1, s : s + 1]

    def rotated_back(s, at):
        span = pl.ds(s * LENGTH, LENGTH)
        values = jnp.where(live(s), cot[span, at].astype(f32), 0.0)
        return values * cosv[...] - pltpu.roll(values, HALF, 1) * sinv[...]

    for load in loads[:3]:
        load.wait()
    mine = jnp.concatenate([rotated_back(s, my_cols) for s in range(rows // LENGTH)], axis=0).astype(bf16)
    d1_src[...] = jnp.dot(place_t[...], mine, preferred_element_type=f32).astype(bf16)

    pl.semaphore_wait(barrier, units - 1 + groups * (tp - 1))

    def slot_rows(v):
        return pl.ds(pl.multiple_of(v * capacity, capacity), capacity)

    def d1(i):
        v, device = unit_of(i)
        return remote(d1_src.at[slot_rows(v)], d1_dst.at[slot_rows(me)], d1_s.at[v], d1_r.at[me], device)

    for i in range(1, units):
        d1(i).start()
    d1_dst[slot_rows(me), :] = d1_src[slot_rows(me), :]

    def w_send(b, c, to, sem):
        i = b * W_PARTS + c
        return remote(w.at[w_slice(b, c)], w.at[w_slice(b, c)], sem.at[i], w_recv.at[i], to)

    def w_routes(b, c):
        return (
            ((z >= z0 + b) & (z < fsdp - 1), w_send(b, c, (g, z + 1, t), w_up)),
            ((z <= z0 + b) & (z > 0), w_send(b, c, (g, z - 1, t), w_dn)),
        )

    def w_forward(n):
        b, c = near_block(n // W_PARTS), lax.rem(n, W_PARTS)
        w_load(b, c).wait()
        for condition, copy in w_routes(b, c):
            pl.when(condition)(copy.start)
        w_send(b, c, peer, w_dd).start()

    @pl.when(carries & inside)
    def _():
        lax.fori_loop(0, W_PARTS, lambda n, carry: (w_forward(n), carry)[1], 0)

    base = jnp.where(inside, W_PARTS, 0)
    early = 2

    y[...] = jnp.zeros_like(y)
    for s in range(rows // LENGTH):
        span = pl.ds(s * LENGTH, LENGTH)
        for h in range(tp):
            at = pl.ds(h * cols, cols)
            back[span, at] = jnp.where(is_img[span, :] > 0.5, 0.0, rotated_back(s, at)).astype(bf16)
    image_units = lax.broadcasted_iota(jnp.int32, (units, images), 0)
    marks = jnp.where(image_units == owner_ref[...], 1.0, 0.0)
    before = jnp.where(
        lax.broadcasted_iota(jnp.int32, (images, images), 0) < lax.broadcasted_iota(jnp.int32, (images, images), 1),
        1.0,
        0.0,
    ).astype(bf16)
    counts = jnp.dot(marks.astype(bf16), before, preferred_element_type=f32)
    rank = jnp.sum(counts * marks, axis=0, keepdims=True).astype(jnp.int32)
    slots_out = owner_ref[...] * capacity + rank
    pick_t[...] = jnp.where(
        lax.broadcasted_iota(jnp.int32, (slots, images), 0) == slots_out, 1.0, 0.0
    ).astype(bf16)

    for i in range(1, units):
        v, device = unit_of(i)
        remote(d1_src.at[slot_rows(v)], d1_dst.at[slot_rows(v)], d1_s.at[v], d1_r.at[v], device).wait_recv()
    returned = lax.dot_general(pick_t[...], d1_dst[...], ROWS_TO_COLS, preferred_element_type=f32).astype(bf16)
    d2_src[...] = returned
    back[pl.ds(rows, images), my_cols] = returned

    def head_cols(q):
        return pl.ds(pl.multiple_of(q * cols, cols), cols)

    def d2(i, source):
        q, device = head_of(i)
        return remote(d2_src, back.at[pl.ds(rows, images), head_cols(source)], d2_s.at[q], d2_r.at[source], device)

    for i in range(1, tp):
        d2(i, t).start()

    @pl.when(carries & adjacent)
    def _():
        w_forward(base)

    for i in range(1, tp):
        d2(i, head_of(i)[0]).wait_recv()
    for load in loads[3:]:
        load.wait()

    @pl.when(carries & adjacent)
    def _():
        w_forward(base + 1)

    def p_copy(i):
        at = pl.ds(pl.multiple_of(i * g_rows, g_rows), g_rows)
        return remote(pa.at[at], pb.at[at], p_s.at[i], p_r.at[i], peer)

    tile = 4 * g_rows

    def p_step(j, carry):
        at = pl.ds(pl.multiple_of(j * tile, tile), tile)
        part = lax.dot_general(x[:, at], back[...], ROWS_TO_COLS, preferred_element_type=f32)
        pf[at, :] = part

        @pl.when(carries)
        def _():
            pa[at, :] = part.astype(bf16)
            for k in range(tile // g_rows):
                p_copy(j * (tile // g_rows) + k).start()

        return carry

    lax.fori_loop(0, columns // tile, p_step, 0)

    forwarded = jnp.where(adjacent, base + early, 0)

    def w_step(n):
        @pl.when(carries & (n >= forwarded))
        def _():
            w_forward(n)

        b, c = near_block(n // W_PARTS), lax.rem(n, W_PARTS)

        @pl.when(jnp.logical_not(carries))
        def _():
            w_load(b, c).wait()

        at = w_slice(b, c)
        y[...] += jnp.dot(x[:, at], w[at, :], preferred_element_type=f32)

        @pl.when(n == w_steps - 1)
        def _():
            c1_send()

        gout[:, at] = lax.dot_general(back[...], w[at, :], COLS_TO_COLS, preferred_element_type=f32).astype(bf16)
        for copy in grad_stores(n):
            copy.start()

    def grad_stores(n):
        b, c = near_block(n // W_PARTS), lax.rem(n, W_PARTS)
        at = w_slice(b, c)
        return (
            pltpu.make_async_copy(gout.at[pl.ds(0, rows), at], text_out.at[:, at], st.at[n]),
            pltpu.make_async_copy(gout.at[pl.ds(rows, images), at], image_out.at[:, at], st.at[w_steps + n]),
        )

    text_rows, image_rows = pl.ds(0, rows), pl.ds(rows, images)

    def c1(i, source, which, send, recv):
        q, device = head_of(i)
        return remote(yb.at[q, which], yr.at[source, which], send.at[q], recv.at[source], device)

    def c1_send():
        for q in range(tp):
            yb[q] = y[:, q * cols : (q + 1) * cols].astype(bf16)
        for i in range(1, tp):
            c1(i, t, image_rows, ci_s, ci_r).start()
        for i in range(1, tp):
            c1(i, t, text_rows, ct_s, ct_r).start()

    def c2(i):
        v, device = unit_of(i)
        return remote(c2_src.at[slot_rows(v)], c2_dst.at[slot_rows(me)], c2_s.at[v], c2_r.at[me], device)

    def c2_send():
        total = y[image_rows, my_cols]
        for i in range(1, tp):
            q = head_of(i)[0]
            c1(i, q, image_rows, ci_s, ci_r).wait_recv()
            total = total + yr[q, image_rows, :].astype(f32)
        c2_src[...] = jnp.dot(pick_t[...], total.astype(bf16), preferred_element_type=f32).astype(bf16)
        for i in range(1, units):
            c2(i).start()
        c2_dst[slot_rows(me), :] = c2_src[slot_rows(me), :]

    def g_slice(b, c):
        return pl.ds(pl.multiple_of(b * block + c * g_rows, g_rows), g_rows)

    def chain_copies(b, c):
        i, at = b * G_PARTS + c, g_slice(b, c)
        return (
            (z > z0 + b, remote(chain.at[at], above.at[at], ch_s.at[i], ab_r.at[i], (g, z - 1, t))),
            (z < z0 + b, remote(chain.at[at], below.at[at], ch_s.at[i], be_r.at[i], (g, z + 1, t))),
        )

    def landing(c):
        return landed.at[pl.ds(pl.multiple_of(c * g_rows, g_rows), g_rows)]

    def result_copy(b, c, q):
        return remote(
            chain.at[g_slice(b, c), q * cols : (q + 1) * cols], landing(c), g_s.at[c * tp + q], g_r.at[c], (1 - g, z, q)
        )

    def g_step(m):
        b, c = near_block(blocks - 1 - m // G_PARTS), lax.rem(m, G_PARTS)
        i, at, zb = b * G_PARTS + c, g_slice(b, c), z0 + b
        p_copy(i).wait_recv()
        pf[at, :] += pb[at, :].astype(f32)

        @pl.when((z >= zb) & (z < fsdp - 1))
        def _():
            remote(chain.at[at], above.at[at], ch_s.at[i], ab_r.at[i], peer).wait_recv()
            pf[at, :] += above[at, :].astype(f32)

        @pl.when((z <= zb) & (z > 0))
        def _():
            remote(chain.at[at], below.at[at], ch_s.at[i], be_r.at[i], peer).wait_recv()
            pf[at, :] += below[at, :].astype(f32)

        chain[at, :] = pf[at, :].astype(bf16)
        for condition, copy in chain_copies(b, c):
            pl.when(condition)(copy.start)

        @pl.when(z == zb)
        def _():
            for q in range(tp):
                result_copy(b, c, q).start()

    ratio = g_steps // w_steps
    turns = 2 * w_steps
    sums = jnp.logical_not(carries)
    w_at = jnp.where(sums & far_end, w_steps, 0)
    g_at = jnp.where(far_end, 0, jnp.where(inside, w_steps, w_steps // 2 - 1))
    c2_at = jnp.where(sums & inside, w_steps + w_steps // 2, jnp.where(sums & jnp.logical_not(far_end), w_steps + 1, turns - 1))

    def turn(s, carry):
        n, m = s - w_at, s - g_at

        @pl.when(sums & (m >= 0) & (m < w_steps))
        def _():
            lax.fori_loop(0, ratio, lambda k, unused: (g_step(m * ratio + k), unused)[1], 0)

        @pl.when((n >= 0) & (n < w_steps))
        def _():
            w_step(n)

        @pl.when(s == c2_at)
        def _():
            c2_send()

        return carry

    lax.fori_loop(0, turns, turn, 0)

    total = y[text_rows, my_cols]
    for i in range(1, tp):
        q = head_of(i)[0]
        c1(i, q, text_rows, ct_s, ct_r).wait_recv()
        total = total + yr[q, text_rows, :].astype(f32)
    for i in range(1, units):
        v, device = unit_of(i)
        remote(c2_src.at[slot_rows(v)], c2_dst.at[slot_rows(v)], c2_s.at[v], c2_r.at[v], device).wait_recv()
    placed = lax.dot_general(place_t[...], c2_dst[...], ROWS_TO_COLS, preferred_element_type=f32)
    projected = jnp.where(is_img[...] > 0.5, placed, total) + bias_ref[...]
    for s in range(rows // LENGTH):
        values = projected[s * LENGTH : (s + 1) * LENGTH]
        turned = values * cosv[...] + pltpu.roll(values, HALF, 1) * sinv[...]
        keys[s * LENGTH : (s + 1) * LENGTH, :] = jnp.where(live(s), turned, 0.0).astype(bf16)
    keys_store = pltpu.make_async_copy(keys, keys_out, ld.at[0])
    keys_store.start()

    for c in range(G_PARTS):
        remote(landing(c), landing(c), g_s.at[0], g_r.at[c], peer).wait_recv()
    wg[...] = landed[...].astype(f32) * (1.0 / rows)
    wg_store = pltpu.make_async_copy(wg, wgrad_out, ld.at[1])
    wg_store.start()

    def each(count, body):
        lax.fori_loop(0, count, lambda n, unused: (body(n), unused)[1], 0)

    def w_sent(n):
        b, c = n // W_PARTS, lax.rem(n, W_PARTS)
        for condition, copy in w_routes(b, c):
            pl.when(condition)(copy.wait_send)
        w_send(b, c, peer, w_dd).wait_send()

    @pl.when(carries)
    def _():
        each(w_steps, w_sent)
        each(g_steps, lambda n: p_copy(n).wait_send())

    def g_sent(n):
        b, c = n // G_PARTS, lax.rem(n, G_PARTS)
        for condition, copy in chain_copies(b, c):
            pl.when(condition)(copy.wait_send)

        @pl.when(z == z0 + b)
        def _():
            for q in range(tp):
                result_copy(b, c, q).wait_send()

    @pl.when(sums)
    def _():
        each(g_steps, g_sent)

    for i in range(1, units):
        d1(i).wait_send()
        c2(i).wait_send()
    for i in range(1, tp):
        d2(i, t).wait_send()
        c1(i, t, image_rows, ci_s, ci_r).wait_send()
        c1(i, t, text_rows, ct_s, ct_r).wait_send()

    def stored(n):
        for copy in grad_stores(n):
            copy.wait()

    each(w_steps, stored)
    keys_store.wait()
    wg_store.wait()


def rotary_tables():
    frequency = ROPE_BASE ** (-(np.arange(HALF, dtype=np.float64) * 2.0) / HEAD_DIM)
    table = np.arange(LENGTH, dtype=np.float64)[:, None] * frequency[None, :]
    cosine, sine = np.cos(table), np.sin(table)
    return (
        np.concatenate([cosine, cosine], axis=1).astype(np.float32),
        np.concatenate([-sine, sine], axis=1).astype(np.float32),
    )


def fits(groups, fsdp, tp, rows, head_cols, block):
    units = groups * fsdp
    if groups != 2 or units % tp or head_cols != HEAD_DIM or rows % LENGTH:
        return False
    blocks = units // tp
    return blocks == 2 and fsdp % blocks == 0 and block % (G_PARTS * HEAD_DIM) == 0 and (rows // units) % 16 == 0


def per_device(
    text_embeds, image_embeds, key_weight, key_bias, key_cot, image_owner, image_slot, seq_lengths
):
    groups, fsdp, tp = lax.axis_size("group"), lax.axis_size("fsdp"), lax.axis_size("tp")
    rows, columns = text_embeds.shape
    images = image_embeds.shape[0]
    cols = key_bias.shape[0]
    block = key_weight.shape[0]
    if not fits(groups, fsdp, tp, rows, cols, block):
        return per_device_plain(
            text_embeds, image_embeds, key_weight, key_bias, key_cot, image_owner, image_slot, seq_lengths
        )
    units = groups * fsdp
    capacity = rows // units
    slots = units * capacity
    both, key_cols = rows + images, cols * tp
    blocks = units // tp
    w_steps, g_steps = blocks * W_PARTS, blocks * G_PARTS
    cosine, sine = rotary_tables()
    bf16, f32 = jnp.bfloat16, jnp.float32
    hbm = pl.BlockSpec(memory_space=pl.ANY)
    vmem = pl.BlockSpec(memory_space=pltpu.VMEM)
    dma = lambda n: pltpu.SemaphoreType.DMA((n,))
    return pl.pallas_call(
        functools.partial(fused_kernel, groups, fsdp, tp, capacity),
        out_shape=(
            jax.ShapeDtypeStruct((rows, cols), bf16),
            jax.ShapeDtypeStruct((rows, columns), bf16),
            jax.ShapeDtypeStruct((images, columns), bf16),
            jax.ShapeDtypeStruct((block, cols), f32),
        ),
        in_specs=[hbm, hbm, hbm, vmem, hbm, vmem, vmem, vmem, hbm, hbm],
        out_specs=(hbm, hbm, hbm, hbm),
        scratch_shapes=[
            pltpu.VMEM((both, columns), bf16),
            pltpu.VMEM((columns, key_cols), bf16),
            pltpu.VMEM((rows, key_cols), bf16),
            pltpu.VMEM((LENGTH, cols), f32),
            pltpu.VMEM((LENGTH, cols), f32),
            pltpu.VMEM((both, key_cols), bf16),
            pltpu.VMEM((slots, images), bf16),
            pltpu.VMEM((slots, rows), bf16),
            pltpu.VMEM((rows, cols), f32),
            pltpu.VMEM((slots, cols), bf16),
            pltpu.VMEM((slots, cols), bf16),
            pltpu.VMEM((images, cols), bf16),
            pltpu.VMEM((columns, key_cols), f32),
            pltpu.VMEM((columns, key_cols), bf16),
            pltpu.VMEM((columns, key_cols), bf16),
            pltpu.VMEM((columns, key_cols), bf16),
            pltpu.VMEM((columns, key_cols), bf16),
            pltpu.VMEM((columns, key_cols), bf16),
            pltpu.VMEM((both, key_cols), f32),
            pltpu.VMEM((tp, both, cols), bf16),
            pltpu.VMEM((tp, both, cols), bf16),
            pltpu.VMEM((slots, cols), bf16),
            pltpu.VMEM((slots, cols), bf16),
            pltpu.VMEM((both, columns), bf16),
            pltpu.VMEM((block, cols), bf16),
            pltpu.VMEM((block, cols), f32),
            pltpu.VMEM((rows, cols), bf16),
            dma(5), dma(w_steps), dma(w_steps), dma(w_steps), dma(w_steps),
            dma(units), dma(units), dma(tp), dma(tp),
            dma(tp), dma(tp), dma(tp), dma(tp), dma(units), dma(units),
            dma(g_steps), dma(g_steps), dma(g_steps), dma(g_steps), dma(g_steps),
            dma(G_PARTS * tp), dma(G_PARTS), dma(2 * w_steps),
        ],
        compiler_params=pltpu.CompilerParams(
            collective_id=0, has_side_effects=True, vmem_limit_bytes=60 * 1024 * 1024
        ),
        name="fused",
    )(
        text_embeds, image_embeds, key_weight, key_bias.reshape(1, -1), key_cot,
        image_owner.reshape(1, -1), image_slot.reshape(1, -1), seq_lengths.reshape(1, -1), cosine, sine,
    )


def solution(mesh):
    in_specs = (
        P(("group", "fsdp"), "tp"),
        P(("group", "fsdp"), "tp"),
        P(("group", "fsdp"), None),
        P("tp"),
        P(("group", "fsdp"), None),
        P(("group", "fsdp")),
        P(("group", "fsdp")),
        P(("group", "fsdp")),
    )
    out_specs = (
        P(("group", "fsdp"), "tp"),
        P(("group", "fsdp"), "tp"),
        P(("group", "fsdp"), "tp"),
        P(("group", "fsdp"), "tp"),
    )
    return jax.shard_map(
        per_device, mesh=mesh, in_specs=in_specs, out_specs=out_specs, check_vma=False
    )
```

```python
import functools

import jax
import jax.numpy as jnp
import numpy as np
from jax import lax
from jax.experimental import pallas as pl
from jax.experimental.pallas import tpu as pltpu
from jax.sharding import PartitionSpec as P

HEAD_DIM = 128
LENGTH = 256


ROPE_BASE = 1000000.0


def angles(row_total):
    position = (jnp.arange(row_total, dtype=jnp.int32) % LENGTH).astype(jnp.float32)
    frequency = ROPE_BASE ** (-(jnp.arange(HEAD_DIM // 2, dtype=jnp.float32) * 2.0) / HEAD_DIM)
    angle_table = position[:, None] * frequency[None, :]
    return (jnp.cos(angle_table), jnp.sin(angle_table))


def rotate(values, cosine, sine, direction):
    row_total = values.shape[0]
    by_head = values.reshape(row_total, -1, HEAD_DIM)
    half_dim = HEAD_DIM // 2
    front_half = by_head[..., :half_dim]
    second = by_head[..., half_dim:]
    cos_part = cosine[:, None, :]
    sin_part = direction * sine[:, None, :]
    rotated = jnp.concatenate(
        [front_half * cos_part - second * sin_part, second * cos_part + front_half * sin_part],
        axis=-1,
    )
    return rotated.reshape(row_total, -1)


def send_slots(owners, unit_count, capacity):
    onehot_marks = (owners[:, None] == jnp.arange(unit_count, dtype=jnp.int32)[None, :]).astype(
        jnp.int32
    )
    before = jnp.cumsum(onehot_marks, axis=0) - onehot_marks
    owner_rank = jnp.sum(before * onehot_marks, axis=1)
    return owners * capacity + owner_rank


def share_kernel(text_ref, image_ref, back_ref, image_back_ref, out_ref):
    contract = (((0,), (0,)), ((), ()))
    part = lax.dot_general(
        text_ref[...], back_ref[...], contract, preferred_element_type=jnp.float32
    ) + lax.dot_general(
        image_ref[...], image_back_ref[...], contract, preferred_element_type=jnp.float32
    )
    part = part.astype(out_ref.dtype)
    width = out_ref.shape[2]
    for head in range(out_ref.shape[0]):
        out_ref[head] = part[:, head * width : (head + 1) * width]


def weight_shares(text, image, back, image_back, head_cols):
    columns = text.shape[1]
    heads = back.shape[1] // head_cols
    tile = min(512, columns)
    return pl.pallas_call(
        share_kernel,
        grid=(columns // tile,),
        in_specs=[
            pl.BlockSpec((text.shape[0], tile), lambda i: (0, i)),
            pl.BlockSpec((image.shape[0], tile), lambda i: (0, i)),
            pl.BlockSpec(back.shape, lambda i: (0, 0)),
            pl.BlockSpec(image_back.shape, lambda i: (0, 0)),
        ],
        out_specs=pl.BlockSpec((heads, tile, head_cols), lambda i: (0, i, 0)),
        out_shape=jax.ShapeDtypeStruct((heads, columns, head_cols), jnp.bfloat16),
        cost_estimate=pl.CostEstimate(
            flops=2 * (text.size + image.size) * back.shape[1],
            bytes_accessed=2 * (text.size + image.size + columns * back.shape[1]),
            transcendentals=0,
        ),
    )(text, image, back, image_back)


def project_kernel(text_ref, image_ref, weight_ref, out_ref):
    step = pl.program_id(0)
    last = pl.num_programs(0) - 1
    rows = jnp.where(step == last, image_ref[...], text_ref[...])
    part = jnp.dot(rows, weight_ref[...], preferred_element_type=jnp.float32).astype(out_ref.dtype)
    width = out_ref.shape[2]
    for head in range(out_ref.shape[0]):
        out_ref[head] = part[:, head * width : (head + 1) * width]


def projection_parts(text, image, weight, head_cols):
    heads = weight.shape[1] // head_cols
    tile, columns = image.shape
    text_tiles = text.shape[0] // tile
    return pl.pallas_call(
        project_kernel,
        grid=(text_tiles + 1,),
        in_specs=[
            pl.BlockSpec((tile, columns), lambda i: (jnp.minimum(i, text_tiles - 1), 0)),
            pl.BlockSpec((tile, columns), lambda i: (0, 0)),
            pl.BlockSpec(weight.shape, lambda i: (0, 0)),
        ],
        out_specs=pl.BlockSpec((heads, tile, head_cols), lambda i: (0, i, 0)),
        out_shape=jax.ShapeDtypeStruct((heads, text.shape[0] + tile, head_cols), jnp.bfloat16),
        cost_estimate=pl.CostEstimate(
            flops=2 * (text.size + image.size) * weight.shape[1],
            bytes_accessed=2 * (text.size + image.size + weight.size),
            transcendentals=0,
        ),
    )(text, image, weight)


def spread(piece, axis):
    count = lax.axis_size(axis)
    copies = jnp.broadcast_to(piece[None], (count,) + piece.shape)
    got = lax.all_to_all(copies, axis, split_axis=0, concat_axis=0, tiled=True)
    return got.reshape((count * piece.shape[0],) + piece.shape[1:])


def shifted(values, axis, step):
    count = lax.axis_size(axis)
    return lax.ppermute(values, axis, [(i, (i + step) % count) for i in range(count)])


def exchange_sum(blocks, axis):
    count = lax.axis_size(axis)
    me = lax.axis_index(axis)
    total = lax.dynamic_index_in_dim(blocks, me, 0, keepdims=False).astype(jnp.float32)
    for step in range(1, count):
        block = lax.dynamic_index_in_dim(blocks, (me + step) % count, 0, keepdims=False)
        total = total + shifted(block, axis, step).astype(jnp.float32)
    return total


def share_rows(piece, axis):
    count = lax.axis_size(axis)
    me = lax.axis_index(axis)
    rows = piece.shape[0]
    full = jnp.zeros((count * rows,) + piece.shape[1:], piece.dtype)
    full = lax.dynamic_update_slice_in_dim(full, piece, me * rows, 0)
    for step in range(1, count):
        source = (me + count - step) % count
        full = lax.dynamic_update_slice_in_dim(full, shifted(piece, axis, step), source * rows, 0)
    return full


def per_device_plain(
    text_embeds, image_embeds, key_weight, key_bias, key_cot, image_owner, image_slot, seq_lengths
):
    row_count, columns = text_embeds.shape
    image_count = image_embeds.shape[0]
    units = ("group", "fsdp")
    core_count = lax.axis_size("group")
    fsdp_count = lax.axis_size("fsdp")
    tp_count = lax.axis_size("tp")
    unit_count = core_count * fsdp_count
    capacity = row_count // unit_count
    slot_count = unit_count * capacity
    head_cols = key_bias.shape[0]
    key_cols = head_cols * tp_count
    weight_block = key_weight.shape[0]
    halves = unit_count // tp_count
    tp_index = lax.axis_index("tp")

    position = jnp.arange(row_count, dtype=jnp.int32)
    seq_ids = position // LENGTH
    seq_marks = seq_ids[:, None] == jnp.arange(seq_lengths.shape[0], dtype=jnp.int32)[None, :]
    live_limit = jnp.sum(jnp.where(seq_marks, seq_lengths[None, :], 0), axis=1)
    live_mask = (position % LENGTH < live_limit).astype(jnp.float32)
    cosine, sine = angles(row_count)
    masked = key_cot.astype(jnp.float32) * live_mask[:, None]
    rotated_back = rotate(masked, cosine, sine, -1.0).astype(jnp.bfloat16)
    is_image = image_slot >= 0
    text_back = jnp.where(is_image[:, None], jnp.zeros_like(rotated_back), rotated_back)

    slot_ids = jnp.arange(slot_count, dtype=jnp.int32)
    place = (image_slot[:, None] == slot_ids[None, :]).astype(jnp.bfloat16)
    returning = lax.dot_general(
        place, rotated_back, (((0,), (0,)), ((), ())), preferred_element_type=jnp.float32
    ).astype(jnp.bfloat16)
    returned = lax.all_to_all(
        returning.reshape(unit_count, capacity, key_cols), units, split_axis=0, concat_axis=0,
        tiled=True,
    ).reshape(slot_count, key_cols)
    slots_out = send_slots(image_owner, unit_count, capacity)
    pick = (slots_out[:, None] == slot_ids[None, :]).astype(jnp.bfloat16)
    image_back = jnp.dot(pick, returned, preferred_element_type=jnp.float32).astype(jnp.bfloat16)

    piece_rows = weight_block // tp_count
    own_piece = lax.dynamic_slice_in_dim(key_weight, tp_index * piece_rows, piece_rows, 0)
    moves = []
    for unit in range(unit_count):
        for part in range(tp_count):
            target = (unit % halves) * tp_count + part
            moves.append((unit * tp_count + part, target * tp_count + unit // halves))
    own_piece = lax.ppermute(own_piece, units + ("tp",), moves)
    chip_rows = spread(own_piece, "fsdp")

    shares = weight_shares(text_embeds, image_embeds, text_back, image_back, head_cols)
    shares = shares.reshape(core_count, fsdp_count, weight_block, head_cols)
    shares = exchange_sum(shares, "group").astype(jnp.bfloat16)
    shares, chip_rows = lax.optimization_barrier((shares, chip_rows))
    shares = lax.all_to_all(shares, "fsdp", split_axis=0, concat_axis=0, tiled=True)
    weight_grad = jnp.sum(shares.astype(jnp.float32), axis=0) / row_count
    returns = []
    for unit in range(unit_count):
        for part in range(tp_count):
            holder = (unit % halves) + part * halves
            returns.append((holder * tp_count + unit // halves, unit * tp_count + part))
    weight_grad = lax.ppermute(weight_grad, units + ("tp",), returns)

    weight_rows = share_rows(chip_rows, "group")
    both = projection_parts(text_embeds, image_embeds, weight_rows, head_cols)
    both = exchange_sum(both, "tp")
    image_proj = both[row_count:].astype(jnp.bfloat16)
    outgoing = lax.dot_general(
        pick, image_proj, (((0,), (0,)), ((), ())), preferred_element_type=jnp.float32
    ).astype(jnp.bfloat16)
    received = lax.all_to_all(
        outgoing.reshape(unit_count, capacity, head_cols), units, split_axis=0, concat_axis=0,
        tiled=True,
    ).reshape(slot_count, head_cols)
    placed = jnp.dot(place, received, preferred_element_type=jnp.float32)
    projected = jnp.where(is_image[:, None], placed, both[:row_count]) + key_bias
    key_rows = (rotate(projected, cosine, sine, 1.0) * live_mask[:, None]).astype(jnp.bfloat16)

    contract = (((1,), (1,)), ((), ()))
    text_grad = lax.dot_general(
        text_back, weight_rows, contract, preferred_element_type=jnp.float32
    ).astype(jnp.bfloat16)
    image_grad = lax.dot_general(
        image_back, weight_rows, contract, preferred_element_type=jnp.float32
    ).astype(jnp.bfloat16)
    return (key_rows, text_grad, image_grad, weight_grad)


MESH = pl.DeviceIdType.MESH
HALF = HEAD_DIM // 2
ROWS_TO_COLS = (((0,), (0,)), ((), ()))
COLS_TO_COLS = (((1,), (1,)), ((), ()))
W_PARTS = 4
G_PARTS = 8


def fused_kernel(
    groups, fsdp, tp, capacity,
    text_ref, image_ref, weight_ref, bias_hbm, cot_ref, owner_hbm, slot_hbm, lens_hbm, cos_ref, sin_ref,
    keys_out, text_out, image_out, wgrad_out,
    bias_ref, owner_ref, slot_ref, lens_ref, x, w, cot, cosv, sinv, back, pick_t, place_t, is_img,
    d1_src, d1_dst, d2_src, pf, pa, pb, chain, above, below, y, yb, yr, c2_src, c2_dst, landed,
    ld, w_recv, w_up, w_dn, w_dd, d1_s, d1_r, d2_s, d2_r, ci_s, ci_r, ct_s, ct_r, c2_s, c2_r,
    p_s, p_r, ab_r, be_r, ch_s, g_s, g_r,
):
    f32, bf16 = jnp.float32, jnp.bfloat16
    g, z, t = lax.axis_index("group"), lax.axis_index("fsdp"), lax.axis_index("tp")
    units = groups * fsdp
    me = g * fsdp + z
    rows, images = text_ref.shape[0], image_ref.shape[0]
    both = rows + images
    columns = text_ref.shape[1]
    slots = units * capacity
    cols = bias_ref.shape[1]
    block = weight_ref.shape[0]
    blocks = units // tp
    w_rows, g_rows = block // W_PARTS, block // G_PARTS
    w_steps, g_steps = blocks * W_PARTS, blocks * G_PARTS
    first = t * blocks
    carrier, z0 = first // fsdp, lax.rem(first, fsdp)
    carries = g == carrier
    inside = (z >= z0) & (z < z0 + blocks)
    far_end = jnp.logical_not(inside) & ((z == 0) | (z == fsdp - 1))
    adjacent = inside | (z == z0 - 1) | (z == z0 + blocks)
    my_cols = pl.ds(pl.multiple_of(t * cols, cols), cols)
    peer = (1 - g, z, t)

    def near_block(k):
        within = lax.rem(z - z0 + k + blocks, blocks)
        return jnp.where(inside, within, jnp.where(z < z0, k, blocks - 1 - k))

    def unit_of(i):
        v = lax.rem(me + i, units)
        return v, (v // fsdp, lax.rem(v, fsdp), t)

    def head_of(i):
        q = lax.rem(t + i, tp)
        return q, (g, z, q)

    def remote(src, dst, send, recv, device):
        return pltpu.make_async_remote_copy(
            src_ref=src, dst_ref=dst, send_sem=send, recv_sem=recv, device_id=device, device_id_type=MESH
        )

    barrier = pltpu.get_barrier_semaphore()
    for i in range(1, units):
        pl.semaphore_signal(barrier, inc=1, device_id=unit_of(i)[1], device_id_type=MESH)
    for i in range(1, tp):
        q = head_of(i)[0]
        for core in range(groups):
            pl.semaphore_signal(barrier, inc=1, device_id=(core, z, q), device_id_type=MESH)

    pairs = (
        (slot_hbm, slot_ref),
        (cot_ref, cot),
        (cos_ref, cosv),
        (sin_ref, sinv),
        (lens_hbm, lens_ref),
        (owner_hbm, owner_ref),
        (bias_hbm, bias_ref),
        (text_ref, x.at[pl.ds(0, rows)]),
        (image_ref, x.at[pl.ds(rows, images)]),
    )
    loads = [pltpu.make_async_copy(source, target, ld.at[i]) for i, (source, target) in enumerate(pairs)]
    for load in loads[:5]:
        load.start()

    def w_slice(b, c):
        return pl.ds(pl.multiple_of(b * block + c * w_rows, w_rows), w_rows)

    def w_load(b, c):
        return pltpu.make_async_copy(
            weight_ref.at[pl.ds(pl.multiple_of(c * w_rows, w_rows), w_rows)], w.at[w_slice(b, c)], w_recv.at[b * W_PARTS + c]
        )

    @pl.when(carries & inside)
    def _():
        for c in range(W_PARTS):
            w_load(z - z0, c).start()

    for load in loads[5:]:
        load.start()

    loads[0].wait()
    slot_ids = lax.broadcasted_iota(jnp.int32, (slots, rows), 0)
    place_t[...] = jnp.where(slot_ids == slot_ref[...], 1.0, 0.0).astype(bf16)
    is_img[...] = lax.dot_general(
        place_t[...], jnp.ones((slots, cols), bf16), ROWS_TO_COLS, preferred_element_type=f32
    )
    row_ids = lax.broadcasted_iota(jnp.int32, (LENGTH, HEAD_DIM), 0)

    def live(s):
        return row_ids < lens_ref[0:1, s : s + 1]

    def rotated_back(s, at):
        span = pl.ds(s * LENGTH, LENGTH)
        values = jnp.where(live(s), cot[span, at].astype(f32), 0.0)
        return values * cosv[...] - pltpu.roll(values, HALF, 1) * sinv[...]

    for load in loads[1:5]:
        load.wait()
    mine = jnp.concatenate([rotated_back(s, my_cols) for s in range(rows // LENGTH)], axis=0).astype(bf16)
    d1_src[...] = jnp.dot(place_t[...], mine, preferred_element_type=f32).astype(bf16)

    pl.semaphore_wait(barrier, units - 1 + groups * (tp - 1))

    def slot_rows(v):
        return pl.ds(pl.multiple_of(v * capacity, capacity), capacity)

    def d1(i):
        v, device = unit_of(i)
        return remote(d1_src.at[slot_rows(v)], d1_dst.at[slot_rows(me)], d1_s.at[v], d1_r.at[me], device)

    for i in range(1, units):
        d1(i).start()
    d1_dst[slot_rows(me), :] = d1_src[slot_rows(me), :]

    def w_send(b, c, to, sem):
        i = b * W_PARTS + c
        return remote(w.at[w_slice(b, c)], w.at[w_slice(b, c)], sem.at[i], w_recv.at[i], to)

    def w_routes(b, c):
        return (
            ((z >= z0 + b) & (z < fsdp - 1), w_send(b, c, (g, z + 1, t), w_up)),
            ((z <= z0 + b) & (z > 0), w_send(b, c, (g, z - 1, t), w_dn)),
        )

    def w_forward(n):
        b, c = near_block(n // W_PARTS), lax.rem(n, W_PARTS)
        w_load(b, c).wait()
        for condition, copy in w_routes(b, c):
            pl.when(condition)(copy.start)
        w_send(b, c, peer, w_dd).start()

    @pl.when(carries & inside)
    def _():
        lax.fori_loop(0, W_PARTS, lambda n, carry: (w_forward(n), carry)[1], 0)

    base = jnp.where(inside, W_PARTS, 0)
    early = 2

    y[...] = jnp.zeros_like(y)
    for s in range(rows // LENGTH):
        span = pl.ds(s * LENGTH, LENGTH)
        for h in range(tp):
            at = pl.ds(h * cols, cols)
            back[span, at] = jnp.where(is_img[span, :] > 0.5, 0.0, rotated_back(s, at)).astype(bf16)
    loads[5].wait()
    image_units = lax.broadcasted_iota(jnp.int32, (units, images), 0)
    marks = jnp.where(image_units == owner_ref[...], 1.0, 0.0)
    before = jnp.where(
        lax.broadcasted_iota(jnp.int32, (images, images), 0) < lax.broadcasted_iota(jnp.int32, (images, images), 1),
        1.0,
        0.0,
    ).astype(bf16)
    counts = jnp.dot(marks.astype(bf16), before, preferred_element_type=f32)
    rank = jnp.sum(counts * marks, axis=0, keepdims=True).astype(jnp.int32)
    slots_out = owner_ref[...] * capacity + rank
    pick_t[...] = jnp.where(
        lax.broadcasted_iota(jnp.int32, (slots, images), 0) == slots_out, 1.0, 0.0
    ).astype(bf16)

    for i in range(1, units):
        v, device = unit_of(i)
        remote(d1_src.at[slot_rows(v)], d1_dst.at[slot_rows(v)], d1_s.at[v], d1_r.at[v], device).wait_recv()
    returned = lax.dot_general(pick_t[...], d1_dst[...], ROWS_TO_COLS, preferred_element_type=f32).astype(bf16)
    d2_src[...] = returned
    back[pl.ds(rows, images), my_cols] = returned

    def head_cols(q):
        return pl.ds(pl.multiple_of(q * cols, cols), cols)

    def d2(i, source):
        q, device = head_of(i)
        return remote(d2_src, back.at[pl.ds(rows, images), head_cols(source)], d2_s.at[q], d2_r.at[source], device)

    for i in range(1, tp):
        d2(i, t).start()

    @pl.when(carries & adjacent)
    def _():
        w_forward(base)

    for i in range(1, tp):
        d2(i, head_of(i)[0]).wait_recv()
    for load in loads[6:]:
        load.wait()

    @pl.when(carries & adjacent)
    def _():
        w_forward(base + 1)

    def p_copy(i):
        at = pl.ds(pl.multiple_of(i * g_rows, g_rows), g_rows)
        return remote(pa.at[at], pb.at[at], p_s.at[i], p_r.at[i], peer)

    tile = 4 * g_rows

    def p_step(j, carry):
        at = pl.ds(pl.multiple_of(j * tile, tile), tile)
        part = lax.dot_general(x[:, at], back[...], ROWS_TO_COLS, preferred_element_type=f32)
        pf[at, :] = part

        @pl.when(carries)
        def _():
            pa[at, :] = part.astype(bf16)
            for k in range(tile // g_rows):
                p_copy(j * (tile // g_rows) + k).start()

        return carry

    lax.fori_loop(0, columns // tile, p_step, 0)

    forwarded = jnp.where(adjacent, base + early, 0)

    def w_step(n):
        @pl.when(carries & (n >= forwarded))
        def _():
            w_forward(n)

        b, c = near_block(n // W_PARTS), lax.rem(n, W_PARTS)

        @pl.when(jnp.logical_not(carries))
        def _():
            w_load(b, c).wait()

        at = w_slice(b, c)
        y[...] += jnp.dot(x[:, at], w[at, :], preferred_element_type=f32)

        @pl.when(n == w_steps - 1)
        def _():
            c1_send()

        grads = lax.dot_general(back[...], w[at, :], COLS_TO_COLS, preferred_element_type=f32).astype(bf16)
        text_out[:, at] = grads[:rows]
        image_out[:, at] = grads[rows:]

    text_rows, image_rows = pl.ds(0, rows), pl.ds(rows, images)

    def c1(i, source, which, send, recv):
        q, device = head_of(i)
        return remote(yb.at[q, which], yr.at[source, which], send.at[q], recv.at[source], device)

    def c1_send():
        for q in range(tp):
            yb[q] = y[:, q * cols : (q + 1) * cols].astype(bf16)
        for i in range(1, tp):
            c1(i, t, image_rows, ci_s, ci_r).start()
        for i in range(1, tp):
            c1(i, t, text_rows, ct_s, ct_r).start()

    def c2(i):
        v, device = unit_of(i)
        return remote(c2_src.at[slot_rows(v)], c2_dst.at[slot_rows(me)], c2_s.at[v], c2_r.at[me], device)

    def c2_send():
        total = y[image_rows, my_cols]
        for i in range(1, tp):
            q = head_of(i)[0]
            c1(i, q, image_rows, ci_s, ci_r).wait_recv()
            total = total + yr[q, image_rows, :].astype(f32)
        c2_src[...] = jnp.dot(pick_t[...], total.astype(bf16), preferred_element_type=f32).astype(bf16)
        for i in range(1, units):
            c2(i).start()
        c2_dst[slot_rows(me), :] = c2_src[slot_rows(me), :]

    def g_slice(b, c):
        return pl.ds(pl.multiple_of(b * block + c * g_rows, g_rows), g_rows)

    def chain_copies(b, c):
        i, at = b * G_PARTS + c, g_slice(b, c)
        return (
            (z > z0 + b, remote(chain.at[at], above.at[at], ch_s.at[i], ab_r.at[i], (g, z - 1, t))),
            (z < z0 + b, remote(chain.at[at], below.at[at], ch_s.at[i], be_r.at[i], (g, z + 1, t))),
        )

    def landing(c):
        return landed.at[pl.ds(pl.multiple_of(c * g_rows, g_rows), g_rows)]

    def result_copy(b, c, q):
        return remote(
            chain.at[g_slice(b, c), q * cols : (q + 1) * cols], landing(c), g_s.at[c * tp + q], g_r.at[c], (1 - g, z, q)
        )

    def g_step(m):
        b, c = near_block(blocks - 1 - m // G_PARTS), lax.rem(m, G_PARTS)
        i, at, zb = b * G_PARTS + c, g_slice(b, c), z0 + b
        p_copy(i).wait_recv()
        pf[at, :] += pb[at, :].astype(f32)

        @pl.when((z >= zb) & (z < fsdp - 1))
        def _():
            remote(chain.at[at], above.at[at], ch_s.at[i], ab_r.at[i], peer).wait_recv()
            pf[at, :] += above[at, :].astype(f32)

        @pl.when((z <= zb) & (z > 0))
        def _():
            remote(chain.at[at], below.at[at], ch_s.at[i], be_r.at[i], peer).wait_recv()
            pf[at, :] += below[at, :].astype(f32)

        chain[at, :] = pf[at, :].astype(bf16)
        for condition, copy in chain_copies(b, c):
            pl.when(condition)(copy.start)

        @pl.when(z == zb)
        def _():
            for q in range(tp):
                result_copy(b, c, q).start()

    ratio = g_steps // w_steps
    turns = 2 * w_steps
    sums = jnp.logical_not(carries)
    w_at = jnp.where(sums & far_end, w_steps, 0)
    g_at = jnp.where(far_end, 0, jnp.where(inside, w_steps, w_steps // 2 - 1))
    c2_at = jnp.where(sums & inside, w_steps + w_steps // 2, jnp.where(sums & jnp.logical_not(far_end), w_steps + 1, turns - 1))

    def turn(s, carry):
        n, m = s - w_at, s - g_at

        @pl.when(sums & (m >= 0) & (m < w_steps))
        def _():
            lax.fori_loop(0, ratio, lambda k, unused: (g_step(m * ratio + k), unused)[1], 0)

        @pl.when((n >= 0) & (n < w_steps))
        def _():
            w_step(n)

        @pl.when(s == c2_at)
        def _():
            c2_send()

        return carry

    lax.fori_loop(0, turns, turn, 0)

    total = y[text_rows, my_cols]
    for i in range(1, tp):
        q = head_of(i)[0]
        c1(i, q, text_rows, ct_s, ct_r).wait_recv()
        total = total + yr[q, text_rows, :].astype(f32)
    for i in range(1, units):
        v, device = unit_of(i)
        remote(c2_src.at[slot_rows(v)], c2_dst.at[slot_rows(v)], c2_s.at[v], c2_r.at[v], device).wait_recv()
    placed = lax.dot_general(place_t[...], c2_dst[...], ROWS_TO_COLS, preferred_element_type=f32)
    projected = jnp.where(is_img[...] > 0.5, placed, total) + bias_ref[...]
    for s in range(rows // LENGTH):
        values = projected[s * LENGTH : (s + 1) * LENGTH]
        turned = values * cosv[...] + pltpu.roll(values, HALF, 1) * sinv[...]
        keys_out[s * LENGTH : (s + 1) * LENGTH, :] = jnp.where(live(s), turned, 0.0).astype(bf16)

    for c in range(G_PARTS):
        remote(landing(c), landing(c), g_s.at[0], g_r.at[c], peer).wait_recv()
    wgrad_out[...] = landed[...].astype(f32) * (1.0 / rows)

    def each(count, body):
        lax.fori_loop(0, count, lambda n, unused: (body(n), unused)[1], 0)

    def w_sent(n):
        b, c = n // W_PARTS, lax.rem(n, W_PARTS)
        for condition, copy in w_routes(b, c):
            pl.when(condition)(copy.wait_send)
        w_send(b, c, peer, w_dd).wait_send()

    @pl.when(carries)
    def _():
        each(w_steps, w_sent)
        each(g_steps, lambda n: p_copy(n).wait_send())

    def g_sent(n):
        b, c = n // G_PARTS, lax.rem(n, G_PARTS)
        for condition, copy in chain_copies(b, c):
            pl.when(condition)(copy.wait_send)

        @pl.when(z == z0 + b)
        def _():
            for q in range(tp):
                result_copy(b, c, q).wait_send()

    @pl.when(sums)
    def _():
        each(g_steps, g_sent)

    for i in range(1, units):
        d1(i).wait_send()
        c2(i).wait_send()
    for i in range(1, tp):
        d2(i, t).wait_send()
        c1(i, t, image_rows, ci_s, ci_r).wait_send()
        c1(i, t, text_rows, ct_s, ct_r).wait_send()


def write_kernel(*refs):
    count = (len(refs) - 1) // 2
    copies = [pltpu.make_async_copy(refs[i], refs[count + i], refs[-1].at[i]) for i in range(count)]
    for copy in copies:
        copy.start()
    for copy in copies:
        copy.wait()


def rotary_tables():
    frequency = ROPE_BASE ** (-(np.arange(HALF, dtype=np.float64) * 2.0) / HEAD_DIM)
    table = np.arange(LENGTH, dtype=np.float64)[:, None] * frequency[None, :]
    cosine, sine = np.cos(table), np.sin(table)
    return (
        np.concatenate([cosine, cosine], axis=1).astype(np.float32),
        np.concatenate([-sine, sine], axis=1).astype(np.float32),
    )


def fits(groups, fsdp, tp, rows, head_cols, block):
    units = groups * fsdp
    if groups != 2 or units % tp or head_cols != HEAD_DIM or rows % LENGTH:
        return False
    blocks = units // tp
    return blocks == 2 and fsdp % blocks == 0 and block % (G_PARTS * HEAD_DIM) == 0 and (rows // units) % 16 == 0


def per_device(
    text_embeds, image_embeds, key_weight, key_bias, key_cot, image_owner, image_slot, seq_lengths
):
    groups, fsdp, tp = lax.axis_size("group"), lax.axis_size("fsdp"), lax.axis_size("tp")
    rows, columns = text_embeds.shape
    images = image_embeds.shape[0]
    cols = key_bias.shape[0]
    block = key_weight.shape[0]
    if not fits(groups, fsdp, tp, rows, cols, block):
        return per_device_plain(
            text_embeds, image_embeds, key_weight, key_bias, key_cot, image_owner, image_slot, seq_lengths
        )
    units = groups * fsdp
    capacity = rows // units
    slots = units * capacity
    both, key_cols = rows + images, cols * tp
    blocks = units // tp
    w_steps, g_steps = blocks * W_PARTS, blocks * G_PARTS
    cosine, sine = rotary_tables()
    bf16, f32 = jnp.bfloat16, jnp.float32
    hbm = pl.BlockSpec(memory_space=pltpu.HBM)
    vmem = pl.BlockSpec(memory_space=pltpu.VMEM)
    dma = lambda n: pltpu.SemaphoreType.DMA((n,))
    shapes = (
        jax.ShapeDtypeStruct((rows, cols), bf16),
        jax.ShapeDtypeStruct((rows, columns), bf16),
        jax.ShapeDtypeStruct((images, columns), bf16),
        jax.ShapeDtypeStruct((block, cols), f32),
    )
    operands = (
        text_embeds, image_embeds, key_weight, key_bias.reshape(1, -1), key_cot,
        image_owner.reshape(1, -1), image_slot.reshape(1, -1), seq_lengths.reshape(1, -1), jnp.asarray(cosine), jnp.asarray(sine),
    )
    held = pl.pallas_call(
        functools.partial(fused_kernel, groups, fsdp, tp, capacity),
        out_shape=tuple(pltpu.VMEM(leaf.shape, leaf.dtype) for leaf in shapes),
        in_specs=[hbm] * 10,
        out_specs=(vmem, vmem, vmem, vmem),
        scratch_shapes=[
            pltpu.VMEM((1, cols), f32),
            pltpu.VMEM((1, images), jnp.int32),
            pltpu.VMEM((1, rows), jnp.int32),
            pltpu.VMEM((1, seq_lengths.shape[0]), jnp.int32),
            pltpu.VMEM((both, columns), bf16),
            pltpu.VMEM((columns, key_cols), bf16),
            pltpu.VMEM((rows, key_cols), bf16),
            pltpu.VMEM((LENGTH, cols), f32),
            pltpu.VMEM((LENGTH, cols), f32),
            pltpu.VMEM((both, key_cols), bf16),
            pltpu.VMEM((slots, images), bf16),
            pltpu.VMEM((slots, rows), bf16),
            pltpu.VMEM((rows, cols), f32),
            pltpu.VMEM((slots, cols), bf16),
            pltpu.VMEM((slots, cols), bf16),
            pltpu.VMEM((images, cols), bf16),
            pltpu.VMEM((columns, key_cols), f32),
            pltpu.VMEM((columns, key_cols), bf16),
            pltpu.VMEM((columns, key_cols), bf16),
            pltpu.VMEM((columns, key_cols), bf16),
            pltpu.VMEM((columns, key_cols), bf16),
            pltpu.VMEM((columns, key_cols), bf16),
            pltpu.VMEM((both, key_cols), f32),
            pltpu.VMEM((tp, both, cols), bf16),
            pltpu.VMEM((tp, both, cols), bf16),
            pltpu.VMEM((slots, cols), bf16),
            pltpu.VMEM((slots, cols), bf16),
            pltpu.VMEM((block, cols), bf16),
            dma(9), dma(w_steps), dma(w_steps), dma(w_steps), dma(w_steps),
            dma(units), dma(units), dma(tp), dma(tp),
            dma(tp), dma(tp), dma(tp), dma(tp), dma(units), dma(units),
            dma(g_steps), dma(g_steps), dma(g_steps), dma(g_steps), dma(g_steps),
            dma(G_PARTS * tp), dma(G_PARTS),
        ],
        compiler_params=pltpu.CompilerParams(
            collective_id=0, has_side_effects=True, vmem_limit_bytes=44 * 1024 * 1024
        ),
        name="fused",
    )(*(pltpu.with_memory_space_constraint(operand, pltpu.HBM) for operand in operands))
    return pl.pallas_call(
        write_kernel,
        out_shape=shapes,
        in_specs=[vmem] * 4,
        out_specs=(pl.BlockSpec(memory_space=pl.ANY),) * 4,
        scratch_shapes=[dma(4)],
        compiler_params=pltpu.CompilerParams(vmem_limit_bytes=4 * 1024 * 1024),
        name="write",
    )(*held)


def solution(mesh):
    in_specs = (
        P(("group", "fsdp"), "tp"),
        P(("group", "fsdp"), "tp"),
        P(("group", "fsdp"), None),
        P("tp"),
        P(("group", "fsdp"), None),
        P(("group", "fsdp")),
        P(("group", "fsdp")),
        P(("group", "fsdp")),
    )
    out_specs = (
        P(("group", "fsdp"), "tp"),
        P(("group", "fsdp"), "tp"),
        P(("group", "fsdp"), "tp"),
        P(("group", "fsdp"), "tp"),
    )
    return jax.shard_map(
        per_device, mesh=mesh, in_specs=in_specs, out_specs=out_specs, check_vma=False
    )
```

```python
import functools

import jax
import jax.numpy as jnp
import numpy as np
from jax import lax
from jax.experimental import pallas as pl
from jax.experimental.pallas import tpu as pltpu
from jax.sharding import PartitionSpec as P

HEAD_DIM = 128
LENGTH = 256


ROPE_BASE = 1000000.0


def angles(row_total):
    position = (jnp.arange(row_total, dtype=jnp.int32) % LENGTH).astype(jnp.float32)
    frequency = ROPE_BASE ** (-(jnp.arange(HEAD_DIM // 2, dtype=jnp.float32) * 2.0) / HEAD_DIM)
    angle_table = position[:, None] * frequency[None, :]
    return (jnp.cos(angle_table), jnp.sin(angle_table))


def rotate(values, cosine, sine, direction):
    row_total = values.shape[0]
    by_head = values.reshape(row_total, -1, HEAD_DIM)
    half_dim = HEAD_DIM // 2
    front_half = by_head[..., :half_dim]
    second = by_head[..., half_dim:]
    cos_part = cosine[:, None, :]
    sin_part = direction * sine[:, None, :]
    rotated = jnp.concatenate(
        [front_half * cos_part - second * sin_part, second * cos_part + front_half * sin_part],
        axis=-1,
    )
    return rotated.reshape(row_total, -1)


def send_slots(owners, unit_count, capacity):
    onehot_marks = (owners[:, None] == jnp.arange(unit_count, dtype=jnp.int32)[None, :]).astype(
        jnp.int32
    )
    before = jnp.cumsum(onehot_marks, axis=0) - onehot_marks
    owner_rank = jnp.sum(before * onehot_marks, axis=1)
    return owners * capacity + owner_rank


def share_kernel(text_ref, image_ref, back_ref, image_back_ref, out_ref):
    contract = (((0,), (0,)), ((), ()))
    part = lax.dot_general(
        text_ref[...], back_ref[...], contract, preferred_element_type=jnp.float32
    ) + lax.dot_general(
        image_ref[...], image_back_ref[...], contract, preferred_element_type=jnp.float32
    )
    part = part.astype(out_ref.dtype)
    width = out_ref.shape[2]
    for head in range(out_ref.shape[0]):
        out_ref[head] = part[:, head * width : (head + 1) * width]


def weight_shares(text, image, back, image_back, head_cols):
    columns = text.shape[1]
    heads = back.shape[1] // head_cols
    tile = min(512, columns)
    return pl.pallas_call(
        share_kernel,
        grid=(columns // tile,),
        in_specs=[
            pl.BlockSpec((text.shape[0], tile), lambda i: (0, i)),
            pl.BlockSpec((image.shape[0], tile), lambda i: (0, i)),
            pl.BlockSpec(back.shape, lambda i: (0, 0)),
            pl.BlockSpec(image_back.shape, lambda i: (0, 0)),
        ],
        out_specs=pl.BlockSpec((heads, tile, head_cols), lambda i: (0, i, 0)),
        out_shape=jax.ShapeDtypeStruct((heads, columns, head_cols), jnp.bfloat16),
        cost_estimate=pl.CostEstimate(
            flops=2 * (text.size + image.size) * back.shape[1],
            bytes_accessed=2 * (text.size + image.size + columns * back.shape[1]),
            transcendentals=0,
        ),
    )(text, image, back, image_back)


def project_kernel(text_ref, image_ref, weight_ref, out_ref):
    step = pl.program_id(0)
    last = pl.num_programs(0) - 1
    rows = jnp.where(step == last, image_ref[...], text_ref[...])
    part = jnp.dot(rows, weight_ref[...], preferred_element_type=jnp.float32).astype(out_ref.dtype)
    width = out_ref.shape[2]
    for head in range(out_ref.shape[0]):
        out_ref[head] = part[:, head * width : (head + 1) * width]


def projection_parts(text, image, weight, head_cols):
    heads = weight.shape[1] // head_cols
    tile, columns = image.shape
    text_tiles = text.shape[0] // tile
    return pl.pallas_call(
        project_kernel,
        grid=(text_tiles + 1,),
        in_specs=[
            pl.BlockSpec((tile, columns), lambda i: (jnp.minimum(i, text_tiles - 1), 0)),
            pl.BlockSpec((tile, columns), lambda i: (0, 0)),
            pl.BlockSpec(weight.shape, lambda i: (0, 0)),
        ],
        out_specs=pl.BlockSpec((heads, tile, head_cols), lambda i: (0, i, 0)),
        out_shape=jax.ShapeDtypeStruct((heads, text.shape[0] + tile, head_cols), jnp.bfloat16),
        cost_estimate=pl.CostEstimate(
            flops=2 * (text.size + image.size) * weight.shape[1],
            bytes_accessed=2 * (text.size + image.size + weight.size),
            transcendentals=0,
        ),
    )(text, image, weight)


def spread(piece, axis):
    count = lax.axis_size(axis)
    copies = jnp.broadcast_to(piece[None], (count,) + piece.shape)
    got = lax.all_to_all(copies, axis, split_axis=0, concat_axis=0, tiled=True)
    return got.reshape((count * piece.shape[0],) + piece.shape[1:])


def shifted(values, axis, step):
    count = lax.axis_size(axis)
    return lax.ppermute(values, axis, [(i, (i + step) % count) for i in range(count)])


def exchange_sum(blocks, axis):
    count = lax.axis_size(axis)
    me = lax.axis_index(axis)
    total = lax.dynamic_index_in_dim(blocks, me, 0, keepdims=False).astype(jnp.float32)
    for step in range(1, count):
        block = lax.dynamic_index_in_dim(blocks, (me + step) % count, 0, keepdims=False)
        total = total + shifted(block, axis, step).astype(jnp.float32)
    return total


def share_rows(piece, axis):
    count = lax.axis_size(axis)
    me = lax.axis_index(axis)
    rows = piece.shape[0]
    full = jnp.zeros((count * rows,) + piece.shape[1:], piece.dtype)
    full = lax.dynamic_update_slice_in_dim(full, piece, me * rows, 0)
    for step in range(1, count):
        source = (me + count - step) % count
        full = lax.dynamic_update_slice_in_dim(full, shifted(piece, axis, step), source * rows, 0)
    return full


def per_device_plain(
    text_embeds, image_embeds, key_weight, key_bias, key_cot, image_owner, image_slot, seq_lengths
):
    row_count, columns = text_embeds.shape
    image_count = image_embeds.shape[0]
    units = ("group", "fsdp")
    core_count = lax.axis_size("group")
    fsdp_count = lax.axis_size("fsdp")
    tp_count = lax.axis_size("tp")
    unit_count = core_count * fsdp_count
    capacity = row_count // unit_count
    slot_count = unit_count * capacity
    head_cols = key_bias.shape[0]
    key_cols = head_cols * tp_count
    weight_block = key_weight.shape[0]
    halves = unit_count // tp_count
    tp_index = lax.axis_index("tp")

    position = jnp.arange(row_count, dtype=jnp.int32)
    seq_ids = position // LENGTH
    seq_marks = seq_ids[:, None] == jnp.arange(seq_lengths.shape[0], dtype=jnp.int32)[None, :]
    live_limit = jnp.sum(jnp.where(seq_marks, seq_lengths[None, :], 0), axis=1)
    live_mask = (position % LENGTH < live_limit).astype(jnp.float32)
    cosine, sine = angles(row_count)
    masked = key_cot.astype(jnp.float32) * live_mask[:, None]
    rotated_back = rotate(masked, cosine, sine, -1.0).astype(jnp.bfloat16)
    is_image = image_slot >= 0
    text_back = jnp.where(is_image[:, None], jnp.zeros_like(rotated_back), rotated_back)

    slot_ids = jnp.arange(slot_count, dtype=jnp.int32)
    place = (image_slot[:, None] == slot_ids[None, :]).astype(jnp.bfloat16)
    returning = lax.dot_general(
        place, rotated_back, (((0,), (0,)), ((), ())), preferred_element_type=jnp.float32
    ).astype(jnp.bfloat16)
    returned = lax.all_to_all(
        returning.reshape(unit_count, capacity, key_cols), units, split_axis=0, concat_axis=0,
        tiled=True,
    ).reshape(slot_count, key_cols)
    slots_out = send_slots(image_owner, unit_count, capacity)
    pick = (slots_out[:, None] == slot_ids[None, :]).astype(jnp.bfloat16)
    image_back = jnp.dot(pick, returned, preferred_element_type=jnp.float32).astype(jnp.bfloat16)

    piece_rows = weight_block // tp_count
    own_piece = lax.dynamic_slice_in_dim(key_weight, tp_index * piece_rows, piece_rows, 0)
    moves = []
    for unit in range(unit_count):
        for part in range(tp_count):
            target = (unit % halves) * tp_count + part
            moves.append((unit * tp_count + part, target * tp_count + unit // halves))
    own_piece = lax.ppermute(own_piece, units + ("tp",), moves)
    chip_rows = spread(own_piece, "fsdp")

    shares = weight_shares(text_embeds, image_embeds, text_back, image_back, head_cols)
    shares = shares.reshape(core_count, fsdp_count, weight_block, head_cols)
    shares = exchange_sum(shares, "group").astype(jnp.bfloat16)
    shares, chip_rows = lax.optimization_barrier((shares, chip_rows))
    shares = lax.all_to_all(shares, "fsdp", split_axis=0, concat_axis=0, tiled=True)
    weight_grad = jnp.sum(shares.astype(jnp.float32), axis=0) / row_count
    returns = []
    for unit in range(unit_count):
        for part in range(tp_count):
            holder = (unit % halves) + part * halves
            returns.append((holder * tp_count + unit // halves, unit * tp_count + part))
    weight_grad = lax.ppermute(weight_grad, units + ("tp",), returns)

    weight_rows = share_rows(chip_rows, "group")
    both = projection_parts(text_embeds, image_embeds, weight_rows, head_cols)
    both = exchange_sum(both, "tp")
    image_proj = both[row_count:].astype(jnp.bfloat16)
    outgoing = lax.dot_general(
        pick, image_proj, (((0,), (0,)), ((), ())), preferred_element_type=jnp.float32
    ).astype(jnp.bfloat16)
    received = lax.all_to_all(
        outgoing.reshape(unit_count, capacity, head_cols), units, split_axis=0, concat_axis=0,
        tiled=True,
    ).reshape(slot_count, head_cols)
    placed = jnp.dot(place, received, preferred_element_type=jnp.float32)
    projected = jnp.where(is_image[:, None], placed, both[:row_count]) + key_bias
    key_rows = (rotate(projected, cosine, sine, 1.0) * live_mask[:, None]).astype(jnp.bfloat16)

    contract = (((1,), (1,)), ((), ()))
    text_grad = lax.dot_general(
        text_back, weight_rows, contract, preferred_element_type=jnp.float32
    ).astype(jnp.bfloat16)
    image_grad = lax.dot_general(
        image_back, weight_rows, contract, preferred_element_type=jnp.float32
    ).astype(jnp.bfloat16)
    return (key_rows, text_grad, image_grad, weight_grad)


MESH = pl.DeviceIdType.MESH
HALF = HEAD_DIM // 2
ROWS_TO_COLS = (((0,), (0,)), ((), ()))
COLS_TO_COLS = (((1,), (1,)), ((), ()))
W_PARTS = 4
W_MAIN = 3
G_PARTS = 8
G_MAIN = 6


def fused_kernel(
    groups, fsdp, tp, capacity,
    text_ref, image_ref, weight_ref, bias_hbm, cot_ref, owner_hbm, slot_hbm, lens_hbm, cos_ref, sin_ref,
    keys_out, text_out, image_out, wgrad_out,
    bias_ref, owner_ref, slot_ref, lens_ref, x, w, cot, cosv, sinv, back, pick_t, place_t, is_img,
    d1_src, d1_dst, d2_src, pf, pa, pb, chain, above, below, y, yb, yr, c2_src, c2_dst, landed, side,
    ld, w_recv, w_up, w_dn, w_dd, d1_s, d1_r, d2_s, d2_r, ci_s, ci_r, ct_s, ct_r, c2_s, c2_r,
    p_s, p_r, ab_r, be_r, ch_s, g_s, g_r, x_s, x_r, h_r, h_z, h_x,
):
    f32, bf16 = jnp.float32, jnp.bfloat16
    g, z, t = lax.axis_index("group"), lax.axis_index("fsdp"), lax.axis_index("tp")
    units = groups * fsdp
    me = g * fsdp + z
    rows, images = text_ref.shape[0], image_ref.shape[0]
    both = rows + images
    columns = text_ref.shape[1]
    slots = units * capacity
    cols = bias_ref.shape[1]
    block = weight_ref.shape[0]
    blocks = units // tp
    w_rows, g_rows = block // W_PARTS, block // G_PARTS
    w_steps, g_steps = blocks * W_PARTS, blocks * G_PARTS
    first = t * blocks
    carrier, z0 = first // fsdp, lax.rem(first, fsdp)
    carries = g == carrier
    inside = (z >= z0) & (z < z0 + blocks)
    far_end = jnp.logical_not(inside) & ((z == 0) | (z == fsdp - 1))
    adjacent = inside | (z == z0 - 1) | (z == z0 + blocks)
    my_cols = pl.ds(pl.multiple_of(t * cols, cols), cols)
    peer = (1 - g, z, t)
    other = lax.bitwise_xor(t, 1)
    beside = (g, z, other)
    other_z0 = fsdp - blocks - z0
    upward = z0 > 0
    entry = jnp.where(upward, z == z0, z == z0 + blocks - 1)
    border = jnp.where(upward, z == z0 - 1, z == z0 + blocks)

    def near_block(k):
        within = lax.rem(z - z0 + k + blocks, blocks)
        return jnp.where(inside, within, jnp.where(z < z0, k, blocks - 1 - k))

    def far_other(k):
        within = lax.rem(z - other_z0 + blocks - 1 - k + blocks, blocks)
        return jnp.where(inside, jnp.where(upward, k, blocks - 1 - k), within)

    def w_part(n):
        late = n >= blocks * W_MAIN
        k = jnp.where(late, n - blocks * W_MAIN, n // W_MAIN)
        return near_block(k), jnp.where(late, W_MAIN, lax.rem(n, W_MAIN))

    def unit_of(i):
        v = lax.rem(me + i, units)
        return v, (v // fsdp, lax.rem(v, fsdp), t)

    def head_of(i):
        q = lax.rem(t + i, tp)
        return q, (g, z, q)

    def remote(src, dst, send, recv, device):
        return pltpu.make_async_remote_copy(
            src_ref=src, dst_ref=dst, send_sem=send, recv_sem=recv, device_id=device, device_id_type=MESH
        )

    barrier = pltpu.get_barrier_semaphore()
    for i in range(1, units):
        pl.semaphore_signal(barrier, inc=1, device_id=unit_of(i)[1], device_id_type=MESH)
    for i in range(1, tp):
        q = head_of(i)[0]
        for core in range(groups):
            pl.semaphore_signal(barrier, inc=1, device_id=(core, z, q), device_id_type=MESH)

    pairs = (
        (slot_hbm, slot_ref),
        (cot_ref, cot),
        (cos_ref, cosv),
        (sin_ref, sinv),
        (lens_hbm, lens_ref),
        (owner_hbm, owner_ref),
        (bias_hbm, bias_ref),
        (text_ref, x.at[pl.ds(0, rows)]),
        (image_ref, x.at[pl.ds(rows, images)]),
    )
    loads = [pltpu.make_async_copy(source, target, ld.at[i]) for i, (source, target) in enumerate(pairs)]
    for load in loads[:5]:
        load.start()

    def w_slice(b, c):
        return pl.ds(pl.multiple_of(b * block + c * w_rows, w_rows), w_rows)

    def w_load(b, c):
        return pltpu.make_async_copy(
            weight_ref.at[pl.ds(pl.multiple_of(c * w_rows, w_rows), w_rows)], w.at[w_slice(b, c)], w_recv.at[b * W_PARTS + c]
        )

    @pl.when(carries & inside)
    def _():
        for c in range(W_PARTS):
            w_load(z - z0, c).start()

    def side_load(b):
        return pltpu.make_async_copy(weight_ref.at[pl.ds(W_MAIN * w_rows, w_rows)], side.at[b], h_r.at[b])

    @pl.when(carries & jnp.logical_not(inside))
    def _():
        side_load(z - other_z0).start()

    for load in loads[5:]:
        load.start()

    loads[0].wait()
    slot_ids = lax.broadcasted_iota(jnp.int32, (slots, rows), 0)
    place_t[...] = jnp.where(slot_ids == slot_ref[...], 1.0, 0.0).astype(bf16)
    is_img[...] = lax.dot_general(
        place_t[...], jnp.ones((slots, cols), bf16), ROWS_TO_COLS, preferred_element_type=f32
    )
    row_ids = lax.broadcasted_iota(jnp.int32, (LENGTH, HEAD_DIM), 0)

    def live(s):
        return row_ids < lens_ref[0:1, s : s + 1]

    def rotated_back(s, at):
        span = pl.ds(s * LENGTH, LENGTH)
        values = jnp.where(live(s), cot[span, at].astype(f32), 0.0)
        return values * cosv[...] - pltpu.roll(values, HALF, 1) * sinv[...]

    for load in loads[1:5]:
        load.wait()
    mine = jnp.concatenate([rotated_back(s, my_cols) for s in range(rows // LENGTH)], axis=0).astype(bf16)
    d1_src[...] = jnp.dot(place_t[...], mine, preferred_element_type=f32).astype(bf16)

    pl.semaphore_wait(barrier, units - 1 + groups * (tp - 1))

    def slot_rows(v):
        return pl.ds(pl.multiple_of(v * capacity, capacity), capacity)

    def d1(i):
        v, device = unit_of(i)
        return remote(d1_src.at[slot_rows(v)], d1_dst.at[slot_rows(me)], d1_s, d1_r, device)

    def d1_all():
        at = pl.ds(0, (units - 1) * capacity)
        return remote(d1_src.at[at], d1_dst.at[at], d1_s, d1_r, peer)

    for i in range(1, units):
        d1(i).start()
    d1_dst[slot_rows(me), :] = d1_src[slot_rows(me), :]

    def w_send(b, c, to, sem):
        i = b * W_PARTS + c
        return remote(w.at[w_slice(b, c)], w.at[w_slice(b, c)], sem.at[i], w_recv.at[i], to)

    def w_share(b, c):
        return remote(w.at[w_slice(b, c)], w.at[w_slice(b, c)], w_dd, w_recv.at[b * W_PARTS + c], peer)

    def w_routes(b, c):
        return (
            ((z >= z0 + b) & (z < fsdp - 1) & ((c < W_MAIN) | (z + 1 < z0 + blocks)), w_send(b, c, (g, z + 1, t), w_up)),
            ((z <= z0 + b) & (z > 0) & ((c < W_MAIN) | (z > z0)), w_send(b, c, (g, z - 1, t), w_dn)),
        )

    def w_inward(c):
        b = z - z0
        return (
            (upward, w_send(b, c, (g, z + 1, t), w_up)),
            (jnp.logical_not(upward), w_send(b, c, (g, z - 1, t), w_dn)),
        )

    def side_routes(b):
        step = jnp.where(upward, 1, -1)
        at = w_slice(b, W_MAIN)
        return (
            ((z + step >= 0) & (z + step < fsdp), remote(side.at[b], side.at[b], h_z.at[b], h_r.at[b], (g, z + step, t))),
            (inside, remote(side.at[b], w.at[at], h_x.at[b], w_recv.at[b * W_PARTS + W_MAIN], beside)),
        )

    def side_forward(b):
        side_load(b).wait()
        for condition, copy in side_routes(b):
            pl.when(condition)(copy.start)

    def side_block(k):
        return jnp.where(upward, blocks - 1 - k, k)

    def w_forward(b, c):
        w_load(b, c).wait()
        held = entry & (z == z0 + b) & (c >= 2)
        for (condition, copy), inward in zip(w_routes(b, c), (upward, jnp.logical_not(upward))):
            pl.when(condition & jnp.logical_not(held & inward))(copy.start)
        w_share(b, c).start()

    @pl.when(carries & inside)
    def _():
        lax.fori_loop(0, W_PARTS, lambda c, carry: (w_forward(z - z0, c), carry)[1], 0)

    @pl.when(carries & jnp.logical_not(inside))
    def _():
        side_forward(z - other_z0)

    base = jnp.where(inside, W_MAIN, 0)

    y[...] = jnp.zeros_like(y)
    for s in range(rows // LENGTH):
        span = pl.ds(s * LENGTH, LENGTH)
        for h in range(tp):
            at = pl.ds(h * cols, cols)
            back[span, at] = jnp.where(is_img[span, :] > 0.5, 0.0, rotated_back(s, at)).astype(bf16)
    loads[5].wait()
    image_units = lax.broadcasted_iota(jnp.int32, (units, images), 0)
    marks = jnp.where(image_units == owner_ref[...], 1.0, 0.0)
    before = jnp.where(
        lax.broadcasted_iota(jnp.int32, (images, images), 0) < lax.broadcasted_iota(jnp.int32, (images, images), 1),
        1.0,
        0.0,
    ).astype(bf16)
    counts = jnp.dot(marks.astype(bf16), before, preferred_element_type=f32)
    rank = jnp.sum(counts * marks, axis=0, keepdims=True).astype(jnp.int32)
    slots_out = owner_ref[...] * capacity + rank
    pick_t[...] = jnp.where(
        lax.broadcasted_iota(jnp.int32, (slots, images), 0) == slots_out, 1.0, 0.0
    ).astype(bf16)

    tile = block // 2
    loads[7].wait()

    def p_text(j, carry):
        at = pl.ds(pl.multiple_of(j * tile, tile), tile)
        pf[at, :] = lax.dot_general(
            x[0:rows, at], back[0:rows, :], ROWS_TO_COLS, preferred_element_type=f32
        )
        return carry

    lax.fori_loop(0, columns // tile, p_text, 0)

    d1_all().wait_recv()
    returned = lax.dot_general(pick_t[...], d1_dst[...], ROWS_TO_COLS, preferred_element_type=f32).astype(bf16)
    d2_src[...] = returned
    back[pl.ds(rows, images), my_cols] = returned

    def head_cols(q):
        return pl.ds(pl.multiple_of(q * cols, cols), cols)

    def d2(i, source):
        q, device = head_of(i)
        return remote(d2_src, back.at[pl.ds(rows, images), head_cols(source)], d2_s, d2_r, device)

    text_rows, image_rows = pl.ds(0, rows), pl.ds(rows, images)

    def d2_all():
        at = pl.ds(0, tp - 1)
        return remote(yb.at[at, image_rows], yr.at[at, image_rows], d2_s, d2_r, peer)

    for i in range(1, tp):
        d2(i, t).start()

    @pl.when(carries & adjacent)
    def _():
        w_forward(*w_part(base))

    @pl.when(carries & (border | entry))
    def _():
        side_forward(side_block(jnp.where(border, 1, 0)))

    d2_all().wait_recv()
    loads[6].wait()
    loads[8].wait()

    @pl.when(carries & adjacent)
    def _():
        w_forward(*w_part(base + 1))

    @pl.when(carries & entry)
    def _():
        for c in range(2, W_PARTS):
            for condition, copy in w_inward(c):
                pl.when(condition)(copy.start)

    def p_copy(i):
        at = pl.ds(pl.multiple_of(i * g_rows, g_rows), g_rows)
        return remote(pa.at[at], pb.at[at], p_s, p_r.at[i], peer)

    def g_slice(b, c):
        return pl.ds(pl.multiple_of(b * block + c * g_rows, g_rows), g_rows)

    def x_copy(b, c):
        i, at = b * G_PARTS + c, g_slice(b, c)
        return remote(pb.at[at], pa.at[at], x_s, x_r.at[i], beside)

    def x_send(b, c):
        i, at = b * G_PARTS + c, g_slice(b, c)
        p_copy(i).wait_recv()
        pb[at, :] = (pf[at, :] + pb[at, :].astype(f32)).astype(bf16)
        x_copy(b, c).start()

    def p_step(k, carry):
        b, half = near_block(blocks - 1 - k // 2), 1 - lax.rem(k, 2)
        j = b * 2 + half
        at = pl.ds(pl.multiple_of(j * tile, tile), tile)
        part = pf[at, :] + lax.dot_general(
            x[rows:both, at], back[rows:both, :], ROWS_TO_COLS, preferred_element_type=f32
        )
        pf[at, :] = part

        @pl.when(carries)
        def _():
            pa[at, :] = part.astype(bf16)
            for c in range(tile // g_rows):
                p_copy(j * (tile // g_rows) + c).start()

        @pl.when(jnp.logical_not(carries) & (half == 0))
        def _():
            lax.fori_loop(G_MAIN, G_PARTS, lambda c, unused: (x_send(b, c), unused)[1], 0)

        return carry

    lax.fori_loop(0, columns // tile, p_step, 0)

    @pl.when(carries & adjacent)
    def _():
        w_forward(*w_part(base + 2))

    @pl.when(carries & inside)
    def _():
        side_forward(side_block(jnp.where(entry, 1, 0)))

    def w_step(n):
        b, c = w_part(n)
        ahead = jnp.where(border, n + 3, n)
        next_b, next_c = w_part(ahead)
        forwarded = (adjacent & (ahead >= base) & (ahead < base + 3)) | (inside & (z == z0 + next_b))

        @pl.when(carries & (ahead < w_steps) & jnp.logical_not(forwarded))
        def _():
            w_forward(next_b, next_c)

        @pl.when(jnp.logical_not(carries))
        def _():
            w_load(b, c).wait()

        at = w_slice(b, c)
        for which, send, recv in ((image_rows, ci_s, ci_r), (text_rows, ct_s, ct_r)):
            y[which, :] += jnp.dot(x[which, at], w[at, :], preferred_element_type=f32)

            @pl.when(n == w_steps - 1)
            def _():
                c1_send(which, send, recv)

        grads = lax.dot_general(back[...], w[at, :], COLS_TO_COLS, preferred_element_type=f32).astype(bf16)
        text_out[:, at] = grads[:rows]
        image_out[:, at] = grads[rows:]

    def c1(i, source, which, send, recv):
        q, device = head_of(i)
        return remote(yb.at[q, which], yr.at[source, which], send, recv, device)

    def c1_all(which, send, recv):
        at = pl.ds(0, tp - 1)
        return remote(yb.at[at, which], yr.at[at, which], send, recv, peer)

    def c1_send(which, send, recv):
        for q in range(tp):
            yb[q, which, :] = y[which, q * cols : (q + 1) * cols].astype(bf16)
        for i in range(1, tp):
            c1(i, t, which, send, recv).start()

    def c2(i):
        v, device = unit_of(i)
        return remote(c2_src.at[slot_rows(v)], c2_dst.at[slot_rows(me)], c2_s, c2_r, device)

    def c2_all():
        at = pl.ds(0, (units - 1) * capacity)
        return remote(c2_src.at[at], c2_dst.at[at], c2_s, c2_r, peer)

    def c2_send():
        total = y[image_rows, my_cols]
        c1_all(image_rows, ci_s, ci_r).wait_recv()
        for i in range(1, tp):
            q = head_of(i)[0]
            total = total + yr[q, image_rows, :].astype(f32)
        c2_src[...] = jnp.dot(pick_t[...], total.astype(bf16), preferred_element_type=f32).astype(bf16)
        for i in range(1, units):
            c2(i).start()
        c2_dst[slot_rows(me), :] = c2_src[slot_rows(me), :]

    def home(b, c):
        return jnp.where(c < G_MAIN, z0, other_z0) + b

    def chain_copies(b, c):
        i, at = b * G_PARTS + c, g_slice(b, c)
        return (
            (z > home(b, c), remote(chain.at[at], above.at[at], ch_s, ab_r.at[i], (g, z - 1, t))),
            (z < home(b, c), remote(chain.at[at], below.at[at], ch_s, be_r.at[i], (g, z + 1, t))),
        )

    def landing(c):
        return landed.at[pl.ds(pl.multiple_of(c * g_rows, g_rows), g_rows)]

    def result_copy(b, c, q):
        return remote(
            chain.at[g_slice(b, c), q * cols : (q + 1) * cols], landing(c), g_s, g_r, (1 - g, z, q)
        )

    def g_step(m):
        sides = blocks * (G_PARTS - G_MAIN)
        mains = blocks * G_MAIN
        own = jnp.where(inside, m >= sides, m < mains)
        own_m, other_m = jnp.where(inside, m - sides, m), jnp.where(inside, m, m - mains)
        b = jnp.where(own, near_block(blocks - 1 - own_m // G_MAIN), far_other(other_m // (G_PARTS - G_MAIN)))
        c = jnp.where(own, lax.rem(own_m, G_MAIN), G_MAIN + lax.rem(other_m, G_PARTS - G_MAIN))
        i, at, zb = b * G_PARTS + c, g_slice(b, c), home(b, c)

        @pl.when(own)
        def _():
            p_copy(i).wait_recv()
            pf[at, :] += pb[at, :].astype(f32)

        @pl.when(jnp.logical_not(own))
        def _():
            x_copy(b, c).wait_recv()
            pf[at, :] = pa[at, :].astype(f32)

        @pl.when((z >= zb) & (z < fsdp - 1))
        def _():
            remote(chain.at[at], above.at[at], ch_s, ab_r.at[i], peer).wait_recv()
            pf[at, :] += above[at, :].astype(f32)

        @pl.when((z <= zb) & (z > 0))
        def _():
            remote(chain.at[at], below.at[at], ch_s, be_r.at[i], peer).wait_recv()
            pf[at, :] += below[at, :].astype(f32)

        chain[at, :] = pf[at, :].astype(bf16)
        for condition, copy in chain_copies(b, c):
            pl.when(condition)(copy.start)

        @pl.when(z == zb)
        def _():
            for q in range(tp):
                result_copy(b, c, q).start()

    ratio = g_steps // w_steps
    half = w_steps // 2
    lead = blocks * G_MAIN // ratio
    turns = w_steps + lead + 1
    sums = jnp.logical_not(carries)
    late = sums & far_end
    w_at = jnp.where(late, lead, 0)
    c2_at = jnp.where(carries, w_steps - 1, jnp.where(far_end, lead + w_steps - 1, w_steps + 1))

    def turn(s, carry):
        n = s - w_at
        late_m = jnp.where(s < lead, s, jnp.where(s == lead + w_steps - 2, lead, jnp.where(s == lead + w_steps, lead + 1, -1)))
        m = jnp.where(late, late_m, s - 3)

        @pl.when(carries & inside & jnp.logical_not(entry) & (s == half))
        def _():
            side_forward(side_block(1))

        @pl.when(sums & (m >= 0) & (m < w_steps))
        def _():
            lax.fori_loop(0, ratio, lambda k, unused: (g_step(m * ratio + k), unused)[1], 0)

        @pl.when((n >= 0) & (n < w_steps))
        def _():
            w_step(n)

        @pl.when(s == c2_at)
        def _():
            c2_send()

        return carry

    lax.fori_loop(0, turns, turn, 0)

    def each(count, body):
        lax.fori_loop(0, count, lambda n, unused: (body(n), unused)[1], 0)

    def w_sent(n):
        b, c = n // W_PARTS, lax.rem(n, W_PARTS)
        for condition, copy in w_routes(b, c):
            pl.when(condition)(copy.wait_send)

    def side_sent(b):
        passes = inside | (z == other_z0 + b) | (border & (b == side_block(1)))
        for condition, copy in side_routes(b):
            pl.when(condition & passes)(copy.wait_send)

    @pl.when(carries)
    def _():
        each(w_steps, w_sent)
        each(blocks, side_sent)
        remote(w, w, w_dd, w_dd, peer).wait_send()
        remote(pa, pb, p_s, p_s, peer).wait_send()

    @pl.when(sums)
    def _():
        at = pl.ds(0, blocks * (G_PARTS - G_MAIN) * g_rows)
        remote(pb.at[at], pa.at[at], x_s, x_s, beside).wait_send()

    d1_all().wait_send()
    d2_all().wait_send()
    c1_all(image_rows, ci_s, ci_r).wait_send()
    total = y[text_rows, my_cols]
    c1_all(text_rows, ct_s, ct_r).wait_recv()
    for i in range(1, tp):
        total = total + yr[head_of(i)[0], text_rows, :].astype(f32)
    c2_all().wait_recv()
    placed = lax.dot_general(place_t[...], c2_dst[...], ROWS_TO_COLS, preferred_element_type=f32)
    projected = jnp.where(is_img[...] > 0.5, placed, total) + bias_ref[...]
    for s in range(rows // LENGTH):
        values = projected[s * LENGTH : (s + 1) * LENGTH]
        turned = values * cosv[...] + pltpu.roll(values, HALF, 1) * sinv[...]
        keys_out[s * LENGTH : (s + 1) * LENGTH, :] = jnp.where(live(s), turned, 0.0).astype(bf16)

    remote(landed, landed, g_s, g_r, peer).wait_recv()
    wgrad_out[...] = landed[...].astype(f32) * (1.0 / rows)

    for condition, parts in ((inside, G_MAIN), (jnp.logical_not(inside), G_PARTS - G_MAIN)):

        @pl.when(sums & condition)
        def _():
            ends, passed = pl.ds(0, parts * g_rows), pl.ds(0, (g_steps - parts) * g_rows)
            remote(chain.at[ends], above.at[ends], g_s, g_s, peer).wait_send()
            remote(chain.at[passed], above.at[passed], ch_s, ch_s, peer).wait_send()

    c1_all(text_rows, ct_s, ct_r).wait_send()
    c2_all().wait_send()


def write_kernel(*refs):
    count = (len(refs) - 1) // 2
    copies = [pltpu.make_async_copy(refs[i], refs[count + i], refs[-1].at[i]) for i in range(count)]
    for copy in copies:
        copy.start()
    for copy in copies:
        copy.wait()


def rotary_tables():
    frequency = ROPE_BASE ** (-(np.arange(HALF, dtype=np.float64) * 2.0) / HEAD_DIM)
    table = np.arange(LENGTH, dtype=np.float64)[:, None] * frequency[None, :]
    cosine, sine = np.cos(table), np.sin(table)
    return (
        np.concatenate([cosine, cosine], axis=1).astype(np.float32),
        np.concatenate([-sine, sine], axis=1).astype(np.float32),
    )


def fits(groups, fsdp, tp, rows, head_cols, block):
    units = groups * fsdp
    if groups != 2 or units % tp or head_cols != HEAD_DIM or rows % LENGTH:
        return False
    blocks = units // tp
    return blocks == 2 and fsdp == 2 * blocks and tp % 2 == 0 and block % (G_PARTS * HEAD_DIM) == 0 and (rows // units) % 16 == 0


def per_device(
    text_embeds, image_embeds, key_weight, key_bias, key_cot, image_owner, image_slot, seq_lengths
):
    groups, fsdp, tp = lax.axis_size("group"), lax.axis_size("fsdp"), lax.axis_size("tp")
    rows, columns = text_embeds.shape
    images = image_embeds.shape[0]
    cols = key_bias.shape[0]
    block = key_weight.shape[0]
    if not fits(groups, fsdp, tp, rows, cols, block):
        return per_device_plain(
            text_embeds, image_embeds, key_weight, key_bias, key_cot, image_owner, image_slot, seq_lengths
        )
    units = groups * fsdp
    capacity = rows // units
    slots = units * capacity
    both, key_cols = rows + images, cols * tp
    blocks = units // tp
    w_steps, g_steps = blocks * W_PARTS, blocks * G_PARTS
    cosine, sine = rotary_tables()
    bf16, f32 = jnp.bfloat16, jnp.float32
    hbm = pl.BlockSpec(memory_space=pltpu.HBM)
    vmem = pl.BlockSpec(memory_space=pltpu.VMEM)
    dma = lambda n: pltpu.SemaphoreType.DMA((n,))
    one = pltpu.SemaphoreType.DMA
    shapes = (
        jax.ShapeDtypeStruct((rows, cols), bf16),
        jax.ShapeDtypeStruct((rows, columns), bf16),
        jax.ShapeDtypeStruct((images, columns), bf16),
        jax.ShapeDtypeStruct((block, cols), f32),
    )
    operands = (
        text_embeds, image_embeds, key_weight, key_bias.reshape(1, -1), key_cot,
        image_owner.reshape(1, -1), image_slot.reshape(1, -1), seq_lengths.reshape(1, -1), jnp.asarray(cosine), jnp.asarray(sine),
    )
    held = pl.pallas_call(
        functools.partial(fused_kernel, groups, fsdp, tp, capacity),
        out_shape=tuple(pltpu.VMEM(leaf.shape, leaf.dtype) for leaf in shapes),
        in_specs=[hbm] * 10,
        out_specs=(vmem, vmem, vmem, vmem),
        scratch_shapes=[
            pltpu.VMEM((1, cols), f32),
            pltpu.VMEM((1, images), jnp.int32),
            pltpu.VMEM((1, rows), jnp.int32),
            pltpu.VMEM((1, seq_lengths.shape[0]), jnp.int32),
            pltpu.VMEM((both, columns), bf16),
            pltpu.VMEM((columns, key_cols), bf16),
            pltpu.VMEM((rows, key_cols), bf16),
            pltpu.VMEM((LENGTH, cols), f32),
            pltpu.VMEM((LENGTH, cols), f32),
            pltpu.VMEM((both, key_cols), bf16),
            pltpu.VMEM((slots, images), bf16),
            pltpu.VMEM((slots, rows), bf16),
            pltpu.VMEM((rows, cols), f32),
            pltpu.VMEM((slots, cols), bf16),
            pltpu.VMEM((slots, cols), bf16),
            pltpu.VMEM((images, cols), bf16),
            pltpu.VMEM((columns, key_cols), f32),
            pltpu.VMEM((columns, key_cols), bf16),
            pltpu.VMEM((columns, key_cols), bf16),
            pltpu.VMEM((columns, key_cols), bf16),
            pltpu.VMEM((columns, key_cols), bf16),
            pltpu.VMEM((columns, key_cols), bf16),
            pltpu.VMEM((both, key_cols), f32),
            pltpu.VMEM((tp, both, cols), bf16),
            pltpu.VMEM((tp, both, cols), bf16),
            pltpu.VMEM((slots, cols), bf16),
            pltpu.VMEM((slots, cols), bf16),
            pltpu.VMEM((block, cols), bf16),
            pltpu.VMEM((blocks, block // W_PARTS, key_cols), bf16),
            dma(9), dma(w_steps), dma(w_steps), dma(w_steps), one,
            one, one, one, one, one, one, one, one, one, one,
            one, dma(g_steps), dma(g_steps), dma(g_steps), one, one, one,
            one, dma(g_steps), dma(blocks), dma(blocks), dma(blocks),
        ],
        compiler_params=pltpu.CompilerParams(
            collective_id=0, has_side_effects=True, vmem_limit_bytes=44 * 1024 * 1024
        ),
        name="fused",
    )(*(pltpu.with_memory_space_constraint(operand, pltpu.HBM) for operand in operands))
    return pl.pallas_call(
        write_kernel,
        out_shape=shapes,
        in_specs=[vmem] * 4,
        out_specs=(pl.BlockSpec(memory_space=pl.ANY),) * 4,
        scratch_shapes=[dma(4)],
        compiler_params=pltpu.CompilerParams(vmem_limit_bytes=4 * 1024 * 1024),
        name="write",
    )(*held)


def solution(mesh):
    in_specs = (
        P(("group", "fsdp"), "tp"),
        P(("group", "fsdp"), "tp"),
        P(("group", "fsdp"), None),
        P("tp"),
        P(("group", "fsdp"), None),
        P(("group", "fsdp")),
        P(("group", "fsdp")),
        P(("group", "fsdp")),
    )
    out_specs = (
        P(("group", "fsdp"), "tp"),
        P(("group", "fsdp"), "tp"),
        P(("group", "fsdp"), "tp"),
        P(("group", "fsdp"), "tp"),
    )
    return jax.shard_map(
        per_device, mesh=mesh, in_specs=in_specs, out_specs=out_specs, check_vma=False
    )
```

```python
import functools

import jax
import jax.numpy as jnp
import numpy as np
from jax import lax
from jax.experimental import pallas as pl
from jax.experimental.pallas import tpu as pltpu
from jax.sharding import PartitionSpec as P

HEAD_DIM = 128
LENGTH = 256


ROPE_BASE = 1000000.0


def angles(row_total):
    position = (jnp.arange(row_total, dtype=jnp.int32) % LENGTH).astype(jnp.float32)
    frequency = ROPE_BASE ** (-(jnp.arange(HEAD_DIM // 2, dtype=jnp.float32) * 2.0) / HEAD_DIM)
    angle_table = position[:, None] * frequency[None, :]
    return (jnp.cos(angle_table), jnp.sin(angle_table))


def rotate(values, cosine, sine, direction):
    row_total = values.shape[0]
    by_head = values.reshape(row_total, -1, HEAD_DIM)
    half_dim = HEAD_DIM // 2
    front_half = by_head[..., :half_dim]
    second = by_head[..., half_dim:]
    cos_part = cosine[:, None, :]
    sin_part = direction * sine[:, None, :]
    rotated = jnp.concatenate(
        [front_half * cos_part - second * sin_part, second * cos_part + front_half * sin_part],
        axis=-1,
    )
    return rotated.reshape(row_total, -1)


def send_slots(owners, unit_count, capacity):
    onehot_marks = (owners[:, None] == jnp.arange(unit_count, dtype=jnp.int32)[None, :]).astype(
        jnp.int32
    )
    before = jnp.cumsum(onehot_marks, axis=0) - onehot_marks
    owner_rank = jnp.sum(before * onehot_marks, axis=1)
    return owners * capacity + owner_rank


def share_kernel(text_ref, image_ref, back_ref, image_back_ref, out_ref):
    contract = (((0,), (0,)), ((), ()))
    part = lax.dot_general(
        text_ref[...], back_ref[...], contract, preferred_element_type=jnp.float32
    ) + lax.dot_general(
        image_ref[...], image_back_ref[...], contract, preferred_element_type=jnp.float32
    )
    part = part.astype(out_ref.dtype)
    width = out_ref.shape[2]
    for head in range(out_ref.shape[0]):
        out_ref[head] = part[:, head * width : (head + 1) * width]


def weight_shares(text, image, back, image_back, head_cols):
    columns = text.shape[1]
    heads = back.shape[1] // head_cols
    tile = min(512, columns)
    return pl.pallas_call(
        share_kernel,
        grid=(columns // tile,),
        in_specs=[
            pl.BlockSpec((text.shape[0], tile), lambda i: (0, i)),
            pl.BlockSpec((image.shape[0], tile), lambda i: (0, i)),
            pl.BlockSpec(back.shape, lambda i: (0, 0)),
            pl.BlockSpec(image_back.shape, lambda i: (0, 0)),
        ],
        out_specs=pl.BlockSpec((heads, tile, head_cols), lambda i: (0, i, 0)),
        out_shape=jax.ShapeDtypeStruct((heads, columns, head_cols), jnp.bfloat16),
        cost_estimate=pl.CostEstimate(
            flops=2 * (text.size + image.size) * back.shape[1],
            bytes_accessed=2 * (text.size + image.size + columns * back.shape[1]),
            transcendentals=0,
        ),
    )(text, image, back, image_back)


def project_kernel(text_ref, image_ref, weight_ref, out_ref):
    step = pl.program_id(0)
    last = pl.num_programs(0) - 1
    rows = jnp.where(step == last, image_ref[...], text_ref[...])
    part = jnp.dot(rows, weight_ref[...], preferred_element_type=jnp.float32).astype(out_ref.dtype)
    width = out_ref.shape[2]
    for head in range(out_ref.shape[0]):
        out_ref[head] = part[:, head * width : (head + 1) * width]


def projection_parts(text, image, weight, head_cols):
    heads = weight.shape[1] // head_cols
    tile, columns = image.shape
    text_tiles = text.shape[0] // tile
    return pl.pallas_call(
        project_kernel,
        grid=(text_tiles + 1,),
        in_specs=[
            pl.BlockSpec((tile, columns), lambda i: (jnp.minimum(i, text_tiles - 1), 0)),
            pl.BlockSpec((tile, columns), lambda i: (0, 0)),
            pl.BlockSpec(weight.shape, lambda i: (0, 0)),
        ],
        out_specs=pl.BlockSpec((heads, tile, head_cols), lambda i: (0, i, 0)),
        out_shape=jax.ShapeDtypeStruct((heads, text.shape[0] + tile, head_cols), jnp.bfloat16),
        cost_estimate=pl.CostEstimate(
            flops=2 * (text.size + image.size) * weight.shape[1],
            bytes_accessed=2 * (text.size + image.size + weight.size),
            transcendentals=0,
        ),
    )(text, image, weight)


def spread(piece, axis):
    count = lax.axis_size(axis)
    copies = jnp.broadcast_to(piece[None], (count,) + piece.shape)
    got = lax.all_to_all(copies, axis, split_axis=0, concat_axis=0, tiled=True)
    return got.reshape((count * piece.shape[0],) + piece.shape[1:])


def shifted(values, axis, step):
    count = lax.axis_size(axis)
    return lax.ppermute(values, axis, [(i, (i + step) % count) for i in range(count)])


def exchange_sum(blocks, axis):
    count = lax.axis_size(axis)
    me = lax.axis_index(axis)
    total = lax.dynamic_index_in_dim(blocks, me, 0, keepdims=False).astype(jnp.float32)
    for step in range(1, count):
        block = lax.dynamic_index_in_dim(blocks, (me + step) % count, 0, keepdims=False)
        total = total + shifted(block, axis, step).astype(jnp.float32)
    return total


def share_rows(piece, axis):
    count = lax.axis_size(axis)
    me = lax.axis_index(axis)
    rows = piece.shape[0]
    full = jnp.zeros((count * rows,) + piece.shape[1:], piece.dtype)
    full = lax.dynamic_update_slice_in_dim(full, piece, me * rows, 0)
    for step in range(1, count):
        source = (me + count - step) % count
        full = lax.dynamic_update_slice_in_dim(full, shifted(piece, axis, step), source * rows, 0)
    return full


def per_device_plain(
    text_embeds, image_embeds, key_weight, key_bias, key_cot, image_owner, image_slot, seq_lengths
):
    row_count, columns = text_embeds.shape
    image_count = image_embeds.shape[0]
    units = ("group", "fsdp")
    core_count = lax.axis_size("group")
    fsdp_count = lax.axis_size("fsdp")
    tp_count = lax.axis_size("tp")
    unit_count = core_count * fsdp_count
    capacity = row_count // unit_count
    slot_count = unit_count * capacity
    head_cols = key_bias.shape[0]
    key_cols = head_cols * tp_count
    weight_block = key_weight.shape[0]
    halves = unit_count // tp_count
    tp_index = lax.axis_index("tp")

    position = jnp.arange(row_count, dtype=jnp.int32)
    seq_ids = position // LENGTH
    seq_marks = seq_ids[:, None] == jnp.arange(seq_lengths.shape[0], dtype=jnp.int32)[None, :]
    live_limit = jnp.sum(jnp.where(seq_marks, seq_lengths[None, :], 0), axis=1)
    live_mask = (position % LENGTH < live_limit).astype(jnp.float32)
    cosine, sine = angles(row_count)
    masked = key_cot.astype(jnp.float32) * live_mask[:, None]
    rotated_back = rotate(masked, cosine, sine, -1.0).astype(jnp.bfloat16)
    is_image = image_slot >= 0
    text_back = jnp.where(is_image[:, None], jnp.zeros_like(rotated_back), rotated_back)

    slot_ids = jnp.arange(slot_count, dtype=jnp.int32)
    place = (image_slot[:, None] == slot_ids[None, :]).astype(jnp.bfloat16)
    returning = lax.dot_general(
        place, rotated_back, (((0,), (0,)), ((), ())), preferred_element_type=jnp.float32
    ).astype(jnp.bfloat16)
    returned = lax.all_to_all(
        returning.reshape(unit_count, capacity, key_cols), units, split_axis=0, concat_axis=0,
        tiled=True,
    ).reshape(slot_count, key_cols)
    slots_out = send_slots(image_owner, unit_count, capacity)
    pick = (slots_out[:, None] == slot_ids[None, :]).astype(jnp.bfloat16)
    image_back = jnp.dot(pick, returned, preferred_element_type=jnp.float32).astype(jnp.bfloat16)

    piece_rows = weight_block // tp_count
    own_piece = lax.dynamic_slice_in_dim(key_weight, tp_index * piece_rows, piece_rows, 0)
    moves = []
    for unit in range(unit_count):
        for part in range(tp_count):
            target = (unit % halves) * tp_count + part
            moves.append((unit * tp_count + part, target * tp_count + unit // halves))
    own_piece = lax.ppermute(own_piece, units + ("tp",), moves)
    chip_rows = spread(own_piece, "fsdp")

    shares = weight_shares(text_embeds, image_embeds, text_back, image_back, head_cols)
    shares = shares.reshape(core_count, fsdp_count, weight_block, head_cols)
    shares = exchange_sum(shares, "group").astype(jnp.bfloat16)
    shares, chip_rows = lax.optimization_barrier((shares, chip_rows))
    shares = lax.all_to_all(shares, "fsdp", split_axis=0, concat_axis=0, tiled=True)
    weight_grad = jnp.sum(shares.astype(jnp.float32), axis=0) / row_count
    returns = []
    for unit in range(unit_count):
        for part in range(tp_count):
            holder = (unit % halves) + part * halves
            returns.append((holder * tp_count + unit // halves, unit * tp_count + part))
    weight_grad = lax.ppermute(weight_grad, units + ("tp",), returns)

    weight_rows = share_rows(chip_rows, "group")
    both = projection_parts(text_embeds, image_embeds, weight_rows, head_cols)
    both = exchange_sum(both, "tp")
    image_proj = both[row_count:].astype(jnp.bfloat16)
    outgoing = lax.dot_general(
        pick, image_proj, (((0,), (0,)), ((), ())), preferred_element_type=jnp.float32
    ).astype(jnp.bfloat16)
    received = lax.all_to_all(
        outgoing.reshape(unit_count, capacity, head_cols), units, split_axis=0, concat_axis=0,
        tiled=True,
    ).reshape(slot_count, head_cols)
    placed = jnp.dot(place, received, preferred_element_type=jnp.float32)
    projected = jnp.where(is_image[:, None], placed, both[:row_count]) + key_bias
    key_rows = (rotate(projected, cosine, sine, 1.0) * live_mask[:, None]).astype(jnp.bfloat16)

    contract = (((1,), (1,)), ((), ()))
    text_grad = lax.dot_general(
        text_back, weight_rows, contract, preferred_element_type=jnp.float32
    ).astype(jnp.bfloat16)
    image_grad = lax.dot_general(
        image_back, weight_rows, contract, preferred_element_type=jnp.float32
    ).astype(jnp.bfloat16)
    return (key_rows, text_grad, image_grad, weight_grad)


MESH = pl.DeviceIdType.MESH
HALF = HEAD_DIM // 2
ROWS_TO_COLS = (((0,), (0,)), ((), ()))
COLS_TO_COLS = (((1,), (1,)), ((), ()))
W_PARTS = 4
W_MAIN = 3
W_FINE = 2
W_NEAR_OR_FAR = (0, 0, 0, 1, 0, 1, 1, 1)
W_PART_AT = (0, 1, 2, 0, 3, 1, 3, 2)
FAR_STEPS = (0, 2, 4, 6, 8, 10, 10, 10, 10, 10, 13, 13, 13, 13, 16)
BORDER_STEPS = (0, 0, 0, 0, 2, 4, 6, 8, 8, 13, 13, 16, 16, 16, 16)
ENTRY_STEPS = (0, 0, 0, 0, 0, 0, 0, 0, 0, 4, 8, 14, 16, 16, 16)
LAST_STEPS = (0, 0, 0, 0, 2, 4, 6, 9, 11, 13, 13, 16, 16, 16, 16)
G_PARTS = 8
G_MAIN = 5


def fused_kernel(
    groups, fsdp, tp, capacity,
    text_ref, image_ref, weight_ref, bias_hbm, cot_ref, owner_hbm, slot_hbm, lens_hbm, cos_ref, sin_ref,
    keys_out, text_out, image_out, wgrad_out,
    bias_ref, owner_ref, slot_ref, lens_ref, x, w, cot, cosv, sinv, back, pick_t, place_t, is_img,
    d1_src, d1_dst, d2_src, pf, pa, pb, chain, above, below, y, yb, yr, c2_src, c2_dst, landed, side,
    ld, w_recv, sent, shared, small, d1_r, d2_r, ci_r, ct_r, c2_r, g_r, p_r, chain_r, x_r, h_r,
):
    f32, bf16 = jnp.float32, jnp.bfloat16
    g, z, t = lax.axis_index("group"), lax.axis_index("fsdp"), lax.axis_index("tp")
    units = groups * fsdp
    me = g * fsdp + z
    rows, images = text_ref.shape[0], image_ref.shape[0]
    both = rows + images
    columns = text_ref.shape[1]
    slots = units * capacity
    cols = bias_ref.shape[1]
    block = weight_ref.shape[0]
    blocks = units // tp
    key_cols = tp * cols
    w_rows, g_rows = block // W_PARTS, block // G_PARTS
    w_steps, g_steps = blocks * W_PARTS, blocks * G_PARTS
    first = t * blocks
    carrier, z0 = first // fsdp, lax.rem(first, fsdp)
    carries = g == carrier
    inside = (z >= z0) & (z < z0 + blocks)
    far_end = jnp.logical_not(inside) & ((z == 0) | (z == fsdp - 1))
    my_cols = pl.ds(pl.multiple_of(t * cols, cols), cols)
    peer = (1 - g, z, t)
    other = lax.bitwise_xor(t, 1)
    beside = (g, z, other)
    other_z0 = fsdp - blocks - z0
    upward = z0 > 0
    entry = jnp.where(upward, z == z0, z == z0 + blocks - 1)
    border = jnp.where(upward, z == z0 - 1, z == z0 + blocks)
    relays = entry | border

    def near_block(k):
        within = lax.rem(z - z0 + k + blocks, blocks)
        return jnp.where(inside, within, jnp.where(z < z0, k, blocks - 1 - k))

    def far_other(k):
        within = lax.rem(z - other_z0 + blocks - 1 - k + blocks, blocks)
        return jnp.where(inside, jnp.where(upward, k, blocks - 1 - k), within)

    def look_up(table, n):
        found = table[0]
        for i in range(1, len(table)):
            found = jnp.where(n == i, table[i], found)
        return found

    def w_part(n):
        return near_block(look_up(W_NEAR_OR_FAR, n)), look_up(W_PART_AT, n)

    def unit_of(i):
        v = lax.rem(me + i, units)
        return v, (v // fsdp, lax.rem(v, fsdp), t)

    def head_of(i):
        q = lax.rem(t + i, tp)
        return q, (g, z, q)

    def remote(src, dst, send, recv, device):
        return pltpu.make_async_remote_copy(
            src_ref=src, dst_ref=dst, send_sem=send, recv_sem=recv, device_id=device, device_id_type=MESH
        )

    barrier = pltpu.get_barrier_semaphore()
    for i in range(1, units):
        pl.semaphore_signal(barrier, inc=1, device_id=unit_of(i)[1], device_id_type=MESH)
    for i in range(1, tp):
        q = head_of(i)[0]
        for core in range(groups):
            pl.semaphore_signal(barrier, inc=1, device_id=(core, z, q), device_id_type=MESH)

    pairs = (
        (slot_hbm, slot_ref),
        (cot_ref, cot),
        (cos_ref, cosv),
        (sin_ref, sinv),
        (lens_hbm, lens_ref),
        (owner_hbm, owner_ref),
        (bias_hbm, bias_ref),
        (text_ref, x.at[pl.ds(0, rows)]),
        (image_ref, x.at[pl.ds(rows, images)]),
    )
    loads = [pltpu.make_async_copy(source, target, ld.at[i]) for i, (source, target) in enumerate(pairs)]
    for load in loads[:5]:
        load.start()

    def w_slice(b, c):
        return pl.ds(pl.multiple_of(b * block + c * w_rows, w_rows), w_rows)

    fine = w_rows // W_FINE

    def w_fine(b, c, h):
        return pl.ds(pl.multiple_of(b * block + c * w_rows + h * fine, fine), fine)

    def w_index(b, c, h):
        return (b * W_PARTS + c) * W_FINE + h

    def w_load(b, c, h):
        source = weight_ref.at[pl.ds(pl.multiple_of(c * w_rows + h * fine, fine), fine)]
        return pltpu.make_async_copy(source, w.at[w_fine(b, c, h)], w_recv.at[w_index(b, c, h)])

    def side_rows(b, h):
        return side.at[b, pl.ds(h * fine, fine)]

    def side_load(b, h):
        source = weight_ref.at[pl.ds(W_MAIN * w_rows + h * fine, fine)]
        return pltpu.make_async_copy(source, side_rows(b, h), h_r.at[b * W_FINE + h])

    @pl.when(carries & inside)
    def _():
        for c in range(W_PARTS):
            for h in range(W_FINE):
                w_load(z - z0, c, h).start()

    @pl.when(carries & jnp.logical_not(inside))
    def _():
        for h in range(W_FINE):
            side_load(z - other_z0, h).start()

    for load in loads[5:]:
        load.start()

    loads[0].wait()
    slot_ids = lax.broadcasted_iota(jnp.int32, (slots, rows), 0)
    place_t[...] = jnp.where(slot_ids == slot_ref[...], 1.0, 0.0).astype(bf16)
    is_img[...] = lax.dot_general(
        place_t[...], jnp.ones((slots, cols), bf16), ROWS_TO_COLS, preferred_element_type=f32
    )
    row_ids = lax.broadcasted_iota(jnp.int32, (LENGTH, HEAD_DIM), 0)

    def live(s):
        return row_ids < lens_ref[0:1, s : s + 1]

    def rotated_back(s, at):
        span = pl.ds(s * LENGTH, LENGTH)
        values = jnp.where(live(s), cot[span, at].astype(f32), 0.0)
        return values * cosv[...] - pltpu.roll(values, HALF, 1) * sinv[...]

    for load in loads[1:5]:
        load.wait()
    mine = jnp.concatenate([rotated_back(s, my_cols) for s in range(rows // LENGTH)], axis=0).astype(bf16)
    d1_src[...] = jnp.dot(place_t[...], mine, preferred_element_type=f32).astype(bf16)

    pl.semaphore_wait(barrier, units - 1 + groups * (tp - 1))

    def slot_rows(v):
        return pl.ds(pl.multiple_of(v * capacity, capacity), capacity)

    def d1(i):
        v, device = unit_of(i)
        return remote(d1_src.at[slot_rows(v)], d1_dst.at[slot_rows(me)], small, d1_r, device)

    def d1_all():
        at = pl.ds(0, (units - 1) * capacity)
        return remote(d1_src.at[at], d1_dst.at[at], small, d1_r, peer)

    for i in range(1, units):
        d1(i).start()
    d1_dst[slot_rows(me), :] = d1_src[slot_rows(me), :]

    def w_send(b, c, h, to):
        at = w_fine(b, c, h)
        return remote(w.at[at], w.at[at], sent, w_recv.at[w_index(b, c, h)], to)

    def w_share(b, c, h):
        at = w_fine(b, c, h)
        return remote(w.at[at], w.at[at], shared, w_recv.at[w_index(b, c, h)], peer)

    def w_routes(b, c, h):
        up = (z >= z0 + b) & (z < fsdp - 1) & ((c < W_MAIN) | (z + 1 < z0 + blocks))
        down = (z <= z0 + b) & (z > 0) & ((c < W_MAIN) | (z > z0))
        return ((up, w_send(b, c, h, (g, z + 1, t))), (down, w_send(b, c, h, (g, z - 1, t))))

    def w_inward(c):
        b = z - z0
        for h in range(W_FINE):
            pl.when(upward)(w_send(b, c, h, (g, z + 1, t)).start)
            pl.when(jnp.logical_not(upward))(w_send(b, c, h, (g, z - 1, t)).start)

    def side_routes(b, h):
        step = jnp.where(upward, 1, -1)
        i, at = b * W_FINE + h, w_fine(b, W_MAIN, h)
        return (
            ((z + step >= 0) & (z + step < fsdp), remote(side_rows(b, h), side_rows(b, h), sent, h_r.at[i], (g, z + step, t))),
            (inside, remote(side_rows(b, h), w.at[at], sent, w_recv.at[w_index(b, W_MAIN, h)], beside)),
        )

    def side_forward(b):
        for h in range(W_FINE):
            side_load(b, h).wait()
            for condition, copy in side_routes(b, h):
                pl.when(condition)(copy.start)

    def side_block(k):
        return jnp.where(upward, blocks - 1 - k, k)

    def w_forward(b, c):
        held = entry & (z == z0 + b) & (c >= 2)
        for h in range(W_FINE):
            w_load(b, c, h).wait()
            for (condition, copy), inward in zip(w_routes(b, c, h), (upward, jnp.logical_not(upward))):
                pl.when(condition & jnp.logical_not(held & inward))(copy.start)
            w_share(b, c, h).start()

    @pl.when(carries & inside)
    def _():
        lax.fori_loop(0, W_PARTS, lambda c, carry: (w_forward(z - z0, c), carry)[1], 0)

    @pl.when(carries & jnp.logical_not(inside))
    def _():
        side_forward(z - other_z0)

    early = jnp.where(inside, near_block(1), near_block(0))

    y[...] = jnp.zeros_like(y)
    for s in range(rows // LENGTH):
        span = pl.ds(s * LENGTH, LENGTH)
        for h in range(tp):
            at = pl.ds(h * cols, cols)
            back[span, at] = jnp.where(is_img[span, :] > 0.5, 0.0, rotated_back(s, at)).astype(bf16)
    loads[5].wait()
    image_units = lax.broadcasted_iota(jnp.int32, (units, images), 0)
    marks = jnp.where(image_units == owner_ref[...], 1.0, 0.0)
    before = jnp.where(
        lax.broadcasted_iota(jnp.int32, (images, images), 0) < lax.broadcasted_iota(jnp.int32, (images, images), 1),
        1.0,
        0.0,
    ).astype(bf16)
    counts = jnp.dot(marks.astype(bf16), before, preferred_element_type=f32)
    rank = jnp.sum(counts * marks, axis=0, keepdims=True).astype(jnp.int32)
    slots_out = owner_ref[...] * capacity + rank
    pick_t[...] = jnp.where(
        lax.broadcasted_iota(jnp.int32, (slots, images), 0) == slots_out, 1.0, 0.0
    ).astype(bf16)

    tile = block // 2
    loads[7].wait()

    def p_text(j, carry):
        at = pl.ds(pl.multiple_of(j * tile, tile), tile)
        pf[at, :] = lax.dot_general(
            x[0:rows, at], back[0:rows, :], ROWS_TO_COLS, preferred_element_type=f32
        )
        return carry

    lax.fori_loop(0, columns // tile, p_text, 0)

    d1_all().wait_recv()
    returned = lax.dot_general(pick_t[...], d1_dst[...], ROWS_TO_COLS, preferred_element_type=f32).astype(bf16)
    d2_src[...] = returned
    back[pl.ds(rows, images), my_cols] = returned

    def head_cols(q):
        return pl.ds(pl.multiple_of(q * cols, cols), cols)

    def d2(i, source):
        q, device = head_of(i)
        return remote(d2_src, back.at[pl.ds(rows, images), head_cols(source)], small, d2_r, device)

    text_rows, image_rows = pl.ds(0, rows), pl.ds(rows, images)

    def d2_all():
        at = pl.ds(0, tp - 1)
        return remote(yb.at[at, image_rows], yr.at[at, image_rows], small, d2_r, peer)

    for i in range(1, tp):
        d2(i, t).start()

    @pl.when(carries & (inside | border))
    def _():
        w_forward(early, 0)

    @pl.when(carries & relays)
    def _():
        side_forward(side_block(jnp.where(border, 1, 0)))

    d2_all().wait_recv()
    loads[6].wait()
    loads[8].wait()

    @pl.when(carries & (inside | border))
    def _():
        w_forward(early, 1)

    def p_copy(i):
        at = pl.ds(pl.multiple_of(i * g_rows, g_rows), g_rows)
        return remote(pa.at[at], pb.at[at], shared, p_r.at[i], peer)

    def g_slice(b, c):
        return pl.ds(pl.multiple_of(b * block + c * g_rows, g_rows), g_rows)

    def x_copy(b, c):
        i, at = b * (G_PARTS - G_MAIN) + c - G_MAIN, g_slice(b, c)
        return remote(pb.at[at], pa.at[at], sent, x_r.at[i], beside)

    def x_send(b, c):
        i, at = b * G_PARTS + c, g_slice(b, c)
        p_copy(i).wait_recv()
        pb[at, :] = (pf[at, :] + pb[at, :].astype(f32)).astype(bf16)
        x_copy(b, c).start()

    def p_step(k, carry):
        b, half = near_block(blocks - 1 - k // 2), lax.rem(k, 2)
        j = b * 2 + half
        at = pl.ds(pl.multiple_of(j * tile, tile), tile)
        part = pf[at, :] + lax.dot_general(
            x[rows:both, at], back[rows:both, :], ROWS_TO_COLS, preferred_element_type=f32
        )
        pf[at, :] = part

        @pl.when(carries)
        def _():
            pa[at, :] = part.astype(bf16)
            for c in range(tile // g_rows):
                p_copy(j * (tile // g_rows) + c).start()

        return carry

    lax.fori_loop(0, columns // tile, p_step, 0)

    @pl.when(carries & relays)
    def _():
        w_forward(early, 2)

    @pl.when(carries & inside)
    def _():
        side_forward(side_block(jnp.where(entry, 1, 0)))

    @pl.when(carries & entry)
    def _():
        for c in range(2, W_PARTS):
            w_inward(c)

    def w_step(n):
        b, c = w_part(n)
        ahead = jnp.where(border, n + 3, n)
        next_b, next_c = w_part(ahead)
        main = next_c < W_MAIN
        forwarded = (inside & (z == z0 + next_b)) | ((relays & main | inside & (next_c < 2)) & (next_b == early))

        @pl.when(carries & (ahead < w_steps) & jnp.logical_not(forwarded))
        def _():
            w_forward(next_b, next_c)

        @pl.when(jnp.logical_not(carries))
        def _():
            for h in range(W_FINE):
                w_load(b, c, h).wait()

        at = w_slice(b, c)
        for which, recv in ((image_rows, ci_r), (text_rows, ct_r)):
            y[which, :] += jnp.dot(x[which, at], w[at, :], preferred_element_type=f32)

            @pl.when(n == w_steps - 1)
            def _():
                c1_send(which, recv)

        last, kept = n == w_steps - 1, w_steps - 3
        start = jnp.where(last, kept, n)
        lax.fori_loop(start, jnp.where((n < kept) | last, n + 1, n), grad_step, 0)

    def grad_step(n, carry):
        at = w_slice(*w_part(n))
        grads = lax.dot_general(back[...], w[at, :], COLS_TO_COLS, preferred_element_type=f32).astype(bf16)
        text_out[:, at] = grads[:rows]
        image_out[:, at] = grads[rows:]
        return carry

    def c1(i, source, which, recv):
        q, device = head_of(i)
        return remote(yb.at[q, which], yr.at[source, which], small, recv, device)

    def c1_all(which, recv):
        at = pl.ds(0, tp - 1)
        return remote(yb.at[at, which], yr.at[at, which], small, recv, peer)

    def c1_send(which, recv):
        for q in range(tp):
            yb[q, which, :] = y[which, q * cols : (q + 1) * cols].astype(bf16)
        for i in range(1, tp):
            c1(i, t, which, recv).start()

    def c2(i):
        v, device = unit_of(i)
        return remote(c2_src.at[slot_rows(v)], c2_dst.at[slot_rows(me)], small, c2_r, device)

    def c2_all():
        at = pl.ds(0, (units - 1) * capacity)
        return remote(c2_src.at[at], c2_dst.at[at], small, c2_r, peer)

    def c2_send():
        total = y[image_rows, my_cols]
        c1_all(image_rows, ci_r).wait_recv()
        for i in range(1, tp):
            q = head_of(i)[0]
            total = total + yr[q, image_rows, :].astype(f32)
        c2_src[...] = jnp.dot(pick_t[...], total.astype(bf16), preferred_element_type=f32).astype(bf16)
        for i in range(1, units):
            c2(i).start()
        c2_dst[slot_rows(me), :] = c2_src[slot_rows(me), :]

    def home(b, c):
        return jnp.where(c < G_MAIN, z0, other_z0) + b

    def chain_copies(b, c):
        i, at = b * G_PARTS + c, g_slice(b, c)
        return (
            (z > home(b, c), remote(chain.at[at], above.at[at], sent, chain_r.at[i], (g, z - 1, t))),
            (z < home(b, c), remote(chain.at[at], below.at[at], sent, chain_r.at[i], (g, z + 1, t))),
        )

    def landing(c):
        return landed.at[pl.ds(pl.multiple_of(c * g_rows, g_rows), g_rows)]

    def result_copy(b, c, q):
        return remote(
            chain.at[g_slice(b, c), q * cols : (q + 1) * cols], landing(c), sent, g_r, (1 - g, z, q)
        )

    def g_step(m):
        own = jnp.where(inside, m >= blocks * (G_PARTS - G_MAIN), m < blocks * G_MAIN)
        own_m = jnp.where(inside, m - blocks * (G_PARTS - G_MAIN), m)
        other_m = jnp.where(inside, m, m - blocks * G_MAIN)
        b = jnp.where(own, near_block(blocks - 1 - own_m // G_MAIN), far_other(other_m // (G_PARTS - G_MAIN)))
        c = jnp.where(own, lax.rem(own_m, G_MAIN), G_MAIN + lax.rem(other_m, G_PARTS - G_MAIN))
        i, at, zb = b * G_PARTS + c, g_slice(b, c), home(b, c)

        @pl.when(own)
        def _():
            p_copy(i).wait_recv()
            pf[at, :] += pb[at, :].astype(f32)

        @pl.when(jnp.logical_not(own))
        def _():
            x_copy(b, c).wait_recv()
            pf[at, :] = pa[at, :].astype(f32)

        from_above, from_below = (z >= zb) & (z < fsdp - 1), (z <= zb) & (z > 0)
        pair = pl.ds(0, 2 * g_rows)

        @pl.when(from_above & from_below)
        def _():
            remote(chain.at[pair], above.at[pair], sent, chain_r.at[i], peer).wait_recv()

        @pl.when(from_above != from_below)
        def _():
            remote(chain.at[at], above.at[at], sent, chain_r.at[i], peer).wait_recv()

        for arrives, source in ((from_above, above), (from_below, below)):

            @pl.when(arrives)
            def _():
                pf[at, :] += source[at, :].astype(f32)

        chain[at, :] = pf[at, :].astype(bf16)
        for condition, copy in chain_copies(b, c):
            pl.when(condition)(copy.start)

        @pl.when(z == zb)
        def _():
            for q in range(tp):
                result_copy(b, c, q).start()

    ratio = g_steps // w_steps
    half = w_steps // 2
    mains, sides = blocks * G_MAIN, G_PARTS - G_MAIN
    lead = mains // ratio
    turns = len(FAR_STEPS) - 1
    sums = jnp.logical_not(carries)
    late = sums & far_end
    w_at = jnp.where(late, lead, 0)
    c2_at = jnp.where(far_end, lead + w_steps - 1, jnp.where(entry, w_steps + 2, w_steps + 1))
    c2_at = jnp.where(carries, w_steps - 1, c2_at)
    spot = mains - ratio

    def in_turn(m):
        moved = jnp.where(m < spot + sides, m - spot + mains, jnp.where(m < mains + sides, m - sides, m))
        group, place = m // (2 * ratio), lax.rem(m, 2 * ratio)
        woven = jnp.where(place < ratio, blocks * sides, -ratio) + group * ratio + place
        woven = jnp.where(m < 2 * blocks * sides, woven, m)
        return jnp.where(border & (m >= spot), moved, jnp.where(entry, woven, m))

    def turn(s, carry):
        n = s - w_at
        done = look_up(FAR_STEPS, s), look_up(FAR_STEPS, s + 1)
        for kind, steps in ((border, BORDER_STEPS), (entry, ENTRY_STEPS), (inside & jnp.logical_not(entry), LAST_STEPS)):
            done = tuple(jnp.where(kind, look_up(steps, s + i), done[i]) for i in range(2))
        g_lo, g_hi = done

        x_at = jnp.where(late, jnp.where(s == 1, 0, jnp.where(s == lead // 2 + 1, 1, -1)), jnp.where(s < blocks, s, -1))

        @pl.when(carries & inside & jnp.logical_not(entry) & (s == half))
        def _():
            side_forward(side_block(1))

        @pl.when(sums)
        def _():
            lax.fori_loop(g_lo, g_hi, lambda m, unused: (g_step(in_turn(m)), unused)[1], 0)

        @pl.when(sums & (x_at >= 0))
        def _():
            lax.fori_loop(G_MAIN, G_PARTS, lambda c, unused: (x_send(near_block(blocks - 1 - x_at), c), unused)[1], 0)

        @pl.when((n >= 0) & (n < w_steps))
        def _():
            w_step(n)

        @pl.when(s == c2_at)
        def _():
            c2_send()

        return carry

    lax.fori_loop(0, turns, turn, 0)

    def all_sent(sem, size):
        at = pl.ds(0, size // (2 * key_cols))
        remote(pf.at[at], pf.at[at], sem, sem, peer).wait_send()

    part_size, chunk_size = w_rows * key_cols, g_rows * key_cols
    counts = ((far_end, 1), (border, 2 * W_MAIN + 2), (entry, 2 * W_MAIN + W_PARTS + 4), (inside & jnp.logical_not(entry), W_PARTS + 2))
    for kind, parts in counts:

        @pl.when(carries & kind)
        def _():
            all_sent(sent, parts * part_size)

    @pl.when(carries)
    def _():
        all_sent(shared, 2 * columns * key_cols)

    total = y[text_rows, my_cols]
    c1_all(text_rows, ct_r).wait_recv()
    for i in range(1, tp):
        total = total + yr[head_of(i)[0], text_rows, :].astype(f32)
    c2_all().wait_recv()
    placed = lax.dot_general(place_t[...], c2_dst[...], ROWS_TO_COLS, preferred_element_type=f32)
    projected = jnp.where(is_img[...] > 0.5, placed, total) + bias_ref[...]
    for s in range(rows // LENGTH):
        values = projected[s * LENGTH : (s + 1) * LENGTH]
        turned = values * cosv[...] + pltpu.roll(values, HALF, 1) * sinv[...]
        keys_out[s * LENGTH : (s + 1) * LENGTH, :] = jnp.where(live(s), turned, 0.0).astype(bf16)

    remote(landed, landed, sent, g_r, peer).wait_recv()
    wgrad_out[...] = landed[...].astype(f32) * (1.0 / rows)

    @pl.when(sums)
    def _():
        all_sent(sent, (g_steps + blocks * sides) * chunk_size)

    all_sent(small, 2 * (units - 1) * capacity * cols + (tp - 1) * (both + images) * cols)


def write_kernel(*refs):
    count = (len(refs) - 1) // 2
    copies = [pltpu.make_async_copy(refs[i], refs[count + i], refs[-1].at[i]) for i in range(count)]
    for copy in copies:
        copy.start()
    for copy in copies:
        copy.wait()


def rotary_tables():
    frequency = ROPE_BASE ** (-(np.arange(HALF, dtype=np.float64) * 2.0) / HEAD_DIM)
    table = np.arange(LENGTH, dtype=np.float64)[:, None] * frequency[None, :]
    cosine, sine = np.cos(table), np.sin(table)
    return (
        np.concatenate([cosine, cosine], axis=1).astype(np.float32),
        np.concatenate([-sine, sine], axis=1).astype(np.float32),
    )


def fits(groups, fsdp, tp, rows, head_cols, block):
    units = groups * fsdp
    if groups != 2 or units % tp or head_cols != HEAD_DIM or rows % LENGTH:
        return False
    blocks = units // tp
    return blocks == 2 and fsdp == 2 * blocks and tp % 2 == 0 and block % (G_PARTS * HEAD_DIM) == 0 and (rows // units) % 16 == 0


def per_device(
    text_embeds, image_embeds, key_weight, key_bias, key_cot, image_owner, image_slot, seq_lengths
):
    groups, fsdp, tp = lax.axis_size("group"), lax.axis_size("fsdp"), lax.axis_size("tp")
    rows, columns = text_embeds.shape
    images = image_embeds.shape[0]
    cols = key_bias.shape[0]
    block = key_weight.shape[0]
    if not fits(groups, fsdp, tp, rows, cols, block):
        return per_device_plain(
            text_embeds, image_embeds, key_weight, key_bias, key_cot, image_owner, image_slot, seq_lengths
        )
    units = groups * fsdp
    capacity = rows // units
    slots = units * capacity
    both, key_cols = rows + images, cols * tp
    blocks = units // tp
    w_steps, g_steps = blocks * W_PARTS, blocks * G_PARTS
    cosine, sine = rotary_tables()
    bf16, f32 = jnp.bfloat16, jnp.float32
    hbm = pl.BlockSpec(memory_space=pltpu.HBM)
    vmem = pl.BlockSpec(memory_space=pltpu.VMEM)
    dma = lambda n: pltpu.SemaphoreType.DMA((n,))
    one = pltpu.SemaphoreType.DMA
    shapes = (
        jax.ShapeDtypeStruct((rows, cols), bf16),
        jax.ShapeDtypeStruct((rows, columns), bf16),
        jax.ShapeDtypeStruct((images, columns), bf16),
        jax.ShapeDtypeStruct((block, cols), f32),
    )
    operands = (
        text_embeds, image_embeds, key_weight, key_bias.reshape(1, -1), key_cot,
        image_owner.reshape(1, -1), image_slot.reshape(1, -1), seq_lengths.reshape(1, -1), jnp.asarray(cosine), jnp.asarray(sine),
    )
    held = pl.pallas_call(
        functools.partial(fused_kernel, groups, fsdp, tp, capacity),
        out_shape=tuple(pltpu.VMEM(leaf.shape, leaf.dtype) for leaf in shapes),
        in_specs=[hbm] * 10,
        out_specs=(vmem, vmem, vmem, vmem),
        scratch_shapes=[
            pltpu.VMEM((1, cols), f32),
            pltpu.VMEM((1, images), jnp.int32),
            pltpu.VMEM((1, rows), jnp.int32),
            pltpu.VMEM((1, seq_lengths.shape[0]), jnp.int32),
            pltpu.VMEM((both, columns), bf16),
            pltpu.VMEM((columns, key_cols), bf16),
            pltpu.VMEM((rows, key_cols), bf16),
            pltpu.VMEM((LENGTH, cols), f32),
            pltpu.VMEM((LENGTH, cols), f32),
            pltpu.VMEM((both, key_cols), bf16),
            pltpu.VMEM((slots, images), bf16),
            pltpu.VMEM((slots, rows), bf16),
            pltpu.VMEM((rows, cols), f32),
            pltpu.VMEM((slots, cols), bf16),
            pltpu.VMEM((slots, cols), bf16),
            pltpu.VMEM((images, cols), bf16),
            pltpu.VMEM((columns, key_cols), f32),
            pltpu.VMEM((columns, key_cols), bf16),
            pltpu.VMEM((columns, key_cols), bf16),
            pltpu.VMEM((columns, key_cols), bf16),
            pltpu.VMEM((columns, key_cols), bf16),
            pltpu.VMEM((columns, key_cols), bf16),
            pltpu.VMEM((both, key_cols), f32),
            pltpu.VMEM((tp, both, cols), bf16),
            pltpu.VMEM((tp, both, cols), bf16),
            pltpu.VMEM((slots, cols), bf16),
            pltpu.VMEM((slots, cols), bf16),
            pltpu.VMEM((block, cols), bf16),
            pltpu.VMEM((blocks, block // W_PARTS, key_cols), bf16),
            dma(9), dma(w_steps * W_FINE), one, one, one, one, one, one, one, one, one,
            dma(g_steps), dma(g_steps), dma(blocks * (G_PARTS - G_MAIN)), dma(blocks * W_FINE),
        ],
        compiler_params=pltpu.CompilerParams(
            collective_id=0, has_side_effects=True, vmem_limit_bytes=44 * 1024 * 1024
        ),
        name="fused",
    )(*(pltpu.with_memory_space_constraint(operand, pltpu.HBM) for operand in operands))
    return pl.pallas_call(
        write_kernel,
        out_shape=shapes,
        in_specs=[vmem] * 4,
        out_specs=(pl.BlockSpec(memory_space=pl.ANY),) * 4,
        scratch_shapes=[dma(4)],
        compiler_params=pltpu.CompilerParams(vmem_limit_bytes=4 * 1024 * 1024),
        name="write",
    )(*held)


def solution(mesh):
    in_specs = (
        P(("group", "fsdp"), "tp"),
        P(("group", "fsdp"), "tp"),
        P(("group", "fsdp"), None),
        P("tp"),
        P(("group", "fsdp"), None),
        P(("group", "fsdp")),
        P(("group", "fsdp")),
        P(("group", "fsdp")),
    )
    out_specs = (
        P(("group", "fsdp"), "tp"),
        P(("group", "fsdp"), "tp"),
        P(("group", "fsdp"), "tp"),
        P(("group", "fsdp"), "tp"),
    )
    return jax.shard_map(
        per_device, mesh=mesh, in_specs=in_specs, out_specs=out_specs, check_vma=False
    )
```

```python
import functools

import jax
import jax.numpy as jnp
import numpy as np
from jax import lax
from jax.experimental import pallas as pl
from jax.experimental.pallas import tpu as pltpu
from jax.sharding import PartitionSpec as P

HEAD_DIM = 128
LENGTH = 256


ROPE_BASE = 1000000.0


def angles(row_total):
    position = (jnp.arange(row_total, dtype=jnp.int32) % LENGTH).astype(jnp.float32)
    frequency = ROPE_BASE ** (-(jnp.arange(HEAD_DIM // 2, dtype=jnp.float32) * 2.0) / HEAD_DIM)
    angle_table = position[:, None] * frequency[None, :]
    return (jnp.cos(angle_table), jnp.sin(angle_table))


def rotate(values, cosine, sine, direction):
    row_total = values.shape[0]
    by_head = values.reshape(row_total, -1, HEAD_DIM)
    half_dim = HEAD_DIM // 2
    front_half = by_head[..., :half_dim]
    second = by_head[..., half_dim:]
    cos_part = cosine[:, None, :]
    sin_part = direction * sine[:, None, :]
    rotated = jnp.concatenate(
        [front_half * cos_part - second * sin_part, second * cos_part + front_half * sin_part],
        axis=-1,
    )
    return rotated.reshape(row_total, -1)


def send_slots(owners, unit_count, capacity):
    onehot_marks = (owners[:, None] == jnp.arange(unit_count, dtype=jnp.int32)[None, :]).astype(
        jnp.int32
    )
    before = jnp.cumsum(onehot_marks, axis=0) - onehot_marks
    owner_rank = jnp.sum(before * onehot_marks, axis=1)
    return owners * capacity + owner_rank


def share_kernel(text_ref, image_ref, back_ref, image_back_ref, out_ref):
    contract = (((0,), (0,)), ((), ()))
    part = lax.dot_general(
        text_ref[...], back_ref[...], contract, preferred_element_type=jnp.float32
    ) + lax.dot_general(
        image_ref[...], image_back_ref[...], contract, preferred_element_type=jnp.float32
    )
    part = part.astype(out_ref.dtype)
    width = out_ref.shape[2]
    for head in range(out_ref.shape[0]):
        out_ref[head] = part[:, head * width : (head + 1) * width]


def weight_shares(text, image, back, image_back, head_cols):
    columns = text.shape[1]
    heads = back.shape[1] // head_cols
    tile = min(512, columns)
    return pl.pallas_call(
        share_kernel,
        grid=(columns // tile,),
        in_specs=[
            pl.BlockSpec((text.shape[0], tile), lambda i: (0, i)),
            pl.BlockSpec((image.shape[0], tile), lambda i: (0, i)),
            pl.BlockSpec(back.shape, lambda i: (0, 0)),
            pl.BlockSpec(image_back.shape, lambda i: (0, 0)),
        ],
        out_specs=pl.BlockSpec((heads, tile, head_cols), lambda i: (0, i, 0)),
        out_shape=jax.ShapeDtypeStruct((heads, columns, head_cols), jnp.bfloat16),
        cost_estimate=pl.CostEstimate(
            flops=2 * (text.size + image.size) * back.shape[1],
            bytes_accessed=2 * (text.size + image.size + columns * back.shape[1]),
            transcendentals=0,
        ),
    )(text, image, back, image_back)


def project_kernel(text_ref, image_ref, weight_ref, out_ref):
    step = pl.program_id(0)
    last = pl.num_programs(0) - 1
    rows = jnp.where(step == last, image_ref[...], text_ref[...])
    part = jnp.dot(rows, weight_ref[...], preferred_element_type=jnp.float32).astype(out_ref.dtype)
    width = out_ref.shape[2]
    for head in range(out_ref.shape[0]):
        out_ref[head] = part[:, head * width : (head + 1) * width]


def projection_parts(text, image, weight, head_cols):
    heads = weight.shape[1] // head_cols
    tile, columns = image.shape
    text_tiles = text.shape[0] // tile
    return pl.pallas_call(
        project_kernel,
        grid=(text_tiles + 1,),
        in_specs=[
            pl.BlockSpec((tile, columns), lambda i: (jnp.minimum(i, text_tiles - 1), 0)),
            pl.BlockSpec((tile, columns), lambda i: (0, 0)),
            pl.BlockSpec(weight.shape, lambda i: (0, 0)),
        ],
        out_specs=pl.BlockSpec((heads, tile, head_cols), lambda i: (0, i, 0)),
        out_shape=jax.ShapeDtypeStruct((heads, text.shape[0] + tile, head_cols), jnp.bfloat16),
        cost_estimate=pl.CostEstimate(
            flops=2 * (text.size + image.size) * weight.shape[1],
            bytes_accessed=2 * (text.size + image.size + weight.size),
            transcendentals=0,
        ),
    )(text, image, weight)


def spread(piece, axis):
    count = lax.axis_size(axis)
    copies = jnp.broadcast_to(piece[None], (count,) + piece.shape)
    got = lax.all_to_all(copies, axis, split_axis=0, concat_axis=0, tiled=True)
    return got.reshape((count * piece.shape[0],) + piece.shape[1:])


def shifted(values, axis, step):
    count = lax.axis_size(axis)
    return lax.ppermute(values, axis, [(i, (i + step) % count) for i in range(count)])


def exchange_sum(blocks, axis):
    count = lax.axis_size(axis)
    me = lax.axis_index(axis)
    total = lax.dynamic_index_in_dim(blocks, me, 0, keepdims=False).astype(jnp.float32)
    for step in range(1, count):
        block = lax.dynamic_index_in_dim(blocks, (me + step) % count, 0, keepdims=False)
        total = total + shifted(block, axis, step).astype(jnp.float32)
    return total


def share_rows(piece, axis):
    count = lax.axis_size(axis)
    me = lax.axis_index(axis)
    rows = piece.shape[0]
    full = jnp.zeros((count * rows,) + piece.shape[1:], piece.dtype)
    full = lax.dynamic_update_slice_in_dim(full, piece, me * rows, 0)
    for step in range(1, count):
        source = (me + count - step) % count
        full = lax.dynamic_update_slice_in_dim(full, shifted(piece, axis, step), source * rows, 0)
    return full


def per_device_plain(
    text_embeds, image_embeds, key_weight, key_bias, key_cot, image_owner, image_slot, seq_lengths
):
    row_count, columns = text_embeds.shape
    image_count = image_embeds.shape[0]
    units = ("group", "fsdp")
    core_count = lax.axis_size("group")
    fsdp_count = lax.axis_size("fsdp")
    tp_count = lax.axis_size("tp")
    unit_count = core_count * fsdp_count
    capacity = row_count // unit_count
    slot_count = unit_count * capacity
    head_cols = key_bias.shape[0]
    key_cols = head_cols * tp_count
    weight_block = key_weight.shape[0]
    halves = unit_count // tp_count
    tp_index = lax.axis_index("tp")

    position = jnp.arange(row_count, dtype=jnp.int32)
    seq_ids = position // LENGTH
    seq_marks = seq_ids[:, None] == jnp.arange(seq_lengths.shape[0], dtype=jnp.int32)[None, :]
    live_limit = jnp.sum(jnp.where(seq_marks, seq_lengths[None, :], 0), axis=1)
    live_mask = (position % LENGTH < live_limit).astype(jnp.float32)
    cosine, sine = angles(row_count)
    masked = key_cot.astype(jnp.float32) * live_mask[:, None]
    rotated_back = rotate(masked, cosine, sine, -1.0).astype(jnp.bfloat16)
    is_image = image_slot >= 0
    text_back = jnp.where(is_image[:, None], jnp.zeros_like(rotated_back), rotated_back)

    slot_ids = jnp.arange(slot_count, dtype=jnp.int32)
    place = (image_slot[:, None] == slot_ids[None, :]).astype(jnp.bfloat16)
    returning = lax.dot_general(
        place, rotated_back, (((0,), (0,)), ((), ())), preferred_element_type=jnp.float32
    ).astype(jnp.bfloat16)
    returned = lax.all_to_all(
        returning.reshape(unit_count, capacity, key_cols), units, split_axis=0, concat_axis=0,
        tiled=True,
    ).reshape(slot_count, key_cols)
    slots_out = send_slots(image_owner, unit_count, capacity)
    pick = (slots_out[:, None] == slot_ids[None, :]).astype(jnp.bfloat16)
    image_back = jnp.dot(pick, returned, preferred_element_type=jnp.float32).astype(jnp.bfloat16)

    piece_rows = weight_block // tp_count
    own_piece = lax.dynamic_slice_in_dim(key_weight, tp_index * piece_rows, piece_rows, 0)
    moves = []
    for unit in range(unit_count):
        for part in range(tp_count):
            target = (unit % halves) * tp_count + part
            moves.append((unit * tp_count + part, target * tp_count + unit // halves))
    own_piece = lax.ppermute(own_piece, units + ("tp",), moves)
    chip_rows = spread(own_piece, "fsdp")

    shares = weight_shares(text_embeds, image_embeds, text_back, image_back, head_cols)
    shares = shares.reshape(core_count, fsdp_count, weight_block, head_cols)
    shares = exchange_sum(shares, "group").astype(jnp.bfloat16)
    shares, chip_rows = lax.optimization_barrier((shares, chip_rows))
    shares = lax.all_to_all(shares, "fsdp", split_axis=0, concat_axis=0, tiled=True)
    weight_grad = jnp.sum(shares.astype(jnp.float32), axis=0) / row_count
    returns = []
    for unit in range(unit_count):
        for part in range(tp_count):
            holder = (unit % halves) + part * halves
            returns.append((holder * tp_count + unit // halves, unit * tp_count + part))
    weight_grad = lax.ppermute(weight_grad, units + ("tp",), returns)

    weight_rows = share_rows(chip_rows, "group")
    both = projection_parts(text_embeds, image_embeds, weight_rows, head_cols)
    both = exchange_sum(both, "tp")
    image_proj = both[row_count:].astype(jnp.bfloat16)
    outgoing = lax.dot_general(
        pick, image_proj, (((0,), (0,)), ((), ())), preferred_element_type=jnp.float32
    ).astype(jnp.bfloat16)
    received = lax.all_to_all(
        outgoing.reshape(unit_count, capacity, head_cols), units, split_axis=0, concat_axis=0,
        tiled=True,
    ).reshape(slot_count, head_cols)
    placed = jnp.dot(place, received, preferred_element_type=jnp.float32)
    projected = jnp.where(is_image[:, None], placed, both[:row_count]) + key_bias
    key_rows = (rotate(projected, cosine, sine, 1.0) * live_mask[:, None]).astype(jnp.bfloat16)

    contract = (((1,), (1,)), ((), ()))
    text_grad = lax.dot_general(
        text_back, weight_rows, contract, preferred_element_type=jnp.float32
    ).astype(jnp.bfloat16)
    image_grad = lax.dot_general(
        image_back, weight_rows, contract, preferred_element_type=jnp.float32
    ).astype(jnp.bfloat16)
    return (key_rows, text_grad, image_grad, weight_grad)


MESH = pl.DeviceIdType.MESH
HALF = HEAD_DIM // 2
ROWS_TO_COLS = (((0,), (0,)), ((), ()))
COLS_TO_COLS = (((1,), (1,)), ((), ()))
W_PARTS = 4
W_MAIN = 3
W_FINE = 2
W_NEAR_OR_FAR = (0, 0, 0, 1, 0, 1, 1, 1)
W_PART_AT = (0, 1, 2, 0, 3, 1, 3, 2)
FAR_LEAD = 4
FAR_STEPS = (0, 3, 6, 9, 11, 11, 11, 11, 11, 14, 14, 14, 14, 16)
BORDER_STEPS = (0, 0, 0, 0, 2, 4, 6, 8, 8, 13, 13, 16, 16, 16)
BORDER_SPOT = 8
ENTRY_STEPS = (0, 0, 0, 0, 0, 0, 0, 0, 0, 4, 8, 14, 16, 16)
ENTRY_ORDER = (5, 6, 0, 1, 7, 8, 2, 3, 9, 10, 4, 11, 12, 13, 14, 15)
LAST_STEPS = (0, 0, 0, 0, 2, 4, 6, 9, 10, 12, 14, 16, 16, 16)
G_PARTS = 8
G_SIDES = (3, 2)


def fused_kernel(
    groups, fsdp, tp, capacity,
    text_ref, image_ref, weight_ref, bias_hbm, cot_ref, owner_hbm, slot_hbm, lens_hbm, cos_ref, sin_ref,
    keys_out, text_out, image_out, wgrad_out,
    bias_ref, owner_ref, slot_ref, lens_ref, x, w, cot, cosv, sinv, back, pick_t, place_t, is_img,
    d1_src, d1_dst, d2_src, pf, pa, pb, chain, above, below, y, yb, yr, c2_src, c2_dst, landed, side,
    ld, w_recv, sent, shared, small, d1_r, d2_r, ci_r, ct_r, c2_r, g_r, p_r, chain_r, x_r, h_r,
):
    f32, bf16 = jnp.float32, jnp.bfloat16
    g, z, t = lax.axis_index("group"), lax.axis_index("fsdp"), lax.axis_index("tp")
    units = groups * fsdp
    me = g * fsdp + z
    rows, images = text_ref.shape[0], image_ref.shape[0]
    both = rows + images
    columns = text_ref.shape[1]
    slots = units * capacity
    cols = bias_ref.shape[1]
    block = weight_ref.shape[0]
    blocks = units // tp
    key_cols = tp * cols
    w_rows, g_rows = block // W_PARTS, block // G_PARTS
    w_steps, g_steps = blocks * W_PARTS, blocks * G_PARTS
    first = t * blocks
    carrier, z0 = first // fsdp, lax.rem(first, fsdp)
    carries = g == carrier
    inside = (z >= z0) & (z < z0 + blocks)
    far_end = jnp.logical_not(inside) & ((z == 0) | (z == fsdp - 1))
    my_cols = pl.ds(pl.multiple_of(t * cols, cols), cols)
    peer = (1 - g, z, t)
    other = lax.bitwise_xor(t, 1)
    beside = (g, z, other)
    other_z0 = fsdp - blocks - z0
    upward = z0 > 0
    entry = jnp.where(upward, z == z0, z == z0 + blocks - 1)
    border = jnp.where(upward, z == z0 - 1, z == z0 + blocks)
    relays = entry | border

    def near_block(k):
        within = lax.rem(z - z0 + k + blocks, blocks)
        return jnp.where(inside, within, jnp.where(z < z0, k, blocks - 1 - k))

    def far_other(k):
        within = lax.rem(z - other_z0 + blocks - 1 - k + blocks, blocks)
        return jnp.where(inside, jnp.where(upward, k, blocks - 1 - k), within)

    def look_up(table, n):
        found = table[0]
        for i in range(1, len(table)):
            found = jnp.where(n == i, table[i], found)
        return found

    def w_part(n):
        return near_block(look_up(W_NEAR_OR_FAR, n)), look_up(W_PART_AT, n)

    def unit_of(i):
        far = units - i
        core, plane = lax.bitwise_xor(g, far % groups), lax.bitwise_xor(z, far // groups)
        return core * fsdp + plane, (core, plane, t)

    def head_of(i):
        q = lax.bitwise_xor(t, tp - 1 if i == 1 else i - 1)
        return q, (g, z, q)

    def remote(src, dst, send, recv, device):
        return pltpu.make_async_remote_copy(
            src_ref=src, dst_ref=dst, send_sem=send, recv_sem=recv, device_id=device, device_id_type=MESH
        )

    barrier = pltpu.get_barrier_semaphore()
    for i in range(1, units):
        pl.semaphore_signal(barrier, inc=1, device_id=unit_of(i)[1], device_id_type=MESH)
    for i in range(1, tp):
        q = head_of(i)[0]
        for core in range(groups):
            pl.semaphore_signal(barrier, inc=1, device_id=(core, z, q), device_id_type=MESH)

    pairs = (
        (slot_hbm, slot_ref),
        (cot_ref, cot),
        (cos_ref, cosv),
        (sin_ref, sinv),
        (lens_hbm, lens_ref),
        (owner_hbm, owner_ref),
        (bias_hbm, bias_ref),
        (text_ref, x.at[pl.ds(0, rows)]),
        (image_ref, x.at[pl.ds(rows, images)]),
    )
    loads = [pltpu.make_async_copy(source, target, ld.at[i]) for i, (source, target) in enumerate(pairs)]
    for load in loads[:5]:
        load.start()

    def w_slice(b, c):
        return pl.ds(pl.multiple_of(b * block + c * w_rows, w_rows), w_rows)

    fine = w_rows // W_FINE

    def w_fine(b, c, h):
        return pl.ds(pl.multiple_of(b * block + c * w_rows + h * fine, fine), fine)

    def w_index(b, c, h):
        return (b * W_PARTS + c) * W_FINE + h

    def w_load(b, c, h):
        source = weight_ref.at[pl.ds(pl.multiple_of(c * w_rows + h * fine, fine), fine)]
        return pltpu.make_async_copy(source, w.at[w_fine(b, c, h)], w_recv.at[w_index(b, c, h)])

    def side_rows(b, h):
        return side.at[b, pl.ds(h * fine, fine)]

    def side_load(b, h):
        source = weight_ref.at[pl.ds(W_MAIN * w_rows + h * fine, fine)]
        return pltpu.make_async_copy(source, side_rows(b, h), h_r.at[b * W_FINE + h])

    @pl.when(carries & inside)
    def _():
        for c in range(W_PARTS):
            for h in range(W_FINE):
                w_load(z - z0, c, h).start()

    @pl.when(carries & jnp.logical_not(inside))
    def _():
        for h in range(W_FINE):
            side_load(z - other_z0, h).start()

    for load in loads[5:]:
        load.start()

    loads[0].wait()
    slot_ids = lax.broadcasted_iota(jnp.int32, (slots, rows), 0)
    place_t[...] = jnp.where(slot_ids == slot_ref[...], 1.0, 0.0).astype(bf16)
    row_ids = lax.broadcasted_iota(jnp.int32, (LENGTH, HEAD_DIM), 0)

    def live(s):
        return row_ids < lens_ref[0:1, s : s + 1]

    def rotated_back(s, at):
        span = pl.ds(s * LENGTH, LENGTH)
        values = jnp.where(live(s), cot[span, at].astype(f32), 0.0)
        return values * cosv[...] - pltpu.roll(values, HALF, 1) * sinv[...]

    for load in loads[1:5]:
        load.wait()
    mine = jnp.concatenate([rotated_back(s, my_cols) for s in range(rows // LENGTH)], axis=0).astype(bf16)
    d1_src[...] = jnp.dot(place_t[...], mine, preferred_element_type=f32).astype(bf16)

    pl.semaphore_wait(barrier, units - 1 + groups * (tp - 1))

    def slot_rows(v):
        return pl.ds(pl.multiple_of(v * capacity, capacity), capacity)

    def d1(i):
        v, device = unit_of(i)
        return remote(d1_src.at[slot_rows(v)], d1_dst.at[slot_rows(me)], small, d1_r, device)

    def d1_all():
        at = pl.ds(0, (units - 1) * capacity)
        return remote(d1_src.at[at], d1_dst.at[at], small, d1_r, peer)

    for i in range(1, units):
        d1(i).start()
    d1_dst[slot_rows(me), :] = d1_src[slot_rows(me), :]

    def w_send(b, c, h, to):
        at = w_fine(b, c, h)
        return remote(w.at[at], w.at[at], sent, w_recv.at[w_index(b, c, h)], to)

    def w_share(b, c, h):
        at = w_fine(b, c, h)
        return remote(w.at[at], w.at[at], shared, w_recv.at[w_index(b, c, h)], peer)

    def w_routes(b, c, h):
        up = (z >= z0 + b) & (z < fsdp - 1) & ((c < W_MAIN) | (z + 1 < z0 + blocks))
        down = (z <= z0 + b) & (z > 0) & ((c < W_MAIN) | (z > z0))
        return ((up, w_send(b, c, h, (g, z + 1, t))), (down, w_send(b, c, h, (g, z - 1, t))))

    def w_inward(c):
        b = z - z0
        for h in range(W_FINE):
            pl.when(upward)(w_send(b, c, h, (g, z + 1, t)).start)
            pl.when(jnp.logical_not(upward))(w_send(b, c, h, (g, z - 1, t)).start)

    def side_routes(b, h):
        step = jnp.where(upward, 1, -1)
        i, at = b * W_FINE + h, w_fine(b, W_MAIN, h)
        return (
            ((z + step >= 0) & (z + step < fsdp), remote(side_rows(b, h), side_rows(b, h), sent, h_r.at[i], (g, z + step, t))),
            (inside, remote(side_rows(b, h), w.at[at], sent, w_recv.at[w_index(b, W_MAIN, h)], beside)),
        )

    def side_forward(b):
        for h in range(W_FINE):
            side_load(b, h).wait()
            for condition, copy in side_routes(b, h):
                pl.when(condition)(copy.start)

    def side_block(k):
        return jnp.where(upward, blocks - 1 - k, k)

    def w_forward(b, c):
        held = entry & (z == z0 + b) & (c >= 2)
        for h in range(W_FINE):
            w_load(b, c, h).wait()
            for (condition, copy), inward in zip(w_routes(b, c, h), (upward, jnp.logical_not(upward))):
                pl.when(condition & jnp.logical_not(held & inward))(copy.start)
            w_share(b, c, h).start()

    early = jnp.where(inside, near_block(1), near_block(0))

    is_img[...] = lax.dot_general(
        place_t[...], jnp.ones((slots, cols), bf16), ROWS_TO_COLS, preferred_element_type=f32
    )
    y[...] = jnp.zeros_like(y)
    for s in range(rows // LENGTH):
        span = pl.ds(s * LENGTH, LENGTH)
        for h in range(tp):
            at = pl.ds(h * cols, cols)
            back[span, at] = jnp.where(is_img[span, :] > 0.5, 0.0, rotated_back(s, at)).astype(bf16)
    @pl.when(carries & inside)
    def _():
        lax.fori_loop(0, W_PARTS, lambda c, carry: (w_forward(z - z0, c), carry)[1], 0)

    @pl.when(carries & jnp.logical_not(inside))
    def _():
        side_forward(z - other_z0)

    loads[5].wait()
    image_units = lax.broadcasted_iota(jnp.int32, (units, images), 0)
    marks = jnp.where(image_units == owner_ref[...], 1.0, 0.0)
    before = jnp.where(
        lax.broadcasted_iota(jnp.int32, (images, images), 0) < lax.broadcasted_iota(jnp.int32, (images, images), 1),
        1.0,
        0.0,
    ).astype(bf16)
    counts = jnp.dot(marks.astype(bf16), before, preferred_element_type=f32)
    rank = jnp.sum(counts * marks, axis=0, keepdims=True).astype(jnp.int32)
    slots_out = owner_ref[...] * capacity + rank
    pick_t[...] = jnp.where(
        lax.broadcasted_iota(jnp.int32, (slots, images), 0) == slots_out, 1.0, 0.0
    ).astype(bf16)

    tile = block // 2
    loads[7].wait()

    def p_text(j, carry):
        at = pl.ds(pl.multiple_of(j * tile, tile), tile)
        pf[at, :] = lax.dot_general(
            x[0:rows, at], back[0:rows, :], ROWS_TO_COLS, preferred_element_type=f32
        )
        return carry

    lax.fori_loop(0, columns // tile, p_text, 0)

    d1_all().wait_recv()
    returned = lax.dot_general(pick_t[...], d1_dst[...], ROWS_TO_COLS, preferred_element_type=f32).astype(bf16)
    d2_src[...] = returned
    back[pl.ds(rows, images), my_cols] = returned

    def head_cols(q):
        return pl.ds(pl.multiple_of(q * cols, cols), cols)

    def d2(i, source):
        q, device = head_of(i)
        return remote(d2_src, back.at[pl.ds(rows, images), head_cols(source)], small, d2_r, device)

    text_rows, image_rows = pl.ds(0, rows), pl.ds(rows, images)

    def d2_all():
        at = pl.ds(0, tp - 1)
        return remote(yb.at[at, image_rows], yr.at[at, image_rows], small, d2_r, peer)

    for i in range(1, tp):
        d2(i, t).start()

    @pl.when(carries & (inside | border))
    def _():
        w_forward(early, 0)

    @pl.when(carries & relays)
    def _():
        side_forward(side_block(jnp.where(border, 1, 0)))

    d2_all().wait_recv()
    loads[6].wait()
    loads[8].wait()

    @pl.when(carries & (inside | border))
    def _():
        w_forward(early, 1)

    def p_copy(i):
        at = pl.ds(pl.multiple_of(i * g_rows, g_rows), g_rows)
        return remote(pa.at[at], pb.at[at], shared, p_r.at[i], peer)

    def g_slice(b, c):
        return pl.ds(pl.multiple_of(b * block + c * g_rows, g_rows), g_rows)

    def x_copy(b, c):
        i, at = b * G_SIDES[0] + c - (G_PARTS - G_SIDES[0]), g_slice(b, c)
        return remote(pb.at[at], pa.at[at], sent, x_r.at[i], beside)

    def x_send(b, c):
        i, at = b * G_PARTS + c, g_slice(b, c)
        p_copy(i).wait_recv()
        pb[at, :] = (pf[at, :] + pb[at, :].astype(f32)).astype(bf16)
        x_copy(b, c).start()

    def p_step(k, carry):
        b, half = near_block(blocks - 1 - k // 2), lax.rem(k, 2)
        j = b * 2 + half
        at = pl.ds(pl.multiple_of(j * tile, tile), tile)
        part = pf[at, :] + lax.dot_general(
            x[rows:both, at], back[rows:both, :], ROWS_TO_COLS, preferred_element_type=f32
        )
        pf[at, :] = part

        @pl.when(carries)
        def _():
            pa[at, :] = part.astype(bf16)
            for c in range(tile // g_rows):
                p_copy(j * (tile // g_rows) + c).start()

        return carry

    lax.fori_loop(0, columns // tile, p_step, 0)

    @pl.when(carries & relays)
    def _():
        w_forward(early, 2)

    @pl.when(carries & inside)
    def _():
        side_forward(side_block(jnp.where(entry, 1, 0)))

    @pl.when(carries & entry)
    def _():
        for c in range(2, W_PARTS):
            w_inward(c)

    def w_step(n):
        b, c = w_part(n)
        ahead = jnp.where(border, n + 3, n)
        next_b, next_c = w_part(ahead)
        main = next_c < W_MAIN
        forwarded = (inside & (z == z0 + next_b)) | ((relays & main | inside & (next_c < 2)) & (next_b == early))

        @pl.when(carries & (ahead < w_steps) & jnp.logical_not(forwarded))
        def _():
            w_forward(next_b, next_c)

        @pl.when(jnp.logical_not(carries))
        def _():
            for h in range(W_FINE):
                w_load(b, c, h).wait()

        last = n == w_steps - 1
        project(n, image_rows)

        @pl.when(last)
        def _():
            c1_send(image_rows, ci_r)

        def text_step(k, carry):
            project(k, text_rows)
            return carry

        lax.fori_loop(jnp.where(last, n - 1, n), jnp.where(n == w_steps - 2, n, n + 1), text_step, 0)
        kept = w_steps - 3
        lax.fori_loop(jnp.where(last, kept, n), jnp.where((n < kept) | last, n + 1, n), grad_step, 0)

        @pl.when(last)
        def _():
            c1_send(text_rows, ct_r)

    def project(n, which):
        at = w_slice(*w_part(n))
        y[which, :] += jnp.dot(x[which, at], w[at, :], preferred_element_type=f32)

    def grad_step(n, carry):
        at = w_slice(*w_part(n))
        grads = lax.dot_general(back[...], w[at, :], COLS_TO_COLS, preferred_element_type=f32).astype(bf16)
        text_out[:, at] = grads[:rows]
        image_out[:, at] = grads[rows:]
        return carry

    def c1(i, source, which, recv):
        q, device = head_of(i)
        return remote(yb.at[q, which], yr.at[source, which], small, recv, device)

    def c1_all(which, recv):
        at = pl.ds(0, tp - 1)
        return remote(yb.at[at, which], yr.at[at, which], small, recv, peer)

    def c1_send(which, recv):
        for q in range(tp):
            yb[q, which, :] = y[which, q * cols : (q + 1) * cols].astype(bf16)
        for i in range(1, tp):
            c1(i, t, which, recv).start()

    def c2(i):
        v, device = unit_of(i)
        return remote(c2_src.at[slot_rows(v)], c2_dst.at[slot_rows(me)], small, c2_r, device)

    def c2_all():
        at = pl.ds(0, (units - 1) * capacity)
        return remote(c2_src.at[at], c2_dst.at[at], small, c2_r, peer)

    def c2_send():
        total = y[image_rows, my_cols]
        c1_all(image_rows, ci_r).wait_recv()
        for i in range(1, tp):
            q = head_of(i)[0]
            total = total + yr[q, image_rows, :].astype(f32)
        c2_src[...] = jnp.dot(pick_t[...], total.astype(bf16), preferred_element_type=f32).astype(bf16)
        for i in range(1, units):
            c2(i).start()
        c2_dst[slot_rows(me), :] = c2_src[slot_rows(me), :]

    def chain_copies(i, at, zb):
        return (
            (z > zb, remote(chain.at[at], above.at[at], sent, chain_r.at[i], (g, z - 1, t))),
            (z < zb, remote(chain.at[at], below.at[at], sent, chain_r.at[i], (g, z + 1, t))),
        )

    def landing(c):
        return landed.at[pl.ds(pl.multiple_of(c * g_rows, g_rows), g_rows)]

    def result_copy(at, c, q):
        return remote(chain.at[at, q * cols : (q + 1) * cols], landing(c), sent, g_r, (1 - g, z, q))

    def g_step(m):
        own = jnp.where(inside, m >= all_sides, m < g_steps - all_sides)
        own_m = jnp.where(inside, m - all_sides, m)
        other_m = jnp.where(inside, m, m - (g_steps - all_sides))
        first_own = G_PARTS - jnp.where(inside & jnp.logical_not(entry), G_SIDES[0], G_SIDES[1])
        first_other = jnp.where(far_end, G_SIDES[0], G_SIDES[1])
        own_k, other_k = jnp.where(own_m >= first_own, 1, 0), jnp.where(other_m >= first_other, 1, 0)
        own_c = own_m - own_k * first_own
        other_c = G_PARTS + jnp.where(other_k == 1, other_m - all_sides, other_m - first_other)
        b = jnp.where(own, near_block(blocks - 1 - own_k), far_other(other_k))
        c = jnp.where(own, own_c, other_c)
        zb = jnp.where(own, z0, other_z0) + b
        slot_b = jnp.where(own, b, blocks - 1 - b)
        i, at = slot_b * G_PARTS + c, g_slice(slot_b, c)
        came_at = g_slice(b, c)

        @pl.when(own)
        def _():
            p_copy(i).wait_recv()
            pf[at, :] += pb[at, :].astype(f32)

        @pl.when(jnp.logical_not(own))
        def _():
            x_copy(b, c).wait_recv()
            pf[at, :] = pa[came_at, :].astype(f32)

        from_above, from_below = (z >= zb) & (z < fsdp - 1), (z <= zb) & (z > 0)
        pair = pl.ds(0, 2 * g_rows)

        @pl.when(from_above & from_below)
        def _():
            remote(chain.at[pair], above.at[pair], sent, chain_r.at[i], peer).wait_recv()

        @pl.when(from_above != from_below)
        def _():
            remote(chain.at[at], above.at[at], sent, chain_r.at[i], peer).wait_recv()

        for arrives, source in ((from_above, above), (from_below, below)):

            @pl.when(arrives)
            def _():
                pf[at, :] += source[at, :].astype(f32)

        chain[at, :] = pf[at, :].astype(bf16)
        for condition, copy in chain_copies(i, at, zb):
            pl.when(condition)(copy.start)

        @pl.when(z == zb)
        def _():
            for q in range(tp):
                result_copy(at, c, q).start()

    ratio = g_steps // w_steps
    half = w_steps // 2
    all_sides = sum(G_SIDES)
    mains = g_steps - all_sides
    lead = FAR_LEAD
    turns = len(FAR_STEPS) - 1
    sums = jnp.logical_not(carries)
    late = sums & far_end
    w_at = jnp.where(late, lead, 0)
    c2_at = jnp.where(far_end, lead + w_steps - 1, jnp.where(entry, w_steps + 2, w_steps + 1))
    c2_at = jnp.where(carries, w_steps - 1, c2_at)
    spot = BORDER_SPOT

    def in_turn(m):
        sides = G_SIDES[1]
        moved = jnp.where(m < spot + sides, m - spot + mains, jnp.where(m < mains + sides, m - sides, m))
        woven = look_up(ENTRY_ORDER, m)
        return jnp.where(border & (m >= spot), moved, jnp.where(entry, woven, m))

    def turn(s, carry):
        n = s - w_at
        done = look_up(FAR_STEPS, s), look_up(FAR_STEPS, s + 1)
        for kind, steps in ((border, BORDER_STEPS), (entry, ENTRY_STEPS), (inside & jnp.logical_not(entry), LAST_STEPS)):
            done = tuple(jnp.where(kind, look_up(steps, s + i), done[i]) for i in range(2))
        g_lo, g_hi = done

        x_at = jnp.where(late, jnp.where(s == 1, 0, jnp.where(s == lead // 2 + 1, 1, -1)), jnp.where(s < blocks, s, -1))

        @pl.when(carries & inside & jnp.logical_not(entry) & (s == half))
        def _():
            side_forward(side_block(1))

        @pl.when(sums)
        def _():
            lax.fori_loop(g_lo, g_hi, lambda m, unused: (g_step(in_turn(m)), unused)[1], 0)

        @pl.when(sums & (x_at >= 0))
        def _():
            b = near_block(blocks - 1 - x_at)
            of_entry = b == jnp.where(upward, 0, blocks - 1)
            start = G_PARTS - jnp.where(of_entry, G_SIDES[0], G_SIDES[1])
            lax.fori_loop(start, G_PARTS, lambda c, unused: (x_send(b, c), unused)[1], 0)

        @pl.when((n >= 0) & (n < w_steps))
        def _():
            w_step(n)

        @pl.when(s == c2_at)
        def _():
            c2_send()

        return carry

    lax.fori_loop(0, turns, turn, 0)

    def all_sent(sem, size):
        at = pl.ds(0, size // (2 * key_cols))
        remote(pf.at[at], pf.at[at], sem, sem, peer).wait_send()

    part_size, chunk_size = w_rows * key_cols, g_rows * key_cols
    counts = ((far_end, 1), (border, 2 * W_MAIN + 2), (entry, 2 * W_MAIN + W_PARTS + 4), (inside & jnp.logical_not(entry), W_PARTS + 2))
    for kind, parts in counts:

        @pl.when(carries & kind)
        def _():
            all_sent(sent, parts * part_size)

    @pl.when(carries)
    def _():
        all_sent(shared, 2 * columns * key_cols)

    total = y[text_rows, my_cols]
    c1_all(text_rows, ct_r).wait_recv()
    for i in range(1, tp):
        total = total + yr[head_of(i)[0], text_rows, :].astype(f32)
    c2_all().wait_recv()
    placed = lax.dot_general(place_t[...], c2_dst[...], ROWS_TO_COLS, preferred_element_type=f32)
    projected = jnp.where(is_img[...] > 0.5, placed, total) + bias_ref[...]
    for s in range(rows // LENGTH):
        values = projected[s * LENGTH : (s + 1) * LENGTH]
        turned = values * cosv[...] + pltpu.roll(values, HALF, 1) * sinv[...]
        keys_out[s * LENGTH : (s + 1) * LENGTH, :] = jnp.where(live(s), turned, 0.0).astype(bf16)

    remote(landed, landed, sent, g_r, peer).wait_recv()
    wgrad_out[...] = landed[...].astype(f32) * (1.0 / rows)

    @pl.when(sums)
    def _():
        all_sent(sent, (g_steps + all_sides) * chunk_size)

    all_sent(small, 2 * (units - 1) * capacity * cols + (tp - 1) * (both + images) * cols)


def write_kernel(*refs):
    count = (len(refs) - 1) // 2
    copies = [pltpu.make_async_copy(refs[i], refs[count + i], refs[-1].at[i]) for i in range(count)]
    for copy in copies:
        copy.start()
    for copy in copies:
        copy.wait()


def rotary_tables():
    frequency = ROPE_BASE ** (-(np.arange(HALF, dtype=np.float64) * 2.0) / HEAD_DIM)
    table = np.arange(LENGTH, dtype=np.float64)[:, None] * frequency[None, :]
    cosine, sine = np.cos(table), np.sin(table)
    return (
        np.concatenate([cosine, cosine], axis=1).astype(np.float32),
        np.concatenate([-sine, sine], axis=1).astype(np.float32),
    )


def fits(groups, fsdp, tp, rows, head_cols, block):
    units = groups * fsdp
    if groups != 2 or units % tp or units & (units - 1) or tp & (tp - 1) or head_cols != HEAD_DIM or rows % LENGTH:
        return False
    blocks = units // tp
    return blocks == 2 and fsdp == 2 * blocks and tp % 2 == 0 and block % (G_PARTS * HEAD_DIM) == 0 and (rows // units) % 16 == 0


def per_device(
    text_embeds, image_embeds, key_weight, key_bias, key_cot, image_owner, image_slot, seq_lengths
):
    groups, fsdp, tp = lax.axis_size("group"), lax.axis_size("fsdp"), lax.axis_size("tp")
    rows, columns = text_embeds.shape
    images = image_embeds.shape[0]
    cols = key_bias.shape[0]
    block = key_weight.shape[0]
    if not fits(groups, fsdp, tp, rows, cols, block):
        return per_device_plain(
            text_embeds, image_embeds, key_weight, key_bias, key_cot, image_owner, image_slot, seq_lengths
        )
    units = groups * fsdp
    capacity = rows // units
    slots = units * capacity
    both, key_cols = rows + images, cols * tp
    blocks = units // tp
    w_steps, g_steps = blocks * W_PARTS, blocks * G_PARTS
    cosine, sine = rotary_tables()
    bf16, f32 = jnp.bfloat16, jnp.float32
    hbm = pl.BlockSpec(memory_space=pltpu.HBM)
    vmem = pl.BlockSpec(memory_space=pltpu.VMEM)
    dma = lambda n: pltpu.SemaphoreType.DMA((n,))
    one = pltpu.SemaphoreType.DMA
    shapes = (
        jax.ShapeDtypeStruct((rows, cols), bf16),
        jax.ShapeDtypeStruct((rows, columns), bf16),
        jax.ShapeDtypeStruct((images, columns), bf16),
        jax.ShapeDtypeStruct((block, cols), f32),
    )
    operands = (
        text_embeds, image_embeds, key_weight, key_bias.reshape(1, -1), key_cot,
        image_owner.reshape(1, -1), image_slot.reshape(1, -1), seq_lengths.reshape(1, -1), jnp.asarray(cosine), jnp.asarray(sine),
    )
    held = pl.pallas_call(
        functools.partial(fused_kernel, groups, fsdp, tp, capacity),
        out_shape=tuple(pltpu.VMEM(leaf.shape, leaf.dtype) for leaf in shapes),
        in_specs=[hbm] * 10,
        out_specs=(vmem, vmem, vmem, vmem),
        scratch_shapes=[
            pltpu.VMEM((1, cols), f32),
            pltpu.VMEM((1, images), jnp.int32),
            pltpu.VMEM((1, rows), jnp.int32),
            pltpu.VMEM((1, seq_lengths.shape[0]), jnp.int32),
            pltpu.VMEM((both, columns), bf16),
            pltpu.VMEM((columns, key_cols), bf16),
            pltpu.VMEM((rows, key_cols), bf16),
            pltpu.VMEM((LENGTH, cols), f32),
            pltpu.VMEM((LENGTH, cols), f32),
            pltpu.VMEM((both, key_cols), bf16),
            pltpu.VMEM((slots, images), bf16),
            pltpu.VMEM((slots, rows), bf16),
            pltpu.VMEM((rows, cols), f32),
            pltpu.VMEM((slots, cols), bf16),
            pltpu.VMEM((slots, cols), bf16),
            pltpu.VMEM((images, cols), bf16),
            pltpu.VMEM((columns, key_cols), f32),
            pltpu.VMEM((columns, key_cols), bf16),
            pltpu.VMEM((columns, key_cols), bf16),
            pltpu.VMEM((columns, key_cols), bf16),
            pltpu.VMEM((columns, key_cols), bf16),
            pltpu.VMEM((columns, key_cols), bf16),
            pltpu.VMEM((both, key_cols), f32),
            pltpu.VMEM((tp, both, cols), bf16),
            pltpu.VMEM((tp, both, cols), bf16),
            pltpu.VMEM((slots, cols), bf16),
            pltpu.VMEM((slots, cols), bf16),
            pltpu.VMEM((block, cols), bf16),
            pltpu.VMEM((blocks, block // W_PARTS, key_cols), bf16),
            dma(9), dma(w_steps * W_FINE), one, one, one, one, one, one, one, one, one,
            dma(g_steps), dma(g_steps), dma(blocks * G_SIDES[0]), dma(blocks * W_FINE),
        ],
        compiler_params=pltpu.CompilerParams(
            collective_id=0, has_side_effects=True, vmem_limit_bytes=44 * 1024 * 1024
        ),
        name="fused",
    )(*(pltpu.with_memory_space_constraint(operand, pltpu.HBM) for operand in operands))
    return pl.pallas_call(
        write_kernel,
        out_shape=shapes,
        in_specs=[vmem] * 4,
        out_specs=(pl.BlockSpec(memory_space=pl.ANY),) * 4,
        scratch_shapes=[dma(4)],
        compiler_params=pltpu.CompilerParams(vmem_limit_bytes=4 * 1024 * 1024),
        name="write",
    )(*held)


def solution(mesh):
    in_specs = (
        P(("group", "fsdp"), "tp"),
        P(("group", "fsdp"), "tp"),
        P(("group", "fsdp"), None),
        P("tp"),
        P(("group", "fsdp"), None),
        P(("group", "fsdp")),
        P(("group", "fsdp")),
        P(("group", "fsdp")),
    )
    out_specs = (
        P(("group", "fsdp"), "tp"),
        P(("group", "fsdp"), "tp"),
        P(("group", "fsdp"), "tp"),
        P(("group", "fsdp"), "tp"),
    )
    return jax.shard_map(
        per_device, mesh=mesh, in_specs=in_specs, out_specs=out_specs, check_vma=False
    )
```

```python
import functools

import jax
import jax.numpy as jnp
import numpy as np
from jax import lax
from jax.experimental import pallas as pl
from jax.experimental.pallas import tpu as pltpu
from jax.sharding import PartitionSpec as P

HEAD_DIM = 128
LENGTH = 256


ROPE_BASE = 1000000.0


def angles(row_total):
    position = (jnp.arange(row_total, dtype=jnp.int32) % LENGTH).astype(jnp.float32)
    frequency = ROPE_BASE ** (-(jnp.arange(HEAD_DIM // 2, dtype=jnp.float32) * 2.0) / HEAD_DIM)
    angle_table = position[:, None] * frequency[None, :]
    return (jnp.cos(angle_table), jnp.sin(angle_table))


def rotate(values, cosine, sine, direction):
    row_total = values.shape[0]
    by_head = values.reshape(row_total, -1, HEAD_DIM)
    half_dim = HEAD_DIM // 2
    front_half = by_head[..., :half_dim]
    second = by_head[..., half_dim:]
    cos_part = cosine[:, None, :]
    sin_part = direction * sine[:, None, :]
    rotated = jnp.concatenate(
        [front_half * cos_part - second * sin_part, second * cos_part + front_half * sin_part],
        axis=-1,
    )
    return rotated.reshape(row_total, -1)


def send_slots(owners, unit_count, capacity):
    onehot_marks = (owners[:, None] == jnp.arange(unit_count, dtype=jnp.int32)[None, :]).astype(
        jnp.int32
    )
    before = jnp.cumsum(onehot_marks, axis=0) - onehot_marks
    owner_rank = jnp.sum(before * onehot_marks, axis=1)
    return owners * capacity + owner_rank


def share_kernel(text_ref, image_ref, back_ref, image_back_ref, out_ref):
    contract = (((0,), (0,)), ((), ()))
    part = lax.dot_general(
        text_ref[...], back_ref[...], contract, preferred_element_type=jnp.float32
    ) + lax.dot_general(
        image_ref[...], image_back_ref[...], contract, preferred_element_type=jnp.float32
    )
    part = part.astype(out_ref.dtype)
    width = out_ref.shape[2]
    for head in range(out_ref.shape[0]):
        out_ref[head] = part[:, head * width : (head + 1) * width]


def weight_shares(text, image, back, image_back, head_cols):
    columns = text.shape[1]
    heads = back.shape[1] // head_cols
    tile = min(512, columns)
    return pl.pallas_call(
        share_kernel,
        grid=(columns // tile,),
        in_specs=[
            pl.BlockSpec((text.shape[0], tile), lambda i: (0, i)),
            pl.BlockSpec((image.shape[0], tile), lambda i: (0, i)),
            pl.BlockSpec(back.shape, lambda i: (0, 0)),
            pl.BlockSpec(image_back.shape, lambda i: (0, 0)),
        ],
        out_specs=pl.BlockSpec((heads, tile, head_cols), lambda i: (0, i, 0)),
        out_shape=jax.ShapeDtypeStruct((heads, columns, head_cols), jnp.bfloat16),
        cost_estimate=pl.CostEstimate(
            flops=2 * (text.size + image.size) * back.shape[1],
            bytes_accessed=2 * (text.size + image.size + columns * back.shape[1]),
            transcendentals=0,
        ),
    )(text, image, back, image_back)


def project_kernel(text_ref, image_ref, weight_ref, out_ref):
    step = pl.program_id(0)
    last = pl.num_programs(0) - 1
    rows = jnp.where(step == last, image_ref[...], text_ref[...])
    part = jnp.dot(rows, weight_ref[...], preferred_element_type=jnp.float32).astype(out_ref.dtype)
    width = out_ref.shape[2]
    for head in range(out_ref.shape[0]):
        out_ref[head] = part[:, head * width : (head + 1) * width]


def projection_parts(text, image, weight, head_cols):
    heads = weight.shape[1] // head_cols
    tile, columns = image.shape
    text_tiles = text.shape[0] // tile
    return pl.pallas_call(
        project_kernel,
        grid=(text_tiles + 1,),
        in_specs=[
            pl.BlockSpec((tile, columns), lambda i: (jnp.minimum(i, text_tiles - 1), 0)),
            pl.BlockSpec((tile, columns), lambda i: (0, 0)),
            pl.BlockSpec(weight.shape, lambda i: (0, 0)),
        ],
        out_specs=pl.BlockSpec((heads, tile, head_cols), lambda i: (0, i, 0)),
        out_shape=jax.ShapeDtypeStruct((heads, text.shape[0] + tile, head_cols), jnp.bfloat16),
        cost_estimate=pl.CostEstimate(
            flops=2 * (text.size + image.size) * weight.shape[1],
            bytes_accessed=2 * (text.size + image.size + weight.size),
            transcendentals=0,
        ),
    )(text, image, weight)


def spread(piece, axis):
    count = lax.axis_size(axis)
    copies = jnp.broadcast_to(piece[None], (count,) + piece.shape)
    got = lax.all_to_all(copies, axis, split_axis=0, concat_axis=0, tiled=True)
    return got.reshape((count * piece.shape[0],) + piece.shape[1:])


def shifted(values, axis, step):
    count = lax.axis_size(axis)
    return lax.ppermute(values, axis, [(i, (i + step) % count) for i in range(count)])


def exchange_sum(blocks, axis):
    count = lax.axis_size(axis)
    me = lax.axis_index(axis)
    total = lax.dynamic_index_in_dim(blocks, me, 0, keepdims=False).astype(jnp.float32)
    for step in range(1, count):
        block = lax.dynamic_index_in_dim(blocks, (me + step) % count, 0, keepdims=False)
        total = total + shifted(block, axis, step).astype(jnp.float32)
    return total


def share_rows(piece, axis):
    count = lax.axis_size(axis)
    me = lax.axis_index(axis)
    rows = piece.shape[0]
    full = jnp.zeros((count * rows,) + piece.shape[1:], piece.dtype)
    full = lax.dynamic_update_slice_in_dim(full, piece, me * rows, 0)
    for step in range(1, count):
        source = (me + count - step) % count
        full = lax.dynamic_update_slice_in_dim(full, shifted(piece, axis, step), source * rows, 0)
    return full


def per_device_plain(
    text_embeds, image_embeds, key_weight, key_bias, key_cot, image_owner, image_slot, seq_lengths
):
    row_count, columns = text_embeds.shape
    image_count = image_embeds.shape[0]
    units = ("group", "fsdp")
    core_count = lax.axis_size("group")
    fsdp_count = lax.axis_size("fsdp")
    tp_count = lax.axis_size("tp")
    unit_count = core_count * fsdp_count
    capacity = row_count // unit_count
    slot_count = unit_count * capacity
    head_cols = key_bias.shape[0]
    key_cols = head_cols * tp_count
    weight_block = key_weight.shape[0]
    halves = unit_count // tp_count
    tp_index = lax.axis_index("tp")

    position = jnp.arange(row_count, dtype=jnp.int32)
    seq_ids = position // LENGTH
    seq_marks = seq_ids[:, None] == jnp.arange(seq_lengths.shape[0], dtype=jnp.int32)[None, :]
    live_limit = jnp.sum(jnp.where(seq_marks, seq_lengths[None, :], 0), axis=1)
    live_mask = (position % LENGTH < live_limit).astype(jnp.float32)
    cosine, sine = angles(row_count)
    masked = key_cot.astype(jnp.float32) * live_mask[:, None]
    rotated_back = rotate(masked, cosine, sine, -1.0).astype(jnp.bfloat16)
    is_image = image_slot >= 0
    text_back = jnp.where(is_image[:, None], jnp.zeros_like(rotated_back), rotated_back)

    slot_ids = jnp.arange(slot_count, dtype=jnp.int32)
    place = (image_slot[:, None] == slot_ids[None, :]).astype(jnp.bfloat16)
    returning = lax.dot_general(
        place, rotated_back, (((0,), (0,)), ((), ())), preferred_element_type=jnp.float32
    ).astype(jnp.bfloat16)
    returned = lax.all_to_all(
        returning.reshape(unit_count, capacity, key_cols), units, split_axis=0, concat_axis=0,
        tiled=True,
    ).reshape(slot_count, key_cols)
    slots_out = send_slots(image_owner, unit_count, capacity)
    pick = (slots_out[:, None] == slot_ids[None, :]).astype(jnp.bfloat16)
    image_back = jnp.dot(pick, returned, preferred_element_type=jnp.float32).astype(jnp.bfloat16)

    piece_rows = weight_block // tp_count
    own_piece = lax.dynamic_slice_in_dim(key_weight, tp_index * piece_rows, piece_rows, 0)
    moves = []
    for unit in range(unit_count):
        for part in range(tp_count):
            target = (unit % halves) * tp_count + part
            moves.append((unit * tp_count + part, target * tp_count + unit // halves))
    own_piece = lax.ppermute(own_piece, units + ("tp",), moves)
    chip_rows = spread(own_piece, "fsdp")

    shares = weight_shares(text_embeds, image_embeds, text_back, image_back, head_cols)
    shares = shares.reshape(core_count, fsdp_count, weight_block, head_cols)
    shares = exchange_sum(shares, "group").astype(jnp.bfloat16)
    shares, chip_rows = lax.optimization_barrier((shares, chip_rows))
    shares = lax.all_to_all(shares, "fsdp", split_axis=0, concat_axis=0, tiled=True)
    weight_grad = jnp.sum(shares.astype(jnp.float32), axis=0) / row_count
    returns = []
    for unit in range(unit_count):
        for part in range(tp_count):
            holder = (unit % halves) + part * halves
            returns.append((holder * tp_count + unit // halves, unit * tp_count + part))
    weight_grad = lax.ppermute(weight_grad, units + ("tp",), returns)

    weight_rows = share_rows(chip_rows, "group")
    both = projection_parts(text_embeds, image_embeds, weight_rows, head_cols)
    both = exchange_sum(both, "tp")
    image_proj = both[row_count:].astype(jnp.bfloat16)
    outgoing = lax.dot_general(
        pick, image_proj, (((0,), (0,)), ((), ())), preferred_element_type=jnp.float32
    ).astype(jnp.bfloat16)
    received = lax.all_to_all(
        outgoing.reshape(unit_count, capacity, head_cols), units, split_axis=0, concat_axis=0,
        tiled=True,
    ).reshape(slot_count, head_cols)
    placed = jnp.dot(place, received, preferred_element_type=jnp.float32)
    projected = jnp.where(is_image[:, None], placed, both[:row_count]) + key_bias
    key_rows = (rotate(projected, cosine, sine, 1.0) * live_mask[:, None]).astype(jnp.bfloat16)

    contract = (((1,), (1,)), ((), ()))
    text_grad = lax.dot_general(
        text_back, weight_rows, contract, preferred_element_type=jnp.float32
    ).astype(jnp.bfloat16)
    image_grad = lax.dot_general(
        image_back, weight_rows, contract, preferred_element_type=jnp.float32
    ).astype(jnp.bfloat16)
    return (key_rows, text_grad, image_grad, weight_grad)


MESH = pl.DeviceIdType.MESH
HALF = HEAD_DIM // 2
ROWS_TO_COLS = (((0,), (0,)), ((), ()))
COLS_TO_COLS = (((1,), (1,)), ((), ()))
W_PARTS = 4
W_MAIN = 3
W_FINE = 2
W_NEAR_OR_FAR = (0, 0, 0, 1, 0, 1, 1, 1)
W_PART_AT = (0, 1, 2, 0, 3, 1, 3, 2)
FAR_LEAD = 4
FAR_STEPS = (0, 3, 6, 9, 11, 11, 11, 11, 11, 14, 14, 14, 14, 16)
BORDER_STEPS = (0, 0, 0, 0, 2, 4, 6, 8, 8, 13, 13, 16, 16, 16)
BORDER_SPOT = 11
ENTRY_STEPS = (0, 0, 0, 0, 0, 0, 0, 0, 0, 4, 8, 14, 16, 16)
ENTRY_ORDER = (5, 6, 0, 1, 7, 8, 2, 3, 9, 10, 4, 11, 12, 13, 14, 15)
LAST_STEPS = (0, 0, 0, 0, 2, 4, 6, 9, 10, 12, 14, 16, 16, 16)
G_PARTS = 8
G_SIDES = (3, 2)


def fused_kernel(
    groups, fsdp, tp, capacity,
    text_ref, image_ref, weight_ref, bias_hbm, cot_ref, owner_hbm, slot_hbm, lens_hbm, cos_ref, sin_ref,
    keys_out, text_out, image_out, wgrad_out,
    bias_ref, owner_ref, slot_ref, lens_ref, x, w, cot, cosv, sinv, back, pick_t, place_t, is_img,
    d1_src, d1_dst, d2_src, pf, pa, pb, chain, above, below, y, yb, yr, c2_src, c2_dst, landed, side,
    ld, w_recv, sent, shared, small, d1_r, d2_r, ci_r, ct_r, c2_r, g_r, p_r, chain_r, x_r, h_r,
):
    f32, bf16 = jnp.float32, jnp.bfloat16
    g, z, t = lax.axis_index("group"), lax.axis_index("fsdp"), lax.axis_index("tp")
    units = groups * fsdp
    me = g * fsdp + z
    rows, images = text_ref.shape[0], image_ref.shape[0]
    both = rows + images
    columns = text_ref.shape[1]
    slots = units * capacity
    cols = bias_ref.shape[1]
    block = weight_ref.shape[0]
    blocks = units // tp
    key_cols = tp * cols
    w_rows, g_rows = block // W_PARTS, block // G_PARTS
    w_steps, g_steps = blocks * W_PARTS, blocks * G_PARTS
    first = t * blocks
    carrier, z0 = first // fsdp, lax.rem(first, fsdp)
    carries = g == carrier
    inside = (z >= z0) & (z < z0 + blocks)
    far_end = jnp.logical_not(inside) & ((z == 0) | (z == fsdp - 1))
    my_cols = pl.ds(pl.multiple_of(t * cols, cols), cols)
    peer = (1 - g, z, t)
    other = lax.bitwise_xor(t, 1)
    beside = (g, z, other)
    other_z0 = fsdp - blocks - z0
    upward = z0 > 0
    entry = jnp.where(upward, z == z0, z == z0 + blocks - 1)
    border = jnp.where(upward, z == z0 - 1, z == z0 + blocks)
    relays = entry | border

    def near_block(k):
        within = lax.rem(z - z0 + k + blocks, blocks)
        return jnp.where(inside, within, jnp.where(z < z0, k, blocks - 1 - k))

    def far_other(k):
        within = lax.rem(z - other_z0 + blocks - 1 - k + blocks, blocks)
        return jnp.where(inside, jnp.where(upward, k, blocks - 1 - k), within)

    def look_up(table, n):
        found = table[0]
        for i in range(1, len(table)):
            found = jnp.where(n == i, table[i], found)
        return found

    def w_part(n):
        return near_block(look_up(W_NEAR_OR_FAR, n)), look_up(W_PART_AT, n)

    def unit_of(i):
        far = units - i
        core, plane = lax.bitwise_xor(g, far % groups), lax.bitwise_xor(z, far // groups)
        return core * fsdp + plane, (core, plane, t)

    def head_of(i):
        q = lax.bitwise_xor(t, tp - 1 if i == 1 else i - 1)
        return q, (g, z, q)

    def remote(src, dst, send, recv, device):
        return pltpu.make_async_remote_copy(
            src_ref=src, dst_ref=dst, send_sem=send, recv_sem=recv, device_id=device, device_id_type=MESH
        )

    barrier = pltpu.get_barrier_semaphore()
    for i in range(1, units):
        pl.semaphore_signal(barrier, inc=1, device_id=unit_of(i)[1], device_id_type=MESH)
    for i in range(1, tp):
        q = head_of(i)[0]
        for core in range(groups):
            pl.semaphore_signal(barrier, inc=1, device_id=(core, z, q), device_id_type=MESH)

    pairs = (
        (slot_hbm, slot_ref),
        (cot_ref, cot),
        (cos_ref, cosv),
        (sin_ref, sinv),
        (lens_hbm, lens_ref),
        (owner_hbm, owner_ref),
        (bias_hbm, bias_ref),
        (text_ref, x.at[pl.ds(0, rows)]),
        (image_ref, x.at[pl.ds(rows, images)]),
    )
    loads = [pltpu.make_async_copy(source, target, ld.at[i]) for i, (source, target) in enumerate(pairs)]
    for load in loads[:5]:
        load.start()

    def w_slice(b, c):
        return pl.ds(pl.multiple_of(b * block + c * w_rows, w_rows), w_rows)

    fine = w_rows // W_FINE

    def w_fine(b, c, h):
        return pl.ds(pl.multiple_of(b * block + c * w_rows + h * fine, fine), fine)

    def w_index(b, c, h):
        return (b * W_PARTS + c) * W_FINE + h

    def w_load(b, c, h):
        source = weight_ref.at[pl.ds(pl.multiple_of(c * w_rows + h * fine, fine), fine)]
        return pltpu.make_async_copy(source, w.at[w_fine(b, c, h)], w_recv.at[w_index(b, c, h)])

    def side_rows(b, h):
        return side.at[b, pl.ds(h * fine, fine)]

    def side_load(b, h):
        source = weight_ref.at[pl.ds(W_MAIN * w_rows + h * fine, fine)]
        return pltpu.make_async_copy(source, side_rows(b, h), h_r.at[b * W_FINE + h])

    @pl.when(carries & inside)
    def _():
        for c in range(W_PARTS):
            for h in range(W_FINE):
                w_load(z - z0, c, h).start()

    @pl.when(carries & jnp.logical_not(inside))
    def _():
        for h in range(W_FINE):
            side_load(z - other_z0, h).start()

    for load in loads[5:]:
        load.start()

    loads[0].wait()
    slot_ids = lax.broadcasted_iota(jnp.int32, (slots, rows), 0)
    place_t[...] = jnp.where(slot_ids == slot_ref[...], 1.0, 0.0).astype(bf16)
    row_ids = lax.broadcasted_iota(jnp.int32, (LENGTH, HEAD_DIM), 0)

    def live(s):
        return row_ids < lens_ref[0:1, s : s + 1]

    def rotated_back(s, at):
        span = pl.ds(s * LENGTH, LENGTH)
        values = jnp.where(live(s), cot[span, at].astype(f32), 0.0)
        return values * cosv[...] - pltpu.roll(values, HALF, 1) * sinv[...]

    for load in loads[1:5]:
        load.wait()
    mine = jnp.concatenate([rotated_back(s, my_cols) for s in range(rows // LENGTH)], axis=0).astype(bf16)
    d1_src[...] = jnp.dot(place_t[...], mine, preferred_element_type=f32).astype(bf16)

    pl.semaphore_wait(barrier, units - 1 + groups * (tp - 1))

    def slot_rows(v):
        return pl.ds(pl.multiple_of(v * capacity, capacity), capacity)

    def d1(i):
        v, device = unit_of(i)
        return remote(d1_src.at[slot_rows(v)], d1_dst.at[slot_rows(me)], small, d1_r, device)

    def d1_all():
        at = pl.ds(0, (units - 1) * capacity)
        return remote(d1_src.at[at], d1_dst.at[at], small, d1_r, peer)

    for i in range(1, units):
        d1(i).start()
    d1_dst[slot_rows(me), :] = d1_src[slot_rows(me), :]

    def w_send(b, c, h, to):
        at = w_fine(b, c, h)
        return remote(w.at[at], w.at[at], sent, w_recv.at[w_index(b, c, h)], to)

    def w_share(b, c, h):
        at = w_fine(b, c, h)
        return remote(w.at[at], w.at[at], shared, w_recv.at[w_index(b, c, h)], peer)

    def w_routes(b, c, h):
        up = (z >= z0 + b) & (z < fsdp - 1) & ((c < W_MAIN) | (z + 1 < z0 + blocks))
        down = (z <= z0 + b) & (z > 0) & ((c < W_MAIN) | (z > z0))
        return ((up, w_send(b, c, h, (g, z + 1, t))), (down, w_send(b, c, h, (g, z - 1, t))))

    def w_inward(c):
        b = z - z0
        for h in range(W_FINE):
            pl.when(upward)(w_send(b, c, h, (g, z + 1, t)).start)
            pl.when(jnp.logical_not(upward))(w_send(b, c, h, (g, z - 1, t)).start)

    def side_routes(b, h):
        step = jnp.where(upward, 1, -1)
        i, at = b * W_FINE + h, w_fine(b, W_MAIN, h)
        return (
            ((z + step >= 0) & (z + step < fsdp), remote(side_rows(b, h), side_rows(b, h), sent, h_r.at[i], (g, z + step, t))),
            (inside, remote(side_rows(b, h), w.at[at], sent, w_recv.at[w_index(b, W_MAIN, h)], beside)),
        )

    def side_forward(b):
        for h in range(W_FINE):
            side_load(b, h).wait()
            for condition, copy in side_routes(b, h):
                pl.when(condition)(copy.start)

    def side_block(k):
        return jnp.where(upward, blocks - 1 - k, k)

    def w_forward(b, c):
        held = entry & (z == z0 + b) & (c >= 2)
        for h in range(W_FINE):
            w_load(b, c, h).wait()
            for (condition, copy), inward in zip(w_routes(b, c, h), (upward, jnp.logical_not(upward))):
                pl.when(condition & jnp.logical_not(held & inward))(copy.start)
            w_share(b, c, h).start()

    early = jnp.where(inside, near_block(1), near_block(0))

    is_img[...] = lax.dot_general(
        place_t[...], jnp.ones((slots, cols), bf16), ROWS_TO_COLS, preferred_element_type=f32
    )
    y[...] = jnp.zeros_like(y)
    for s in range(rows // LENGTH):
        span = pl.ds(s * LENGTH, LENGTH)
        for h in range(tp):
            at = pl.ds(h * cols, cols)
            back[span, at] = jnp.where(is_img[span, :] > 0.5, 0.0, rotated_back(s, at)).astype(bf16)
    @pl.when(carries & inside)
    def _():
        lax.fori_loop(0, W_PARTS, lambda c, carry: (w_forward(z - z0, c), carry)[1], 0)

    @pl.when(carries & jnp.logical_not(inside))
    def _():
        side_forward(z - other_z0)

    loads[5].wait()
    image_units = lax.broadcasted_iota(jnp.int32, (units, images), 0)
    marks = jnp.where(image_units == owner_ref[...], 1.0, 0.0)
    before = jnp.where(
        lax.broadcasted_iota(jnp.int32, (images, images), 0) < lax.broadcasted_iota(jnp.int32, (images, images), 1),
        1.0,
        0.0,
    ).astype(bf16)
    counts = jnp.dot(marks.astype(bf16), before, preferred_element_type=f32)
    rank = jnp.sum(counts * marks, axis=0, keepdims=True).astype(jnp.int32)
    slots_out = owner_ref[...] * capacity + rank
    pick_t[...] = jnp.where(
        lax.broadcasted_iota(jnp.int32, (slots, images), 0) == slots_out, 1.0, 0.0
    ).astype(bf16)

    tile = block // 2
    loads[7].wait()

    def p_text(j, carry):
        at = pl.ds(pl.multiple_of(j * tile, tile), tile)
        pf[at, :] = lax.dot_general(
            x[0:rows, at], back[0:rows, :], ROWS_TO_COLS, preferred_element_type=f32
        )
        return carry

    lax.fori_loop(0, columns // tile, p_text, 0)

    d1_all().wait_recv()
    returned = lax.dot_general(pick_t[...], d1_dst[...], ROWS_TO_COLS, preferred_element_type=f32).astype(bf16)
    d2_src[...] = returned
    back[pl.ds(rows, images), my_cols] = returned

    def head_cols(q):
        return pl.ds(pl.multiple_of(q * cols, cols), cols)

    def d2(i, source):
        q, device = head_of(i)
        return remote(d2_src, back.at[pl.ds(rows, images), head_cols(source)], small, d2_r, device)

    text_rows, image_rows = pl.ds(0, rows), pl.ds(rows, images)

    def d2_all():
        at = pl.ds(0, tp - 1)
        return remote(yb.at[at, image_rows], yr.at[at, image_rows], small, d2_r, peer)

    for i in range(1, tp):
        d2(i, t).start()

    @pl.when(carries & (inside | border))
    def _():
        w_forward(early, 0)

    @pl.when(carries & relays)
    def _():
        side_forward(side_block(jnp.where(border, 1, 0)))

    d2_all().wait_recv()
    loads[6].wait()
    loads[8].wait()

    @pl.when(carries & (inside | border))
    def _():
        w_forward(early, 1)

    def p_copy(i):
        at = pl.ds(pl.multiple_of(i * g_rows, g_rows), g_rows)
        return remote(pa.at[at], pb.at[at], shared, p_r.at[i], peer)

    def g_slice(b, c):
        return pl.ds(pl.multiple_of(b * block + c * g_rows, g_rows), g_rows)

    def x_copy(b, c):
        i, at = b * G_SIDES[0] + c - (G_PARTS - G_SIDES[0]), g_slice(b, c)
        return remote(pb.at[at], pa.at[at], sent, x_r.at[i], beside)

    def x_send(b, c):
        i, at = b * G_PARTS + c, g_slice(b, c)
        p_copy(i).wait_recv()
        pb[at, :] = (pf[at, :] + pb[at, :].astype(f32)).astype(bf16)
        x_copy(b, c).start()

    def p_step(k, carry):
        b, half = near_block(blocks - 1 - k // 2), lax.rem(k, 2)
        j = b * 2 + half
        at = pl.ds(pl.multiple_of(j * tile, tile), tile)
        part = pf[at, :] + lax.dot_general(
            x[rows:both, at], back[rows:both, :], ROWS_TO_COLS, preferred_element_type=f32
        )
        pf[at, :] = part

        @pl.when(carries)
        def _():
            pa[at, :] = part.astype(bf16)
            for c in range(tile // g_rows):
                p_copy(j * (tile // g_rows) + c).start()

        return carry

    lax.fori_loop(0, columns // tile, p_step, 0)

    @pl.when(carries & relays)
    def _():
        w_forward(early, 2)

    @pl.when(carries & inside)
    def _():
        side_forward(side_block(jnp.where(entry, 1, 0)))

    @pl.when(carries & entry)
    def _():
        for c in range(2, W_PARTS):
            w_inward(c)

    def w_step(n):
        b, c = w_part(n)
        ahead = jnp.where(border, n + 3, n)
        next_b, next_c = w_part(ahead)
        main = next_c < W_MAIN
        forwarded = (inside & (z == z0 + next_b)) | ((relays & main | inside & (next_c < 2)) & (next_b == early))

        @pl.when(carries & (ahead < w_steps) & jnp.logical_not(forwarded))
        def _():
            w_forward(next_b, next_c)

        @pl.when(jnp.logical_not(carries))
        def _():
            for h in range(W_FINE):
                w_load(b, c, h).wait()

        last = n == w_steps - 1
        project(n, image_rows)

        @pl.when(last)
        def _():
            c1_send(image_rows, ci_r)

        def text_step(k, carry):
            project(k, text_rows)
            return carry

        lax.fori_loop(jnp.where(last, n - 1, n), jnp.where(n == w_steps - 2, n, n + 1), text_step, 0)

        @pl.when(last)
        def _():
            c1_send(text_rows, ct_r)

        kept = w_steps - 3
        lax.fori_loop(jnp.where(last, kept, n), jnp.where((n < kept) | last, n + 1, n), grad_step, 0)

    def project(n, which):
        at = w_slice(*w_part(n))
        y[which, :] += jnp.dot(x[which, at], w[at, :], preferred_element_type=f32)

    def grad_step(n, carry):
        at = w_slice(*w_part(n))
        grads = lax.dot_general(back[...], w[at, :], COLS_TO_COLS, preferred_element_type=f32).astype(bf16)
        text_out[:, at] = grads[:rows]
        image_out[:, at] = grads[rows:]
        return carry

    def c1(i, source, which, recv):
        q, device = head_of(i)
        return remote(yb.at[q, which], yr.at[source, which], small, recv, device)

    def c1_all(which, recv):
        at = pl.ds(0, tp - 1)
        return remote(yb.at[at, which], yr.at[at, which], small, recv, peer)

    def c1_send(which, recv):
        for q in range(tp):
            yb[q, which, :] = y[which, q * cols : (q + 1) * cols].astype(bf16)
        for i in range(1, tp):
            c1(i, t, which, recv).start()

    def c2(i):
        v, device = unit_of(i)
        return remote(c2_src.at[slot_rows(v)], c2_dst.at[slot_rows(me)], small, c2_r, device)

    def c2_all():
        at = pl.ds(0, (units - 1) * capacity)
        return remote(c2_src.at[at], c2_dst.at[at], small, c2_r, peer)

    def c2_send():
        total = y[image_rows, my_cols]
        c1_all(image_rows, ci_r).wait_recv()
        for i in range(1, tp):
            q = head_of(i)[0]
            total = total + yr[q, image_rows, :].astype(f32)
        c2_src[...] = jnp.dot(pick_t[...], total.astype(bf16), preferred_element_type=f32).astype(bf16)
        for i in range(1, units):
            c2(i).start()
        c2_dst[slot_rows(me), :] = c2_src[slot_rows(me), :]

    def chain_copies(i, at, zb):
        return (
            (z > zb, remote(chain.at[at], above.at[at], sent, chain_r.at[i], (g, z - 1, t))),
            (z < zb, remote(chain.at[at], below.at[at], sent, chain_r.at[i], (g, z + 1, t))),
        )

    def landing(c):
        return landed.at[pl.ds(pl.multiple_of(c * g_rows, g_rows), g_rows)]

    def result_copy(at, c, q):
        return remote(chain.at[at, q * cols : (q + 1) * cols], landing(c), sent, g_r, (1 - g, z, q))

    def g_step(m):
        own = jnp.where(inside, m >= all_sides, m < g_steps - all_sides)
        own_m = jnp.where(inside, m - all_sides, m)
        other_m = jnp.where(inside, m, m - (g_steps - all_sides))
        first_own = G_PARTS - jnp.where(inside & jnp.logical_not(entry), G_SIDES[0], G_SIDES[1])
        first_other = jnp.where(far_end, G_SIDES[0], G_SIDES[1])
        own_k, other_k = jnp.where(own_m >= first_own, 1, 0), jnp.where(other_m >= first_other, 1, 0)
        own_c = own_m - own_k * first_own
        other_c = G_PARTS + jnp.where(other_k == 1, other_m - all_sides, other_m - first_other)
        b = jnp.where(own, near_block(blocks - 1 - own_k), far_other(other_k))
        c = jnp.where(own, own_c, other_c)
        zb = jnp.where(own, z0, other_z0) + b
        slot_b = jnp.where(own, b, blocks - 1 - b)
        i, at = slot_b * G_PARTS + c, g_slice(slot_b, c)
        came_at = g_slice(b, c)

        @pl.when(own)
        def _():
            p_copy(i).wait_recv()
            pf[at, :] += pb[at, :].astype(f32)

        @pl.when(jnp.logical_not(own))
        def _():
            x_copy(b, c).wait_recv()
            pf[at, :] = pa[came_at, :].astype(f32)

        from_above, from_below = (z >= zb) & (z < fsdp - 1), (z <= zb) & (z > 0)
        pair = pl.ds(0, 2 * g_rows)

        @pl.when(from_above & from_below)
        def _():
            remote(chain.at[pair], above.at[pair], sent, chain_r.at[i], peer).wait_recv()

        @pl.when(from_above != from_below)
        def _():
            remote(chain.at[at], above.at[at], sent, chain_r.at[i], peer).wait_recv()

        for arrives, source in ((from_above, above), (from_below, below)):

            @pl.when(arrives)
            def _():
                pf[at, :] += source[at, :].astype(f32)

        chain[at, :] = pf[at, :].astype(bf16)
        for condition, copy in chain_copies(i, at, zb):
            pl.when(condition)(copy.start)

        @pl.when(z == zb)
        def _():
            for q in range(tp):
                result_copy(at, c, q).start()

    ratio = g_steps // w_steps
    half = w_steps // 2
    all_sides = sum(G_SIDES)
    mains = g_steps - all_sides
    lead = FAR_LEAD
    turns = len(FAR_STEPS) - 1
    sums = jnp.logical_not(carries)
    late = sums & far_end
    w_at = jnp.where(late, lead, 0)
    c2_at = jnp.where(far_end, lead + w_steps - 1, jnp.where(entry, w_steps + 2, w_steps + 1))
    c2_at = jnp.where(carries, w_steps - 1, c2_at)
    spot = BORDER_SPOT

    def in_turn(m):
        sides = G_SIDES[1]
        moved = jnp.where(m < spot + sides, m - spot + mains, jnp.where(m < mains + sides, m - sides, m))
        woven = look_up(ENTRY_ORDER, m)
        return jnp.where(border & (m >= spot), moved, jnp.where(entry, woven, m))

    def turn(s, carry):
        n = s - w_at
        done = look_up(FAR_STEPS, s), look_up(FAR_STEPS, s + 1)
        for kind, steps in ((border, BORDER_STEPS), (entry, ENTRY_STEPS), (inside & jnp.logical_not(entry), LAST_STEPS)):
            done = tuple(jnp.where(kind, look_up(steps, s + i), done[i]) for i in range(2))
        g_lo, g_hi = done

        x_at = jnp.where(late, jnp.where(s == 1, 0, jnp.where(s == lead // 2 + 1, 1, -1)), jnp.where(s < blocks, s, -1))

        @pl.when(carries & inside & jnp.logical_not(entry) & (s == half))
        def _():
            side_forward(side_block(1))

        @pl.when(sums)
        def _():
            lax.fori_loop(g_lo, g_hi, lambda m, unused: (g_step(in_turn(m)), unused)[1], 0)

        @pl.when(sums & (x_at >= 0))
        def _():
            b = near_block(blocks - 1 - x_at)
            of_entry = b == jnp.where(upward, 0, blocks - 1)
            start = G_PARTS - jnp.where(of_entry, G_SIDES[0], G_SIDES[1])
            lax.fori_loop(start, G_PARTS, lambda c, unused: (x_send(b, c), unused)[1], 0)

        @pl.when((n >= 0) & (n < w_steps))
        def _():
            w_step(n)

        @pl.when(s == c2_at)
        def _():
            c2_send()

        return carry

    lax.fori_loop(0, turns, turn, 0)

    def all_sent(sem, size):
        at = pl.ds(0, size // (2 * key_cols))
        remote(pf.at[at], pf.at[at], sem, sem, peer).wait_send()

    part_size, chunk_size = w_rows * key_cols, g_rows * key_cols
    counts = ((far_end, 1), (border, 2 * W_MAIN + 2), (entry, 2 * W_MAIN + W_PARTS + 4), (inside & jnp.logical_not(entry), W_PARTS + 2))
    for kind, parts in counts:

        @pl.when(carries & kind)
        def _():
            all_sent(sent, parts * part_size)

    @pl.when(carries)
    def _():
        all_sent(shared, 2 * columns * key_cols)

    total = y[text_rows, my_cols]
    c1_all(text_rows, ct_r).wait_recv()
    for i in range(1, tp):
        total = total + yr[head_of(i)[0], text_rows, :].astype(f32)
    c2_all().wait_recv()
    placed = lax.dot_general(place_t[...], c2_dst[...], ROWS_TO_COLS, preferred_element_type=f32)
    projected = jnp.where(is_img[...] > 0.5, placed, total) + bias_ref[...]
    for s in range(rows // LENGTH):
        values = projected[s * LENGTH : (s + 1) * LENGTH]
        turned = values * cosv[...] + pltpu.roll(values, HALF, 1) * sinv[...]
        keys_out[s * LENGTH : (s + 1) * LENGTH, :] = jnp.where(live(s), turned, 0.0).astype(bf16)

    remote(landed, landed, sent, g_r, peer).wait_recv()
    wgrad_out[...] = landed[...].astype(f32) * (1.0 / rows)

    @pl.when(sums)
    def _():
        all_sent(sent, (g_steps + all_sides) * chunk_size)

    all_sent(small, 2 * (units - 1) * capacity * cols + (tp - 1) * (both + images) * cols)


def write_kernel(*refs):
    count = (len(refs) - 1) // 2
    copies = [pltpu.make_async_copy(refs[i], refs[count + i], refs[-1].at[i]) for i in range(count)]
    for copy in copies:
        copy.start()
    for copy in copies:
        copy.wait()


def rotary_tables():
    frequency = ROPE_BASE ** (-(np.arange(HALF, dtype=np.float64) * 2.0) / HEAD_DIM)
    table = np.arange(LENGTH, dtype=np.float64)[:, None] * frequency[None, :]
    cosine, sine = np.cos(table), np.sin(table)
    return (
        np.concatenate([cosine, cosine], axis=1).astype(np.float32),
        np.concatenate([-sine, sine], axis=1).astype(np.float32),
    )


def fits(groups, fsdp, tp, rows, head_cols, block):
    units = groups * fsdp
    if groups != 2 or units % tp or units & (units - 1) or tp & (tp - 1) or head_cols != HEAD_DIM or rows % LENGTH:
        return False
    blocks = units // tp
    return blocks == 2 and fsdp == 2 * blocks and tp % 2 == 0 and block % (G_PARTS * HEAD_DIM) == 0 and (rows // units) % 16 == 0


def per_device(
    text_embeds, image_embeds, key_weight, key_bias, key_cot, image_owner, image_slot, seq_lengths
):
    groups, fsdp, tp = lax.axis_size("group"), lax.axis_size("fsdp"), lax.axis_size("tp")
    rows, columns = text_embeds.shape
    images = image_embeds.shape[0]
    cols = key_bias.shape[0]
    block = key_weight.shape[0]
    if not fits(groups, fsdp, tp, rows, cols, block):
        return per_device_plain(
            text_embeds, image_embeds, key_weight, key_bias, key_cot, image_owner, image_slot, seq_lengths
        )
    units = groups * fsdp
    capacity = rows // units
    slots = units * capacity
    both, key_cols = rows + images, cols * tp
    blocks = units // tp
    w_steps, g_steps = blocks * W_PARTS, blocks * G_PARTS
    cosine, sine = rotary_tables()
    bf16, f32 = jnp.bfloat16, jnp.float32
    hbm = pl.BlockSpec(memory_space=pltpu.HBM)
    vmem = pl.BlockSpec(memory_space=pltpu.VMEM)
    dma = lambda n: pltpu.SemaphoreType.DMA((n,))
    one = pltpu.SemaphoreType.DMA
    shapes = (
        jax.ShapeDtypeStruct((rows, cols), bf16),
        jax.ShapeDtypeStruct((rows, columns), bf16),
        jax.ShapeDtypeStruct((images, columns), bf16),
        jax.ShapeDtypeStruct((block, cols), f32),
    )
    operands = (
        text_embeds, image_embeds, key_weight, key_bias.reshape(1, -1), key_cot,
        image_owner.reshape(1, -1), image_slot.reshape(1, -1), seq_lengths.reshape(1, -1), jnp.asarray(cosine), jnp.asarray(sine),
    )
    held = pl.pallas_call(
        functools.partial(fused_kernel, groups, fsdp, tp, capacity),
        out_shape=tuple(pltpu.VMEM(leaf.shape, leaf.dtype) for leaf in shapes),
        in_specs=[hbm] * 10,
        out_specs=(vmem, vmem, vmem, vmem),
        scratch_shapes=[
            pltpu.VMEM((1, cols), f32),
            pltpu.VMEM((1, images), jnp.int32),
            pltpu.VMEM((1, rows), jnp.int32),
            pltpu.VMEM((1, seq_lengths.shape[0]), jnp.int32),
            pltpu.VMEM((both, columns), bf16),
            pltpu.VMEM((columns, key_cols), bf16),
            pltpu.VMEM((rows, key_cols), bf16),
            pltpu.VMEM((LENGTH, cols), f32),
            pltpu.VMEM((LENGTH, cols), f32),
            pltpu.VMEM((both, key_cols), bf16),
            pltpu.VMEM((slots, images), bf16),
            pltpu.VMEM((slots, rows), bf16),
            pltpu.VMEM((rows, cols), f32),
            pltpu.VMEM((slots, cols), bf16),
            pltpu.VMEM((slots, cols), bf16),
            pltpu.VMEM((images, cols), bf16),
            pltpu.VMEM((columns, key_cols), f32),
            pltpu.VMEM((columns, key_cols), bf16),
            pltpu.VMEM((columns, key_cols), bf16),
            pltpu.VMEM((columns, key_cols), bf16),
            pltpu.VMEM((columns, key_cols), bf16),
            pltpu.VMEM((columns, key_cols), bf16),
            pltpu.VMEM((both, key_cols), f32),
            pltpu.VMEM((tp, both, cols), bf16),
            pltpu.VMEM((tp, both, cols), bf16),
            pltpu.VMEM((slots, cols), bf16),
            pltpu.VMEM((slots, cols), bf16),
            pltpu.VMEM((block, cols), bf16),
            pltpu.VMEM((blocks, block // W_PARTS, key_cols), bf16),
            dma(9), dma(w_steps * W_FINE), one, one, one, one, one, one, one, one, one,
            dma(g_steps), dma(g_steps), dma(blocks * G_SIDES[0]), dma(blocks * W_FINE),
        ],
        compiler_params=pltpu.CompilerParams(
            collective_id=0, has_side_effects=True, vmem_limit_bytes=44 * 1024 * 1024
        ),
        name="fused",
    )(*(pltpu.with_memory_space_constraint(operand, pltpu.HBM) for operand in operands))
    return pl.pallas_call(
        write_kernel,
        out_shape=shapes,
        in_specs=[vmem] * 4,
        out_specs=(pl.BlockSpec(memory_space=pl.ANY),) * 4,
        scratch_shapes=[dma(4)],
        compiler_params=pltpu.CompilerParams(vmem_limit_bytes=4 * 1024 * 1024),
        name="write",
    )(*held)


def solution(mesh):
    in_specs = (
        P(("group", "fsdp"), "tp"),
        P(("group", "fsdp"), "tp"),
        P(("group", "fsdp"), None),
        P("tp"),
        P(("group", "fsdp"), None),
        P(("group", "fsdp")),
        P(("group", "fsdp")),
        P(("group", "fsdp")),
    )
    out_specs = (
        P(("group", "fsdp"), "tp"),
        P(("group", "fsdp"), "tp"),
        P(("group", "fsdp"), "tp"),
        P(("group", "fsdp"), "tp"),
    )
    return jax.shard_map(
        per_device, mesh=mesh, in_specs=in_specs, out_specs=out_specs, check_vma=False
    )
```
